8 devices in a mesh: data: 8 (over z, y, x, core).
Axes of the slice: x: 2, y: 2, z: 1, core: 2. Of those that a mesh axis runs over, the one named last changes fastest.
Arguments:
- grad_attn: bfloat16 [8, 64, 16384], P('data')
- grad_mlp: bfloat16 [8, 32, 65536], P('data')
- grad_wide: bfloat16 [8, 16, 512], P('data')
- grad_vec: bfloat16 [8, 146, 128], P('data')
- weight_attn: float32 [64, 16384], P(None, 'data')
- weight_mlp: float32 [32, 65536], P(None, 'data')
- weight_wide: float32 [16, 512], P(None, 'data')
- weight_vec: float32 [146, 128], P(None, 'data')
- mom1_attn: float32 [64, 16384], P(None, 'data')
- mom1_mlp: float32 [32, 65536], P(None, 'data')
- mom1_wide: float32 [16, 512], P(None, 'data')
- mom1_vec: float32 [146, 128], P(None, 'data')
- mom2_attn: float32 [64, 16384], P(None, 'data')
- mom2_mlp: float32 [32, 65536], P(None, 'data')
- mom2_wide: float32 [16, 512], P(None, 'data')
- mom2_vec: float32 [146, 128], P(None, 'data')
Outputs:
- output 1: bfloat16 [64, 16384], replicated
- output 2: bfloat16 [32, 65536], replicated
- output 3: bfloat16 [16, 512], replicated
- output 4: bfloat16 [146, 128], replicated
- output 5: float32 [64, 16384], P(None, 'data')
- output 6: float32 [32, 65536], P(None, 'data')
- output 7: float32 [16, 512], P(None, 'data')
- output 8: float32 [146, 128], P(None, 'data')
- output 9: float32 [64, 16384], P(None, 'data')
- output 10: float32 [32, 65536], P(None, 'data')
- output 11: float32 [16, 512], P(None, 'data')
- output 12: float32 [146, 128], P(None, 'data')
- output 13: float32 [64, 16384], P(None, 'data')
- output 14: float32 [32, 65536], P(None, 'data')
- output 15: float32 [16, 512], P(None, 'data')
- output 16: float32 [146, 128], P(None, 'data')
All inputs are finite; a program needn't handle non-finite values.
Results may differ from the reference program's by a relative error of at most 0.001.
Values are sent between devices in bfloat16 or wider.
A program may use at most 1 GiB of HBM per device.

```python
import jax
import jax.numpy as jnp

GROUP_SIZE = 8
LAYERS = 16
D = 128
FF = 512
STEP_NUMBER = 10

LEARN_RATE = 0.04
BETA_FIRST = 0.9
BETA_SECOND = 0.999
EPSILON = 1e-6
WEIGHT_DECAY = 0.01
MAX_NORM = 1.0
TARGET_NORM = 3.0


def bank_layout():
    gain_rows = jnp.array([1.0, 0.0, 0.0, 0.0, 0.0, 0.0, 1.0, 0.0, 0.0] * LAYERS + [1.0, 0.0])
    counts = (4 * LAYERS, 2 * LAYERS, LAYERS, 9 * LAYERS + 2)
    lengths = (D * D, D * FF, FF, D)
    base_scales = (
        jnp.full((4 * LAYERS,), D ** -0.5),
        jnp.array([D ** -0.5, FF ** -0.5] * LAYERS),
        jnp.full((LAYERS,), 0.05),
        0.05 + 0.15 * gain_rows,
    )
    offsets = (jnp.zeros((4 * LAYERS,)), jnp.zeros((2 * LAYERS,)), jnp.zeros((LAYERS,)), gain_rows)
    return counts, lengths, base_scales, offsets


def setup_inputs(seed: int = 0) -> dict:
    root_key = jax.random.key(seed)
    counts, lengths, base_scales, offsets = bank_layout()
    bank_keys = [jax.random.split(jax.random.fold_in(root_key, bank_index), 6) for bank_index in range(4)]
    grad_mults = [jnp.exp(jax.random.uniform(bank_keys[bank_index][0], (counts[bank_index],), minval=-1.0, maxval=1.0)) for bank_index in range(4)]
    weighted = sum(lengths[bank_index] * jnp.sum(grad_mults[bank_index] ** 2) for bank_index in range(4))
    grad_unit = TARGET_NORM * jnp.sqrt(GROUP_SIZE / weighted)
    clip_guess = MAX_NORM / TARGET_NORM
    grad_banks, weights, firsts, seconds = [], [], [], []
    for bank_index in range(4):
        bank_keyset = bank_keys[bank_index]
        row_count = counts[bank_index]
        row_length = lengths[bank_index]
        grad_scale = grad_unit * grad_mults[bank_index]
        device_grads = jax.random.normal(bank_keyset[1], (GROUP_SIZE, row_count, row_length)) * grad_scale[None, :, None]
        grad_banks.append(device_grads.astype(jnp.bfloat16))
        weight_spread = jnp.exp(jax.random.uniform(bank_keyset[2], (row_count,), minval=-1.2, maxval=1.2))
        row_scale = base_scales[bank_index] * weight_spread
        weights.append(offsets[bank_index][:, None] + row_scale[:, None] * jax.random.normal(bank_keyset[3], (row_count, row_length)))
        moment_unit = clip_guess * grad_scale / GROUP_SIZE ** 0.5
        firsts.append(0.1 * moment_unit[:, None] * jax.random.normal(bank_keyset[4], (row_count, row_length)))
        seconds.append(0.001 * (moment_unit * moment_unit)[:, None] * jnp.exp(0.5 * jax.random.normal(bank_keyset[5], (row_count, row_length))))
    bank_names = ("attn", "mlp", "wide", "vec")
    inputs = {}
    for prefix, arrays in (("grad_", grad_banks), ("weight_", weights), ("mom1_", firsts), ("mom2_", seconds)):
        for bank_index in range(4):
            inputs[prefix + bank_names[bank_index]] = arrays[bank_index]
    return inputs


def lamb_bank(mean_grad, weight, first_moment, second_moment, clip_coef):
    clipped = clip_coef * mean_grad
    new_first = BETA_FIRST * first_moment + (1.0 - BETA_FIRST) * clipped
    new_second = BETA_SECOND * second_moment + (1.0 - BETA_SECOND) * (clipped * clipped)
    update = (new_first / (1.0 - BETA_FIRST ** STEP_NUMBER)) / (jnp.sqrt(new_second / (1.0 - BETA_SECOND ** STEP_NUMBER)) + EPSILON) + WEIGHT_DECAY * weight
    weight_norm = jnp.sqrt(jnp.sum(weight * weight, axis=1, keepdims=True))
    update_norm = jnp.sqrt(jnp.sum(update * update, axis=1, keepdims=True))
    new_weight = weight - LEARN_RATE * (weight_norm / update_norm) * update
    return new_weight.astype(jnp.bfloat16), new_weight, new_first, new_second


def reference(grad_attn, grad_mlp, grad_wide, grad_vec, weight_attn, weight_mlp, weight_wide, weight_vec, mom1_attn, mom1_mlp, mom1_wide, mom1_vec, mom2_attn, mom2_mlp, mom2_wide, mom2_vec):
    mean_attn = jnp.sum(grad_attn, axis=0, dtype=jnp.float32) / GROUP_SIZE
    mean_mlp = jnp.sum(grad_mlp, axis=0, dtype=jnp.float32) / GROUP_SIZE
    mean_wide = jnp.sum(grad_wide, axis=0, dtype=jnp.float32) / GROUP_SIZE
    mean_vec = jnp.sum(grad_vec, axis=0, dtype=jnp.float32) / GROUP_SIZE
    total_square = jnp.sum(mean_attn * mean_attn) + jnp.sum(mean_mlp * mean_mlp) + jnp.sum(mean_wide * mean_wide) + jnp.sum(mean_vec * mean_vec)
    clip_coef = jnp.minimum(1.0, MAX_NORM / jnp.sqrt(total_square))
    attn_out = lamb_bank(mean_attn, weight_attn, mom1_attn, mom2_attn, clip_coef)
    mlp_out = lamb_bank(mean_mlp, weight_mlp, mom1_mlp, mom2_mlp, clip_coef)
    wide_out = lamb_bank(mean_wide, weight_wide, mom1_wide, mom2_wide, clip_coef)
    vec_out = lamb_bank(mean_vec, weight_vec, mom1_vec, mom2_vec, clip_coef)
    return (attn_out[0], mlp_out[0], wide_out[0], vec_out[0], attn_out[1], mlp_out[1], wide_out[1], vec_out[1], attn_out[2], mlp_out[2], wide_out[2], vec_out[2], attn_out[3], mlp_out[3], wide_out[3], vec_out[3])
```

```python
import functools

import jax
import jax.numpy as jnp
from jax import lax
from jax.experimental import pallas as pl
from jax.experimental.pallas import tpu as pltpu
from jax.sharding import PartitionSpec as P

STEP_NUMBER = 10
LEARN_RATE = 0.04
BETA_FIRST = 0.9
BETA_SECOND = 0.999
EPSILON = 1e-6
WEIGHT_DECAY = 0.01
MAX_NORM = 1.0
FIRST_SCALE = 1.0 / (1.0 - BETA_FIRST ** STEP_NUMBER)
SECOND_SCALE = 1.0 / (1.0 - BETA_SECOND ** STEP_NUMBER)

MESH = pl.DeviceIdType.MESH
LANES = 128
TALL = 16
VEC = 146
VEC_PAD = 256
ATTN_SHARD = 2048
MLP_SHARD = 8192
PIECE = 4096
STEP = 1024
BLOCK = 512
CHUNKS = 3
MIB = 2 ** 20
PEERS = range(1, 8)
CHUNK_HALVES = tuple((chunk, half) for chunk in range(CHUNKS) for half in range(2))
ROWS = (64, 32, TALL, VEC)
LENGTHS = (16384, 65536, BLOCK, LANES)
SHARDS = ((64, ATTN_SHARD), (32, MLP_SHARD), (TALL, 64), (TALL, VEC))


def flip(index, mask):
    core, x, y = index % 2, (index // 2) % 2, index // 4
    if mask & 1:
        core = 1 - core
    if mask & 2:
        x = 1 - x
    if mask & 4:
        y = 1 - y
    return y * 4 + x * 2 + core


def direction(first, weight, second, total, clip):
    clipped = clip * total
    new_first = BETA_FIRST * first + (1.0 - BETA_FIRST) * clipped
    new_second = BETA_SECOND * second + (1.0 - BETA_SECOND) * (clipped * clipped)
    update = (new_first * FIRST_SCALE) / (jnp.sqrt(new_second * SECOND_SCALE) + EPSILON) + WEIGHT_DECAY * weight
    return update, new_first, new_second


def fold(square):
    rows, columns = square.shape
    parts = [square[r:r + 8, k:k + LANES] for r in range(0, rows, 8) for k in range(0, columns, LANES)]
    while len(parts) > 1:
        parts = [a + b for a, b in zip(parts[::2], parts[1::2])] + ([parts[-1]] if len(parts) % 2 else [])
    return parts[0]


def kernel(*refs):
    grads, weights, firsts, seconds = refs[0:4], refs[4:8], refs[8:12], refs[12:TALL]
    replicas, new_weights, new_firsts, new_seconds = refs[TALL:20], refs[20:24], refs[24:28], refs[28:32]
    (recv_attn, recv_mlp, part_attn, part_mlp, last_attn, last_mlp, sum_attn, sum_mlp, sum_wide, sum_vec,
     recv_wide, recv_vec, vec_out, vec_in, vec_wide, vec_tall, vec_wide2, all_wide, all_vec,
     norm_tiles, weight_tiles, update_tiles, rows_acc, vec_row,
     scatter_recv, scatter_send, state_sem, last_send, last_recv, wide_send, wide_recv, vec_send, vec_recv,
     tile_send, tile_recv, own_send, own_recv, pass_send, pass_recv, pair_send, pair_recv,
     small_send, small_recv) = refs[32:]
    me = lax.axis_index("data")
    core = me % 2
    near = ((2, 4), (4, 2))

    loads = []
    for source, target in ((weights, new_weights), (firsts, new_firsts), (seconds, new_seconds)):
        for bank in range(4):
            loads.append(pltpu.make_async_copy(source[bank], target[bank], state_sem.at[len(loads)]))

    def grad_chunk(half, owner, chunk):
        if chunk < 2:
            start = pl.multiple_of(owner * MLP_SHARD + chunk * PIECE, PIECE)
            return grads[1].at[pl.ds(TALL * half, TALL), pl.ds(start, PIECE)]
        return grads[0].at[pl.ds(32 * half, 32), pl.ds(pl.multiple_of(owner * ATTN_SHARD, ATTN_SHARD), ATTN_SHARD)]

    def recv_chunk(half, keep, slot, chunk):
        if chunk < 2:
            return recv_mlp.at[half, keep, slot, :, pl.ds(chunk * PIECE, PIECE)]
        return recv_attn.at[half, keep, slot]

    def pair_chunk(attn, mlp, half, chunk):
        if chunk < 2:
            return mlp.at[half, :, pl.ds(chunk * PIECE, PIECE)]
        return attn.at[half]

    def replica_chunk(half, owner, chunk):
        if chunk < 2:
            start = pl.multiple_of(owner * MLP_SHARD + chunk * PIECE, PIECE)
            return replicas[1].at[pl.ds(TALL * half, TALL), pl.ds(start, PIECE)]
        return replicas[0].at[pl.ds(32 * half, 32), pl.ds(pl.multiple_of(owner * ATTN_SHARD, ATTN_SHARD), ATTN_SHARD)]

    def remote(source, target, send, recv, device):
        return pltpu.make_async_remote_copy(src_ref=source, dst_ref=target, send_sem=send, recv_sem=recv,
                                            device_id=(device,), device_id_type=MESH)

    own = {}
    for keep in range(2):
        for chunk in range(CHUNKS):
            for half in range(2):
                owner = me if keep else flip(me, near[half][1])
                own[half, keep, chunk] = pltpu.make_async_copy(
                    grad_chunk(half, owner, chunk), recv_chunk(half, keep, 0, chunk), scatter_recv.at[half, keep, 0, chunk])
                own[half, keep, chunk].start()
    for load in loads:
        load.start()
    wide_own = pltpu.make_async_copy(
        grads[2].at[:, pl.ds(pl.multiple_of((me // 2) * LANES, LANES), LANES)], recv_wide.at[me], wide_recv.at[0])
    wide_own.start()
    vec_load = pltpu.make_async_copy(grads[3], vec_in, vec_recv.at[0])
    vec_load.start()

    barrier = pltpu.get_barrier_semaphore()
    for mask in PEERS:
        pl.semaphore_signal(barrier, inc=1, device_id=(flip(me, mask),), device_id_type=MESH)
    pl.semaphore_wait(barrier, 7)

    sends = []

    def send(*copy):
        copy = remote(*copy)
        copy.start()
        sends.append(copy)
        return copy

    def scatter(keep):
        for chunk in range(CHUNKS):
            for slot in range(3):
                for half in range(2):
                    target = flip(me, 1) if slot == 0 else flip(me, near[half][0]) // 2 * 2 + slot - 1
                    owner = target if keep else flip(target, near[half][1])
                    index = 1 if slot == 0 else 2 + core
                    send(grad_chunk(half, owner, chunk), recv_chunk(half, keep, index, chunk),
                         scatter_send.at[half, keep, slot, chunk], scatter_recv.at[half, keep, index, chunk], target)

    scatter(0)

    vec_load.wait()
    vec_wide[...] = jnp.zeros_like(vec_wide)
    vec_wide[0:VEC, :] = vec_in[...].astype(jnp.float32)
    vec_out[...] = vec_wide[...].T.astype(jnp.bfloat16)
    recv_vec[me] = vec_out[pl.ds(pl.multiple_of(me * TALL, TALL), TALL), :]
    small = []
    for mask in PEERS:
        target = flip(me, mask)
        small.append(send(grads[2].at[:, pl.ds(pl.multiple_of((target // 2) * LANES, LANES), LANES)], recv_wide.at[me],
                          wide_send.at[mask], wide_recv.at[mask], target))
        small.append(send(vec_out.at[pl.ds(pl.multiple_of(target * TALL, TALL), TALL), :], recv_vec.at[me],
                          vec_send.at[mask], vec_recv.at[mask], target))
    scatter(1)

    def exchange(tiles, which, value):
        tiles[me] = value
        return [send(tiles.at[me], tiles.at[me], tile_send.at[which, mask], tile_recv.at[which, mask], flip(me, mask))
                for mask in PEERS]

    def collect(tiles, copies):
        for copy in copies:
            copy.wait_recv()
        total = tiles[0]
        for index in PEERS:
            total = total + tiles[index]
        return total

    row = lax.broadcasted_iota(jnp.int32, (LANES, LANES), 0)
    lane = lax.broadcasted_iota(jnp.int32, (LANES, LANES), 1)
    eye = row == lane
    sub = lax.broadcasted_iota(jnp.int32, (8, LANES), 0)

    def norm_tile(acc, vec_square):
        column = jnp.sum(acc[...], axis=1, keepdims=True)
        lanes = jnp.sum(jnp.where(eye, column, 0.0), axis=0, keepdims=True)
        vec_row[...] = jnp.zeros_like(vec_row)
        vec_row[0:1, 0:VEC] = jnp.sum(vec_square, axis=0, keepdims=True)
        low, high = vec_row[0:1, 0:LANES], vec_row[0:1, LANES:VEC_PAD]
        return jnp.where(sub == 0, lanes, jnp.where(sub == 1, low, jnp.where(sub == 2, high, 0.0)))

    for load in loads:
        load.wait()
    rows_acc[...] = jnp.zeros_like(rows_acc)

    def square_rows(ref, first, groups, columns):
        def group(g, carry):
            rows = pl.ds(pl.multiple_of(g * 8, 8), 8)

            def step(j, acc):
                value = ref[rows, pl.ds(pl.multiple_of(j * STEP, STEP), STEP)]
                return acc + fold(value * value)

            rows_acc[pl.ds(pl.multiple_of(first + g * 8, 8), 8), :] = lax.fori_loop(
                0, columns // STEP, step, jnp.zeros((8, LANES), jnp.float32))
            return carry

        lax.fori_loop(0, groups, group, 0)

    square_rows(new_weights[0], 0, 8, ATTN_SHARD)
    square_rows(new_weights[1], 64, 4, MLP_SHARD)
    wide_weight, vec_weight = new_weights[2][...], new_weights[3][...]
    rows_acc[96:112, 0:64] = wide_weight * wide_weight
    weight_copies = exchange(weight_tiles, 0, norm_tile(rows_acc, vec_weight * vec_weight))

    wide_own.wait()
    for copy in small:
        copy.wait_recv()
    wide_total = recv_wide[0].astype(jnp.float32)
    vec_total = recv_vec[0].astype(jnp.float32)
    for index in PEERS:
        wide_total = wide_total + recv_wide[index].astype(jnp.float32)
        vec_total = vec_total + recv_vec[index].astype(jnp.float32)
    wide_total = jnp.where(core == 0, wide_total[:, 0:64], wide_total[:, 64:LANES])
    sum_wide[...] = wide_total
    vec_total = vec_total[:, 0:VEC]
    sum_vec[...] = vec_total

    def blocks(chunk, step, init):
        rows, columns = (TALL, PIECE) if chunk < 2 else (32, ATTN_SHARD)
        for r in range(0, rows, TALL):
            init = lax.fori_loop(0, columns // BLOCK, functools.partial(
                lambda first, j, carry: step(first, pl.multiple_of(j * BLOCK, BLOCK), carry), r), init)
        return init

    def gather_sum(half, keep, chunk):
        own[half, keep, chunk].wait()
        for slot in range(1, 4):
            remote(recv_chunk(half, keep, slot, chunk), recv_chunk(half, keep, slot, chunk),
                   scatter_send.at[half, keep, 0, chunk], scatter_recv.at[half, keep, slot, chunk], flip(me, 1)).wait_recv()

        def step(r, c, carry):
            if chunk < 2:
                value = [recv_mlp[half, keep, s, :, pl.ds(chunk * PIECE + c, BLOCK)].astype(jnp.float32) for s in range(4)]
            else:
                value = [recv_attn[half, keep, s, r:r + TALL, pl.ds(c, BLOCK)].astype(jnp.float32) for s in range(4)]
            value = (value[0] + value[1]) + (value[2] + value[3])
            if keep:
                if chunk < 2:
                    sum_mlp[TALL * half:TALL * half + TALL, pl.ds(chunk * PIECE + c, BLOCK)] = value
                else:
                    sum_attn[32 * half + r:32 * half + r + TALL, pl.ds(c, BLOCK)] = value
            elif chunk < 2:
                part_mlp[half, :, pl.ds(chunk * PIECE + c, BLOCK)] = value
            else:
                part_attn[half, r:r + TALL, pl.ds(c, BLOCK)] = value
            return carry

        blocks(chunk, step, 0)

    last = {}
    for chunk, half in CHUNK_HALVES:
        gather_sum(half, 0, chunk)
        last[half, chunk] = send(
            pair_chunk(part_attn, part_mlp, half, chunk), pair_chunk(last_attn, last_mlp, half, chunk),
            last_send.at[half, chunk], last_recv.at[half, chunk], flip(me, near[half][1]))
    for chunk, half in CHUNK_HALVES:
        gather_sum(half, 1, chunk)

    square = jnp.concatenate([wide_total * wide_total, jnp.zeros((TALL, 64), jnp.float32)], axis=1)
    square = fold(square)
    vec_row[...] = jnp.zeros_like(vec_row)
    vec_row[0:1, 0:VEC] = jnp.sum(vec_total * vec_total, axis=0, keepdims=True)
    square = square + vec_row[:, 0:LANES] + vec_row[:, LANES:VEC_PAD]
    for chunk, half in CHUNK_HALVES:
        last[half, chunk].wait_recv()

        def step(r, c, acc):
            if chunk < 2:
                place = (slice(TALL * half, TALL * half + TALL), pl.ds(chunk * PIECE + c, BLOCK))
                value = sum_mlp[place] + last_mlp[half, :, pl.ds(chunk * PIECE + c, BLOCK)]
                sum_mlp[place] = value
            else:
                place = (slice(32 * half + r, 32 * half + r + TALL), pl.ds(c, BLOCK))
                value = sum_attn[place] + last_attn[half, r:r + TALL, pl.ds(c, BLOCK)]
                sum_attn[place] = value
            return acc + fold(value * value)

        square = blocks(chunk, step, square)

    square = collect(norm_tiles, exchange(norm_tiles, 1, square))
    square = jnp.sum(jnp.sum(square, axis=1, keepdims=True), axis=0, keepdims=True)
    clip = jnp.minimum(1.0, (8.0 * MAX_NORM) / jnp.sqrt(jnp.broadcast_to(square, (8, LANES)))) * 0.125

    rows_acc[...] = jnp.zeros_like(rows_acc)
    clip_block = jnp.concatenate([clip] * 8, axis=1)

    def update_rows(bank, totals, first, groups, columns):
        def group(g, carry):
            rows = pl.ds(pl.multiple_of(g * 8, 8), 8)

            def step(j, acc):
                place = (rows, pl.ds(pl.multiple_of(j * STEP, STEP), STEP))
                update, new_first, new_second = direction(
                    new_firsts[bank][place], new_weights[bank][place], new_seconds[bank][place], totals[place], clip_block)
                totals[place] = update
                new_firsts[bank][place] = new_first
                new_seconds[bank][place] = new_second
                return acc + fold(update * update)

            rows_acc[pl.ds(pl.multiple_of(first + g * 8, 8), 8), :] = lax.fori_loop(
                0, columns // STEP, step, jnp.zeros((8, LANES), jnp.float32))
            return carry

        lax.fori_loop(0, groups, group, 0)

    update_rows(0, sum_attn, 0, 8, ATTN_SHARD)
    update_rows(1, sum_mlp, 64, 4, MLP_SHARD)
    wide_update, new_first, new_second = direction(
        new_firsts[2][...], wide_weight, new_seconds[2][...], sum_wide[...], clip[0:1, 0:1])
    new_firsts[2][...] = new_first
    new_seconds[2][...] = new_second
    rows_acc[96:112, 0:64] = wide_update * wide_update
    vec_update, new_first, new_second = direction(
        new_firsts[3][...], vec_weight, new_seconds[3][...], sum_vec[...], clip[0:1, 0:1])
    new_firsts[3][...] = new_first
    new_seconds[3][...] = new_second
    update_copies = exchange(update_tiles, 2, norm_tile(rows_acc, vec_update * vec_update))
    weight_norms = jnp.sqrt(collect(weight_tiles, weight_copies))
    ratio = LEARN_RATE * (weight_norms / jnp.sqrt(collect(update_tiles, update_copies)))
    rows_acc[...] = jnp.broadcast_to(
        jnp.sum(jnp.where(eye, ratio[0:1, :], 0.0), axis=1, keepdims=True), (LANES, LANES))

    own_copies = {}

    def send_own(half, chunk, way):
        device = flip(me, (1, 2, 4)[way])
        place = replica_chunk(half, me, chunk)
        own_copies[half, chunk, way] = send(
            place, place, own_send.at[half, chunk, way], own_recv.at[half, chunk, way], device)

    for chunk, half in CHUNK_HALVES:
        def step(r, c, carry):
            bank = 1 if chunk < 2 else 0
            first = TALL * half if chunk < 2 else 32 * half + r
            column = chunk * PIECE + c if chunk < 2 else c
            scale = jnp.concatenate([rows_acc[64 * bank + first:64 * bank + first + TALL, :]] * (BLOCK // LANES), axis=1)
            place = (slice(first, first + TALL), pl.ds(column, BLOCK))
            totals = sum_mlp if bank else sum_attn
            value = new_weights[bank][place] - scale * totals[place]
            new_weights[bank][place] = value
            start = pl.multiple_of(me * SHARDS[bank][1] + column, BLOCK)
            replicas[bank][first:first + TALL, pl.ds(start, BLOCK)] = value.astype(jnp.bfloat16)
            return carry

        blocks(chunk, step, 0)
        send_own(half, chunk, 1 + half)
        send_own(half, chunk, 0)
    for chunk, half in CHUNK_HALVES:
        send_own(half, chunk, 2 - half)

    value = wide_weight - rows_acc[96:112, 0:64] * wide_update
    new_weights[2][...] = value
    all_wide[me] = jnp.concatenate([value, value], axis=1).astype(jnp.bfloat16)
    vec_row[0:1, 0:LANES] = ratio[1:2, :]
    vec_row[0:1, LANES:VEC_PAD] = ratio[2:3, :]
    value = vec_weight - vec_row[0:1, 0:VEC] * vec_update
    new_weights[3][...] = value
    vec_wide2[...] = jnp.zeros_like(vec_wide2)
    vec_wide2[:, 0:VEC] = value
    all_vec[me] = vec_wide2[...].astype(jnp.bfloat16)
    small = []
    for mask in PEERS:
        target = flip(me, mask)
        small.append(send(all_wide.at[me], all_wide.at[me], small_send.at[0, mask], small_recv.at[0, mask], target))
        small.append(send(all_vec.at[me], all_vec.at[me], small_send.at[1, mask], small_recv.at[1, mask], target))

    pair = []

    def send_pair(half, owner, chunk, slot):
        place = replica_chunk(half, owner, chunk)
        pair.append(send(place, place, pair_send.at[half, chunk, slot], pair_recv.at[half, chunk, slot], flip(me, 1)))

    passed = {}
    for chunk, half in CHUNK_HALVES:
        own_copies[half, chunk, 1 + half].wait_recv()
        owner = flip(me, near[half][0])
        place = replica_chunk(half, owner, chunk)
        passed[half, chunk] = send(place, place, pass_send.at[half, chunk], pass_recv.at[half, chunk],
                                   flip(me, near[half][1]))
        send_pair(half, owner, chunk, 0)
    for copy in small:
        copy.wait_recv()
    low_lanes = lax.broadcasted_iota(jnp.int32, (TALL, LANES), 1) < 64
    for index in range(4):
        tile = jnp.where(low_lanes, all_wide[2 * index].astype(jnp.float32), all_wide[2 * index + 1].astype(jnp.float32))
        replicas[2][:, LANES * index:LANES * index + LANES] = tile.astype(jnp.bfloat16)
    for index in range(8):
        vec_tall[TALL * index:TALL * index + TALL, :] = all_vec[index].astype(jnp.float32)
    vec_wide[...] = vec_tall[...].T
    replicas[3][...] = vec_wide[0:VEC, :].astype(jnp.bfloat16)
    for chunk, half in CHUNK_HALVES:
        own_copies[half, chunk, 2 - half].wait_recv()
        send_pair(half, flip(me, near[half][1]), chunk, 1)
    for chunk, half in CHUNK_HALVES:
        passed[half, chunk].wait_recv()
        send_pair(half, flip(me, 6), chunk, 2)
    for chunk, half in CHUNK_HALVES:
        own_copies[half, chunk, 0].wait_recv()
    for copy in pair:
        copy.wait_recv()
    for copy in sends:
        copy.wait_send()


def write_out(*refs):
    count = (len(refs) - 1) // 2
    copies = [pltpu.make_async_copy(refs[k], refs[count + k], refs[-1].at[k]) for k in range(count)]
    for copy in copies:
        copy.start()
    for copy in copies:
        copy.wait()


def solution(mesh):
    shards = [jax.ShapeDtypeStruct(shape, jnp.float32) for shape in SHARDS]
    shapes = [jax.ShapeDtypeStruct(shape, jnp.bfloat16) for shape in zip(ROWS, LENGTHS)] + shards * 3
    f32, bf16, vmem = jnp.float32, jnp.bfloat16, pltpu.VMEM
    dma = pltpu.SemaphoreType.DMA
    scratch = [
        vmem((2, 2, 4, 32, ATTN_SHARD), bf16), vmem((2, 2, 4, TALL, MLP_SHARD), bf16),
        vmem((2, 32, ATTN_SHARD), f32), vmem((2, TALL, MLP_SHARD), f32), vmem((2, 32, ATTN_SHARD), f32), vmem((2, TALL, MLP_SHARD), f32),
        vmem((64, ATTN_SHARD), f32), vmem((32, MLP_SHARD), f32), vmem((TALL, 64), f32), vmem((TALL, VEC), f32),
        vmem((8, TALL, LANES), bf16), vmem((8, TALL, VEC_PAD), bf16), vmem((LANES, VEC_PAD), bf16),
        vmem((VEC, LANES), bf16), vmem((VEC_PAD, LANES), f32), vmem((LANES, VEC_PAD), f32), vmem((TALL, VEC_PAD), f32),
        vmem((8, TALL, LANES), bf16), vmem((8, TALL, VEC_PAD), bf16),
        vmem((8, 8, LANES), f32), vmem((8, 8, LANES), f32), vmem((8, 8, LANES), f32), vmem((LANES, LANES), f32), vmem((8, VEC_PAD), f32),
        dma((2, 2, 4, CHUNKS)), dma((2, 2, 3, CHUNKS)), dma((12,)), dma((2, CHUNKS)), dma((2, CHUNKS)),
        dma((8,)), dma((8,)), dma((8,)), dma((8,)), dma((3, 8)), dma((3, 8)),
        dma((2, CHUNKS, 3)), dma((2, CHUNKS, 3)), dma((2, CHUNKS)), dma((2, CHUNKS)),
        dma((2, CHUNKS, 3)), dma((2, CHUNKS, 3)), dma((2, 8)), dma((2, 8)),
    ]
    step = pl.pallas_call(
        kernel,
        out_shape=[pltpu.VMEM(shape.shape, shape.dtype) for shape in shapes],
        in_specs=[pl.BlockSpec(memory_space=pl.ANY)] * TALL,
        out_specs=[pl.BlockSpec(memory_space=pltpu.VMEM)] * TALL,
        scratch_shapes=scratch,
        compiler_params=pltpu.CompilerParams(collective_id=0, has_side_effects=True, vmem_limit_bytes=36 * MIB),
        name="lamb_step",
    )
    finish = pl.pallas_call(
        write_out,
        out_shape=shapes,
        in_specs=[pl.BlockSpec(memory_space=pl.ANY)] * TALL,
        out_specs=[pl.BlockSpec(memory_space=pl.ANY)] * TALL,
        scratch_shapes=[dma((TALL,))],
        compiler_params=pltpu.CompilerParams(vmem_limit_bytes=MIB),
        name="write_out",
    )

    def local_step(*banks):
        banks = [bank[0] for bank in banks[:4]] + [bank.T if bank.shape == (VEC, TALL) else bank for bank in banks[4:]]
        banks = [pltpu.with_memory_space_constraint(bank, pltpu.HBM) for bank in banks]
        results = finish(*step(*banks))
        return tuple(value.T if value.shape == (TALL, VEC) else value for value in results)

    grad_spec, shard_spec, full_spec = P("data", None, None), P(None, "data"), P(None, None)
    return jax.shard_map(local_step, mesh=mesh, in_specs=(grad_spec,) * 4 + (shard_spec,) * 12,
                         out_specs=(full_spec,) * 4 + (shard_spec,) * 12, check_vma=False)
```

```python
import functools

import jax
import jax.numpy as jnp
from jax import lax
from jax.experimental import pallas as pl
from jax.experimental.pallas import tpu as pltpu
from jax.sharding import PartitionSpec as P

STEP_NUMBER = 10
LEARN_RATE = 0.04
BETA_FIRST = 0.9
BETA_SECOND = 0.999
EPSILON = 1e-6
WEIGHT_DECAY = 0.01
MAX_NORM = 1.0
FIRST_SCALE = 1.0 / (1.0 - BETA_FIRST ** STEP_NUMBER)
SECOND_SCALE = 1.0 / (1.0 - BETA_SECOND ** STEP_NUMBER)

MESH = pl.DeviceIdType.MESH
LANES = 128
TALL = 16
HALF = 64
VEC = 146
VEC_PAD = 256
ATTN_SHARD = 2048
MLP_SHARD = 8192
STEP = 1024
BLOCK = 512
MIB = 2 ** 20
ROWS = (HALF, 32, TALL, VEC)
LENGTHS = (16384, 65536, BLOCK, LANES)
SHARDS = ((HALF, ATTN_SHARD), (32, MLP_SHARD), (TALL, HALF), (TALL, VEC))
ATTN, MLP, SMALL = range(3)
HALVES = range(2)
SHAPES = ((32, ATTN_SHARD), (TALL, MLP_SHARD))
PEER, ALONG_X, ALONG_Y = 1, 2, 4
NEAR = ((ALONG_X, ALONG_Y), (ALONG_Y, ALONG_X))
FAR_FIRST = tuple(reversed(range(1, 8)))


def flip(index, mask):
    core, x, y = index % 2, (index // 2) % 2, index // 4
    if mask & PEER:
        core = 1 - core
    if mask & ALONG_X:
        x = 1 - x
    if mask & ALONG_Y:
        y = 1 - y
    return y * 4 + x * 2 + core


def aligned(index, size):
    return pl.ds(pl.multiple_of(index * size, size), size)


def moments(first, second, total, clip):
    clipped = clip * total
    new_first = BETA_FIRST * first + (1.0 - BETA_FIRST) * clipped
    new_second = BETA_SECOND * second + (1.0 - BETA_SECOND) * (clipped * clipped)
    return new_first, new_second


def direction(new_first, new_second, weight):
    return (new_first * FIRST_SCALE) / (jnp.sqrt(new_second * SECOND_SCALE) + EPSILON) + WEIGHT_DECAY * weight


def fold(square):
    rows, columns = square.shape
    parts = [square[r:r + 8, k:k + LANES] for r in range(0, rows, 8) for k in range(0, columns, LANES)]
    while len(parts) > 1:
        parts = [a + b for a, b in zip(parts[::2], parts[1::2])] + ([parts[-1]] if len(parts) % 2 else [])
    return parts[0]


def add_all(values):
    return functools.reduce(lambda a, b: a + b, values)


def kernel(*refs):
    grads, weights, firsts, seconds = refs[0:4], refs[4:8], refs[8:12], refs[12:16]
    replicas, new_weights, new_firsts, new_seconds = refs[16:20], refs[20:24], refs[24:28], refs[28:32]
    (recv_attn, recv_mlp, recv_wide, recv_vec, part_attn, part_mlp, part_wide, part_vec,
     last_attn, last_mlp, last_wide, last_vec, sum_attn, sum_mlp, sum_wide, sum_vec, dir_attn, dir_mlp,
     vec_in, vec_out, vec_rows, vec_columns, vec_row, all_wide, all_vec, start_tiles, attn_tiles, rest_tiles, row_acc,
     state_sem, vec_sem, scatter_send, scatter_recv, last_send, last_recv, tile_send, tile_recv,
     own_send, own_recv, pass_send, pass_recv, pair_send, pair_recv) = refs[32:]
    me = lax.axis_index("data")
    core = me % 2

    def grad_chunk(half, owner, chunk):
        if chunk == MLP:
            return grads[1].at[pl.ds(TALL * half, TALL), aligned(owner, MLP_SHARD)]
        if chunk == ATTN:
            return grads[0].at[pl.ds(32 * half, 32), aligned(owner, ATTN_SHARD)]
        return vec_out.at[aligned(owner, TALL), :] if half else grads[2].at[:, aligned(owner // 2, LANES)]

    def recv_chunk(half, keep, slot, chunk):
        if chunk == SMALL:
            return (recv_vec if half else recv_wide).at[keep, slot]
        return (recv_attn, recv_mlp)[chunk].at[half, keep, slot]

    def sum_chunk(half, chunk, buffers):
        if chunk == SMALL:
            return buffers[3] if half else buffers[2]
        return buffers[chunk].at[half]

    parts, lasts = (part_attn, part_mlp, part_wide, part_vec), (last_attn, last_mlp, last_wide, last_vec)

    def replica_chunk(half, owner, chunk):
        if chunk == MLP:
            return replicas[1].at[pl.ds(TALL * half, TALL), aligned(owner, MLP_SHARD)]
        if chunk == ATTN:
            return replicas[0].at[pl.ds(32 * half, 32), aligned(owner, ATTN_SHARD)]
        return (all_vec if half else all_wide).at[owner]

    def remote(source, target, send_sem, recv_sem, device):
        return pltpu.make_async_remote_copy(src_ref=source, dst_ref=target, send_sem=send_sem, recv_sem=recv_sem,
                                            device_id=(device,), device_id_type=MESH)

    sends = []

    def send(*copy):
        copy = remote(*copy)
        copy.start()
        sends.append(copy)
        return copy

    vec_load = pltpu.make_async_copy(grads[3], vec_in, vec_sem)
    vec_load.start()
    own = {}
    for keep in range(2):
        for half in HALVES:
            for chunk in (MLP, ATTN, SMALL)[:3 - half]:
                owner = me if keep else flip(me, NEAR[half][1])
                own[half, keep, chunk] = pltpu.make_async_copy(
                    grad_chunk(half, owner, chunk), recv_chunk(half, keep, 0, chunk), scatter_recv.at[half, keep, 0, chunk])
                own[half, keep, chunk].start()
    loads = []
    for source, target in ((weights, new_weights), (firsts, new_firsts), (seconds, new_seconds)):
        for bank in range(4):
            loads.append(pltpu.make_async_copy(source[bank], target[bank], state_sem.at[len(loads)]))
            loads[-1].start()

    barrier = pltpu.get_barrier_semaphore()
    near = (1, 2, 3, 4, 5)
    for mask in near:
        pl.semaphore_signal(barrier, inc=1, device_id=(flip(me, mask),), device_id_type=MESH)
    pl.semaphore_wait(barrier, len(near))

    def scatter(keep, chunk):
        for slot in range(3):
            for half in HALVES:
                target = flip(me, PEER) if slot == 0 else flip(me, NEAR[half][0]) // 2 * 2 + slot - 1
                owner = target if keep else flip(target, NEAR[half][1])
                index = 1 if slot == 0 else 2 + core
                send(grad_chunk(half, owner, chunk), recv_chunk(half, keep, index, chunk),
                     scatter_send.at[half, keep, slot, chunk], scatter_recv.at[half, keep, index, chunk], target)

    scatter(0, MLP)
    scatter(0, ATTN)
    vec_load.wait()
    vec_rows[...] = jnp.zeros_like(vec_rows)
    vec_rows[0:VEC, :] = vec_in[...].astype(jnp.float32)
    vec_out[...] = vec_rows[...].T.astype(jnp.bfloat16)
    recv_vec[0, 0] = vec_out[aligned(flip(me, NEAR[1][1]), TALL), :]
    recv_vec[1, 0] = vec_out[aligned(me, TALL), :]
    scatter(0, SMALL)
    scatter(1, MLP)
    scatter(1, ATTN)
    scatter(1, SMALL)

    row = lax.broadcasted_iota(jnp.int32, (LANES, LANES), 0)
    lane = lax.broadcasted_iota(jnp.int32, (LANES, LANES), 1)
    eye = row == lane
    sub = lax.broadcasted_iota(jnp.int32, (8, LANES), 0)

    def lanes_of(first, last):
        column = jnp.sum(row_acc[first:last, :], axis=1, keepdims=True)
        return jnp.sum(jnp.where(eye[first:last, :], column, 0.0), axis=0, keepdims=True)

    def vec_lanes(square):
        vec_row[...] = jnp.zeros_like(vec_row)
        vec_row[0:1, 0:VEC] = jnp.sum(square, axis=0, keepdims=True)
        return vec_row[0:1, 0:LANES], vec_row[0:1, LANES:VEC_PAD]

    def tile_of(rows):
        tile = jnp.zeros((8, LANES), jnp.float32)
        for index, value in enumerate(rows):
            tile = jnp.where(sub == index, value, tile)
        return tile

    def exchange(tiles, which, value):
        tiles[me] = value
        return [send(tiles.at[me], tiles.at[me], tile_send.at[which, mask], tile_recv.at[which, mask], flip(me, mask))
                for mask in FAR_FIRST]

    def collect(tiles, copies):
        for copy in copies:
            copy.wait_recv()
        return add_all([tiles[index] for index in range(8)])

    def by_rows(first, groups, columns, step):
        def group(g, carry):
            def inner(j, acc):
                return acc + step((aligned(g, 8), aligned(j, STEP)))

            row_acc[pl.ds(pl.multiple_of(first + g * 8, 8), 8), :] = lax.fori_loop(
                0, columns // STEP, inner, jnp.zeros((8, LANES), jnp.float32))
            return carry

        lax.fori_loop(0, groups, group, 0)

    def square_of(ref):
        return lambda place: fold(ref[place] * ref[place])

    for load in loads:
        load.wait()
    row_acc[...] = jnp.zeros_like(row_acc)
    by_rows(0, 8, ATTN_SHARD, square_of(new_weights[0]))
    by_rows(HALF, 4, MLP_SHARD, square_of(new_weights[1]))
    wide_weight, vec_weight = new_weights[2][...], new_weights[3][...]
    row_acc[96:112, 0:HALF] = wide_weight * wide_weight
    weight_lanes = lanes_of(0, LANES)
    weight_low, weight_high = vec_lanes(vec_weight * vec_weight)

    def by_blocks(chunk, step, init):
        rows, columns = SHAPES[chunk]
        for r in range(0, rows, TALL):
            init = lax.fori_loop(0, columns // BLOCK, functools.partial(
                lambda first, j, carry: step((pl.ds(first, TALL), aligned(j, BLOCK)), carry), r), init)
        return init

    def gather_sum(half, keep, chunk):
        if (half, keep, chunk) in own:
            own[half, keep, chunk].wait()
        for slot in range(1, 4):
            place = recv_chunk(half, keep, slot, chunk)
            remote(place, place, scatter_send.at[half, keep, 0, chunk], scatter_recv.at[half, keep, slot, chunk],
                   flip(me, PEER)).wait_recv()
        target = sum_chunk(half, chunk, (sum_attn, sum_mlp, sum_wide, sum_vec) if keep else parts)
        sources = [recv_chunk(half, keep, slot, chunk) for slot in range(4)]
        if chunk == SMALL:
            target[...] = add_all([source[...].astype(jnp.float32) for source in sources])
            return

        def step(place, carry):
            value = [source[place].astype(jnp.float32) for source in sources]
            target[place] = (value[0] + value[1]) + (value[2] + value[3])
            return carry

        by_blocks(chunk, step, 0)

    last = {}
    for chunk in (MLP, ATTN, SMALL):
        for half in HALVES:
            gather_sum(half, 0, chunk)
    for chunk in (SMALL, MLP, ATTN):
        for half in HALVES:
            last[half, chunk] = send(
                sum_chunk(half, chunk, parts), sum_chunk(half, chunk, lasts),
                last_send.at[half, chunk], last_recv.at[half, chunk], flip(me, NEAR[half][1]))
    for chunk in (MLP, ATTN, SMALL):
        for half in HALVES:
            gather_sum(half, 1, chunk)

    for half in HALVES:
        last[half, SMALL].wait_recv()
    wide_total = sum_wide[...] + last_wide[...]
    wide_total = jnp.where(core == 0, wide_total[:, 0:HALF], wide_total[:, HALF:LANES])
    vec_total = (sum_vec[...] + last_vec[...])[:, 0:VEC]
    square = fold(jnp.concatenate([wide_total * wide_total, jnp.zeros((TALL, HALF), jnp.float32)], axis=1))
    low, high = vec_lanes(vec_total * vec_total)
    square = square + tile_of([low, high])
    for chunk in (MLP, ATTN):
        for half in HALVES:
            last[half, chunk].wait_recv()
            total, rest = sum_chunk(half, chunk, (sum_attn, sum_mlp)), sum_chunk(half, chunk, lasts)

            def step(place, acc):
                value = total[place] + rest[place]
                total[place] = value
                return acc + fold(value * value)

            square = by_blocks(chunk, step, square)

    start = collect(start_tiles, exchange(start_tiles, 0, tile_of(
        [weight_lanes, weight_low, weight_high, jnp.sum(square, axis=0, keepdims=True)])))
    square = jnp.sum(jnp.sum(start[3:4, :], axis=1, keepdims=True), axis=0, keepdims=True)
    clip = jnp.minimum(1.0, (8.0 * MAX_NORM) / jnp.sqrt(jnp.broadcast_to(square, (8, LANES)))) * 0.125
    clip_block = jnp.concatenate([clip] * (STEP // LANES), axis=1)
    weight_norms = LEARN_RATE * jnp.sqrt(start)

    sums, directions = (sum_attn, sum_mlp), (dir_attn, dir_mlp)

    def update(bank, half):
        rows = SHAPES[bank][0]

        def step(place):
            state = (pl.ds(pl.multiple_of(half * rows + place[0].start, 8), 8), place[1])
            new_first, new_second = moments(
                new_firsts[bank][state], new_seconds[bank][state], sums[bank].at[half][place], clip_block)
            value = direction(new_first, new_second, new_weights[bank][state])
            directions[bank].at[half][place] = value
            return fold(value * value)

        by_rows(HALF * bank + half * rows, rows // 8, SHAPES[bank][1], step)

    def store_moments(bank, half):
        rows = SHAPES[bank][0]

        def step(place, carry):
            state = (pl.ds(half * rows + place[0].start, TALL), place[1])
            clip_wide = jnp.concatenate([clip_block[:, 0:BLOCK]] * 2, axis=0)
            new_first, new_second = moments(
                new_firsts[bank][state], new_seconds[bank][state], sums[bank].at[half][place], clip_wide)
            new_firsts[bank][state] = new_first
            new_seconds[bank][state] = new_second
            return carry

        by_blocks(bank, step, 0)

    def update_small(bank, total, weight):
        new_first, new_second = moments(new_firsts[bank][...], new_seconds[bank][...], total, clip[0:1, 0:1])
        new_firsts[bank][...] = new_first
        new_seconds[bank][...] = new_second
        return direction(new_first, new_second, weight)

    for half in HALVES:
        update(ATTN, half)
    attn_copies = exchange(attn_tiles, 1, tile_of([lanes_of(0, HALF)]))
    for half in HALVES:
        update(MLP, half)
    wide_dir = update_small(2, wide_total, wide_weight)
    vec_dir = update_small(3, vec_total, vec_weight)
    row_acc[96:112, 0:HALF] = wide_dir * wide_dir
    rest_copies = exchange(rest_tiles, 2, tile_of([lanes_of(HALF, LANES), *vec_lanes(vec_dir * vec_dir)]))
    for bank in (ATTN, MLP):
        for half in HALVES:
            store_moments(bank, half)

    own_copies = {}

    def send_own(half, chunk, way):
        place = replica_chunk(half, me, chunk)
        own_copies[half, chunk, way] = send(place, place, own_send.at[half, chunk, way], own_recv.at[half, chunk, way],
                                            flip(me, (PEER, ALONG_X, ALONG_Y)[way]))

    def spread_ratio(first, last, ratio):
        row_acc[first:last, :] = jnp.broadcast_to(
            jnp.sum(jnp.where(eye[first:last, :], ratio[0:1, :], 0.0), axis=1, keepdims=True), (last - first, LANES))

    def new_weight(bank, half):
        rows, columns = SHAPES[bank]

        def step(place, carry):
            first = half * rows + place[0].start
            scale = jnp.concatenate([row_acc[HALF * bank + first:HALF * bank + first + TALL, :]] * (BLOCK // LANES), axis=1)
            state = (pl.ds(first, TALL), place[1])
            value = new_weights[bank][state] - scale * directions[bank].at[half][place]
            new_weights[bank][state] = value
            target = pl.ds(pl.multiple_of(me * columns + place[1].start, BLOCK), BLOCK)
            replicas[bank][pl.ds(first, TALL), target] = value.astype(jnp.bfloat16)
            return carry

        by_blocks(bank, step, 0)
        send_own(half, bank, 1 + half)
        send_own(half, bank, 0)

    spread_ratio(0, HALF, weight_norms / jnp.sqrt(collect(attn_tiles, attn_copies)))
    for half in HALVES:
        new_weight(ATTN, half)
    ratio = weight_norms / jnp.sqrt(collect(rest_tiles, rest_copies))
    spread_ratio(HALF, LANES, ratio)
    for half in HALVES:
        new_weight(MLP, half)
    value = wide_weight - row_acc[96:112, 0:HALF] * wide_dir
    new_weights[2][...] = value
    all_wide[me] = jnp.concatenate([value, value], axis=1).astype(jnp.bfloat16)
    vec_row[0:1, 0:LANES] = ratio[1:2, :]
    vec_row[0:1, LANES:VEC_PAD] = ratio[2:3, :]
    value = vec_weight - vec_row[0:1, 0:VEC] * vec_dir
    new_weights[3][...] = value
    vec_columns[0:TALL, :] = jnp.zeros((TALL, VEC_PAD), jnp.float32)
    vec_columns[0:TALL, 0:VEC] = value
    all_vec[me] = vec_columns[0:TALL, :].astype(jnp.bfloat16)
    for half in HALVES:
        send_own(half, SMALL, 1 + half)
        send_own(half, SMALL, 0)
    for chunk in (ATTN, MLP, SMALL):
        for half in HALVES:
            send_own(half, chunk, 2 - half)

    pairs = {}

    def send_pair(half, owner, chunk, slot):
        place = replica_chunk(half, owner, chunk)
        pairs[half, chunk, slot] = send(
            place, place, pair_send.at[half, chunk, slot], pair_recv.at[half, chunk, slot], flip(me, PEER))

    passed = {}
    for chunk in (SMALL, MLP, ATTN):
        for half in HALVES:
            own_copies[half, chunk, 1 + half].wait_recv()
            owner = flip(me, NEAR[half][0])
            place = replica_chunk(half, owner, chunk)
            passed[half, chunk] = send(place, place, pass_send.at[half, chunk], pass_recv.at[half, chunk],
                                       flip(me, NEAR[half][1]))
            send_pair(half, owner, chunk, 0)
    for chunk in (ATTN, MLP, SMALL):
        for half in HALVES:
            own_copies[half, chunk, 2 - half].wait_recv()
            send_pair(half, flip(me, NEAR[half][1]), chunk, 1)
    for chunk in (SMALL, MLP, ATTN):
        for half in HALVES:
            passed[half, chunk].wait_recv()
            send_pair(half, flip(me, ALONG_X + ALONG_Y), chunk, 2)
            if chunk == SMALL:
                own_copies[half, chunk, 0].wait_recv()
                for slot in range(3):
                    pairs[half, chunk, slot].wait_recv()
        if chunk == SMALL:
            low_lanes = lax.broadcasted_iota(jnp.int32, (TALL, LANES), 1) < HALF
            for index in range(4):
                left, right = (all_wide[2 * index + k].astype(jnp.float32) for k in range(2))
                replicas[2][:, pl.ds(LANES * index, LANES)] = jnp.where(low_lanes, left, right).astype(jnp.bfloat16)
            for index in range(8):
                vec_columns[pl.ds(TALL * index, TALL), :] = all_vec[index].astype(jnp.float32)
            vec_rows[...] = vec_columns[...].T
            replicas[3][...] = vec_rows[0:VEC, :].astype(jnp.bfloat16)
    for chunk in (ATTN, MLP):
        for half in HALVES:
            own_copies[half, chunk, 0].wait_recv()
            for slot in range(3):
                pairs[half, chunk, slot].wait_recv()
    for copy in sends:
        copy.wait_send()


def write_out(*refs):
    count = (len(refs) - 1) // 2
    copies = [pltpu.make_async_copy(refs[k], refs[count + k], refs[-1].at[k]) for k in range(count)]
    for copy in copies:
        copy.start()
    for copy in copies:
        copy.wait()


def solution(mesh):
    shards = [jax.ShapeDtypeStruct(shape, jnp.float32) for shape in SHARDS]
    shapes = [jax.ShapeDtypeStruct(shape, jnp.bfloat16) for shape in zip(ROWS, LENGTHS)] + shards * 3
    f32, bf16 = jnp.float32, jnp.bfloat16
    dma = pltpu.SemaphoreType.DMA
    attn, mlp = SHAPES

    def sums(*lead):
        return [pltpu.VMEM((*lead, *attn), f32), pltpu.VMEM((*lead, *mlp), f32)]

    small_sums = [pltpu.VMEM((TALL, LANES), f32), pltpu.VMEM((TALL, VEC_PAD), f32)]
    scratch = [
        pltpu.VMEM((2, 2, 4, *attn), bf16), pltpu.VMEM((2, 2, 4, *mlp), bf16),
        pltpu.VMEM((2, 4, TALL, LANES), bf16), pltpu.VMEM((2, 4, TALL, VEC_PAD), bf16),
        *sums(2), *small_sums, *sums(2), *small_sums, *sums(2), *small_sums, *sums(2),
        pltpu.VMEM((VEC, LANES), bf16), pltpu.VMEM((LANES, VEC_PAD), bf16),
        pltpu.VMEM((VEC_PAD, LANES), f32), pltpu.VMEM((LANES, VEC_PAD), f32), pltpu.VMEM((8, VEC_PAD), f32),
        pltpu.VMEM((8, TALL, LANES), bf16), pltpu.VMEM((8, TALL, VEC_PAD), bf16),
        *[pltpu.VMEM((8, 8, LANES), f32)] * 3, pltpu.VMEM((LANES, LANES), f32),
        dma((12,)), dma, dma((2, 2, 3, 3)), dma((2, 2, 4, 3)), dma((2, 3)), dma((2, 3)), dma((3, 8)), dma((3, 8)),
        dma((2, 3, 3)), dma((2, 3, 3)), dma((2, 3)), dma((2, 3)), dma((2, 3, 3)), dma((2, 3, 3)),
    ]
    count = len(shapes)
    anywhere = [pl.BlockSpec(memory_space=pl.ANY)] * count
    step = pl.pallas_call(
        kernel,
        out_shape=[pltpu.VMEM(shape.shape, shape.dtype) for shape in shapes],
        in_specs=anywhere,
        out_specs=[pl.BlockSpec(memory_space=pltpu.VMEM)] * count,
        scratch_shapes=scratch,
        compiler_params=pltpu.CompilerParams(collective_id=0, has_side_effects=True, vmem_limit_bytes=36 * MIB),
        name="lamb_step",
    )
    finish = pl.pallas_call(
        write_out,
        out_shape=shapes,
        in_specs=anywhere,
        out_specs=anywhere,
        scratch_shapes=[dma((count,))],
        compiler_params=pltpu.CompilerParams(vmem_limit_bytes=MIB),
        name="write_out",
    )

    def local_step(*banks):
        banks = [bank[0] for bank in banks[:4]] + [bank.T if bank.shape == (VEC, TALL) else bank for bank in banks[4:]]
        banks = [pltpu.with_memory_space_constraint(bank, pltpu.HBM) for bank in banks]
        results = finish(*step(*banks))
        return tuple(value.T if value.shape == (TALL, VEC) else value for value in results)

    grad_spec, shard_spec, full_spec = P("data", None, None), P(None, "data"), P(None, None)
    return jax.shard_map(local_step, mesh=mesh, in_specs=(grad_spec,) * 4 + (shard_spec,) * 12,
                         out_specs=(full_spec,) * 4 + (shard_spec,) * 12, check_vma=False)
```

```python
import functools

import jax
import jax.numpy as jnp
from jax import lax
from jax.experimental import pallas as pl
from jax.experimental.pallas import tpu as pltpu
from jax.sharding import PartitionSpec as P

STEP_NUMBER = 10
LEARN_RATE = 0.04
BETA_FIRST = 0.9
BETA_SECOND = 0.999
EPSILON = 1e-6
WEIGHT_DECAY = 0.01
MAX_NORM = 1.0
FIRST_SCALE = 1.0 / (1.0 - BETA_FIRST ** STEP_NUMBER)
SECOND_SCALE = 1.0 / (1.0 - BETA_SECOND ** STEP_NUMBER)

MESH = pl.DeviceIdType.MESH
LANES = 128
TALL = 16
HALF = 64
FIRST = 32
VEC = 146
VEC_PAD = 256
ATTN_SHARD = 2048
MLP_SHARD = 8192
STEP = 1024
BLOCK = 512
MIB = 2 ** 20
ROWS = (HALF, 32, TALL, VEC)
LENGTHS = (16384, 65536, BLOCK, LANES)
SHARDS = ((HALF, ATTN_SHARD), (32, MLP_SHARD), (TALL, HALF), (TALL, VEC))
ATTN, MLP, SMALL = range(3)
HALVES = range(2)
SHAPES = ((32, ATTN_SHARD), (TALL, MLP_SHARD))
PEER, ALONG_X, ALONG_Y = 1, 2, 4
NEAR = ((ALONG_X, ALONG_Y), (ALONG_Y, ALONG_X))
FAR_FIRST = tuple(reversed(range(1, 8)))


def flip(index, mask):
    core, x, y = index % 2, (index // 2) % 2, index // 4
    if mask & PEER:
        core = 1 - core
    if mask & ALONG_X:
        x = 1 - x
    if mask & ALONG_Y:
        y = 1 - y
    return y * 4 + x * 2 + core


def aligned(index, size):
    return pl.ds(pl.multiple_of(index * size, size), size)


def moments(first, second, total, clip):
    clipped = clip * total
    new_first = BETA_FIRST * first + (1.0 - BETA_FIRST) * clipped
    new_second = BETA_SECOND * second + (1.0 - BETA_SECOND) * (clipped * clipped)
    return new_first, new_second


def direction(new_first, new_second, weight):
    return (new_first * FIRST_SCALE) / (jnp.sqrt(new_second * SECOND_SCALE) + EPSILON) + WEIGHT_DECAY * weight


def fold(square):
    rows, columns = square.shape
    parts = [square[r:r + 8, k:k + LANES] for r in range(0, rows, 8) for k in range(0, columns, LANES)]
    while len(parts) > 1:
        parts = [a + b for a, b in zip(parts[::2], parts[1::2])] + ([parts[-1]] if len(parts) % 2 else [])
    return parts[0]


def add_all(values):
    return functools.reduce(lambda a, b: a + b, values)


def kernel(*refs):
    grads, weights, firsts, seconds = refs[0:4], refs[4:8], refs[8:12], refs[12:16]
    replicas, new_weights, new_firsts, new_seconds = refs[16:20], refs[20:24], refs[24:28], refs[28:32]
    (recv_attn, recv_mlp, recv_wide, recv_vec, part_attn, part_mlp, part_wide, part_vec,
     last_attn, last_mlp, last_wide, last_vec, sum_attn, sum_mlp, sum_wide, sum_vec, dir_attn, dir_mlp,
     vec_in, vec_out, vec_rows, vec_columns, vec_row, all_wide, all_vec, start_tiles, first_tiles, rest_tiles, row_acc,
     load_sems, sent, tile_sent, scatter_recv, last_recv, tile_recv, own_recv, pass_recv, pair_recv) = refs[32:]
    me = lax.axis_index("data")
    core = me % 2

    def grad_chunk(half, owner, chunk):
        if chunk == MLP:
            return grads[1].at[pl.ds(TALL * half, TALL), aligned(owner, MLP_SHARD)]
        if chunk == ATTN:
            return grads[0].at[pl.ds(32 * half, 32), aligned(owner, ATTN_SHARD)]
        return vec_out.at[aligned(owner, TALL), :] if half else grads[2].at[:, aligned(owner // 2, LANES)]

    def recv_chunk(half, keep, slot, chunk):
        if chunk == SMALL:
            return (recv_vec if half else recv_wide).at[keep, slot]
        return (recv_attn, recv_mlp)[chunk].at[half, keep, slot]

    def sum_chunk(half, chunk, buffers):
        if chunk == SMALL:
            return buffers[3] if half else buffers[2]
        return buffers[chunk].at[half]

    parts, lasts = (part_attn, part_mlp, part_wide, part_vec), (last_attn, last_mlp, last_wide, last_vec)

    def replica_chunk(half, owner, chunk):
        if chunk == MLP:
            return replicas[1].at[pl.ds(TALL * half, TALL), aligned(owner, MLP_SHARD)]
        if chunk == ATTN:
            return replicas[0].at[pl.ds(32 * half, 32), aligned(owner, ATTN_SHARD)]
        return (all_vec if half else all_wide).at[owner]

    def send(source, target, send_sem, recv_sem, device):
        copy = pltpu.make_async_remote_copy(src_ref=source, dst_ref=target, send_sem=send_sem, recv_sem=recv_sem,
                                            device_id=(device,), device_id_type=MESH)
        copy.start()
        return copy

    def bank_of(half, chunk):
        return chunk + half if chunk == SMALL else chunk

    def wait_bytes(ref, sem):
        pltpu.make_async_copy(ref, ref, sem).wait()

    vec_load = pltpu.make_async_copy(grads[3], vec_in, load_sems.at[8])
    vec_load.start()
    for keep in range(2):
        for half in HALVES:
            for chunk in (MLP, ATTN, SMALL)[:3 - half]:
                owner = me if keep else flip(me, NEAR[half][1])
                pltpu.make_async_copy(grad_chunk(half, owner, chunk), recv_chunk(half, keep, 0, chunk),
                                      scatter_recv.at[half, keep, chunk]).start()
    small_loads = []
    for index, (source, target) in enumerate(((weights, new_weights), (firsts, new_firsts), (seconds, new_seconds))):
        for bank in range(4):
            copy = pltpu.make_async_copy(source[bank], target[bank], load_sems.at[bank if bank < 2 else 2 * index + bank])
            copy.start()
            if bank >= 2:
                small_loads.append(copy)

    barrier = pltpu.get_barrier_semaphore()
    near = (1, 2, 3, 4, 5)
    for mask in near:
        pl.semaphore_signal(barrier, inc=1, device_id=(flip(me, mask),), device_id_type=MESH)
    pl.semaphore_wait(barrier, len(near))

    def scatter(keep, chunk):
        for slot in range(3):
            for half in HALVES:
                target = flip(me, PEER) if slot == 0 else flip(me, NEAR[half][0]) // 2 * 2 + slot - 1
                owner = target if keep else flip(target, NEAR[half][1])
                index = 1 if slot == 0 else 2 + core
                send(grad_chunk(half, owner, chunk), recv_chunk(half, keep, index, chunk),
                     sent.at[0, bank_of(half, chunk)], scatter_recv.at[half, keep, chunk], target)

    scatter(0, MLP)
    scatter(0, ATTN)
    vec_load.wait()
    vec_rows[...] = jnp.zeros_like(vec_rows)
    vec_rows[0:VEC, :] = vec_in[...].astype(jnp.float32)
    vec_out[...] = vec_rows[...].T.astype(jnp.bfloat16)
    recv_vec[0, 0] = vec_out[aligned(flip(me, NEAR[1][1]), TALL), :]
    recv_vec[1, 0] = vec_out[aligned(me, TALL), :]
    scatter(0, SMALL)
    scatter(1, MLP)
    scatter(1, ATTN)
    scatter(1, SMALL)

    row = lax.broadcasted_iota(jnp.int32, (LANES, LANES), 0)
    lane = lax.broadcasted_iota(jnp.int32, (LANES, LANES), 1)
    eye = row == lane
    sub = lax.broadcasted_iota(jnp.int32, (8, LANES), 0)

    def lanes_of(first, last):
        column = jnp.sum(row_acc[first:last, :], axis=1, keepdims=True)
        return jnp.sum(jnp.where(eye[first:last, :], column, 0.0), axis=0, keepdims=True)

    def vec_lanes(square):
        vec_row[...] = jnp.zeros_like(vec_row)
        vec_row[0:1, 0:VEC] = jnp.sum(square, axis=0, keepdims=True)
        return vec_row[0:1, 0:LANES], vec_row[0:1, LANES:VEC_PAD]

    def tile_of(rows):
        tile = jnp.zeros((8, LANES), jnp.float32)
        for index, value in enumerate(rows):
            tile = jnp.where(sub == index, value, tile)
        return tile

    def exchange(tiles, which, value):
        tiles[me] = value
        for mask in FAR_FIRST:
            send(tiles.at[me], tiles.at[me], tile_sent.at[which], tile_recv.at[which], flip(me, mask))

    def collect(tiles, which):
        wait_bytes(tiles.at[pl.ds(0, len(FAR_FIRST))], tile_recv.at[which])
        return add_all([tiles[index] for index in range(8)])

    def by_rows(first, groups, columns, step):
        def group(g, carry):
            def inner(j, acc):
                return acc + step((aligned(g, 8), aligned(j, STEP)))

            row_acc[pl.ds(pl.multiple_of(first + g * 8, 8), 8), :] = lax.fori_loop(
                0, columns // STEP, inner, jnp.zeros((8, LANES), jnp.float32))
            return carry

        lax.fori_loop(0, groups, group, 0)

    def square_of(ref):
        return lambda place: fold(ref[place] * ref[place])

    for buffer, sem in ((recv_attn, load_sems.at[ATTN]), (recv_mlp, load_sems.at[MLP])):
        wait_bytes(buffer.at[:, :, pl.ds(0, 3)], sem)
    for copy in small_loads:
        copy.wait()
    row_acc[...] = jnp.zeros_like(row_acc)
    by_rows(0, 8, ATTN_SHARD, square_of(new_weights[0]))
    by_rows(HALF, 4, MLP_SHARD, square_of(new_weights[1]))
    wide_weight, vec_weight = new_weights[2][...], new_weights[3][...]
    row_acc[96:112, 0:HALF] = wide_weight * wide_weight
    weight_lanes = lanes_of(0, LANES)
    weight_low, weight_high = vec_lanes(vec_weight * vec_weight)

    def by_blocks(chunk, step, init):
        rows, columns = SHAPES[chunk]
        for r in range(0, rows, TALL):
            init = lax.fori_loop(0, columns // BLOCK, functools.partial(
                lambda first, j, carry: step((pl.ds(first, TALL), aligned(j, BLOCK)), carry), r), init)
        return init

    def gather_sum(half, keep, chunk):
        if chunk == SMALL:
            arrived = recv_vec.at[keep, pl.ds(1, 3)] if half else recv_wide.at[keep]
        else:
            arrived = (recv_attn, recv_mlp)[chunk].at[half, keep]
        wait_bytes(arrived, scatter_recv.at[half, keep, chunk])
        target = sum_chunk(half, chunk, (sum_attn, sum_mlp, sum_wide, sum_vec) if keep else parts)
        sources = [recv_chunk(half, keep, slot, chunk) for slot in range(4)]
        if chunk == SMALL:
            target[...] = add_all([source[...].astype(jnp.float32) for source in sources])
            return

        def step(place, carry):
            value = [source[place].astype(jnp.float32) for source in sources]
            target[place] = (value[0] + value[1]) + (value[2] + value[3])
            return carry

        by_blocks(chunk, step, 0)

    last = {}
    for chunk in (MLP, ATTN, SMALL):
        for half in HALVES:
            gather_sum(half, 0, chunk)
    for chunk in (SMALL, MLP, ATTN):
        for half in HALVES:
            last[half, chunk] = send(
                sum_chunk(half, chunk, parts), sum_chunk(half, chunk, lasts),
                sent.at[0, bank_of(half, chunk)], last_recv.at[half, chunk], flip(me, NEAR[half][1]))
    for chunk in (MLP, ATTN, SMALL):
        for half in HALVES:
            gather_sum(half, 1, chunk)

    for half in HALVES:
        last[half, SMALL].wait_recv()
    wide_total = sum_wide[...] + last_wide[...]
    wide_total = jnp.where(core == 0, wide_total[:, 0:HALF], wide_total[:, HALF:LANES])
    vec_total = (sum_vec[...] + last_vec[...])[:, 0:VEC]
    square = fold(jnp.concatenate([wide_total * wide_total, jnp.zeros((TALL, HALF), jnp.float32)], axis=1))
    low, high = vec_lanes(vec_total * vec_total)
    square = square + tile_of([low, high])
    for chunk in (MLP, ATTN):
        for half in HALVES:
            last[half, chunk].wait_recv()
            total, rest = sum_chunk(half, chunk, (sum_attn, sum_mlp)), sum_chunk(half, chunk, lasts)

            def step(place, acc):
                value = total[place] + rest[place]
                total[place] = value
                return acc + fold(value * value)

            square = by_blocks(chunk, step, square)

    exchange(start_tiles, 0, tile_of([weight_lanes, weight_low, weight_high, jnp.sum(square, axis=0, keepdims=True)]))
    start = collect(start_tiles, 0)
    square = jnp.sum(jnp.sum(start[3:4, :], axis=1, keepdims=True), axis=0, keepdims=True)
    clip = jnp.minimum(1.0, (8.0 * MAX_NORM) / jnp.sqrt(jnp.broadcast_to(square, (8, LANES)))) * 0.125
    clip_block = jnp.concatenate([clip] * (STEP // LANES), axis=1)
    weight_norms = LEARN_RATE * jnp.sqrt(start)

    sums, directions = (sum_attn, sum_mlp), (dir_attn, dir_mlp)

    def update(bank, half):
        rows = SHAPES[bank][0]

        def step(place):
            state = (pl.ds(pl.multiple_of(half * rows + place[0].start, 8), 8), place[1])
            new_first, new_second = moments(
                new_firsts[bank][state], new_seconds[bank][state], sums[bank].at[half][place], clip_block)
            value = direction(new_first, new_second, new_weights[bank][state])
            directions[bank].at[half][place] = value
            return fold(value * value)

        by_rows(HALF * bank + half * rows, rows // 8, SHAPES[bank][1], step)

    def store_moments(bank, half):
        rows = SHAPES[bank][0]

        def step(place, carry):
            state = (pl.ds(half * rows + place[0].start, TALL), place[1])
            clip_wide = jnp.concatenate([clip_block[:, 0:BLOCK]] * 2, axis=0)
            new_first, new_second = moments(
                new_firsts[bank][state], new_seconds[bank][state], sums[bank].at[half][place], clip_wide)
            new_firsts[bank][state] = new_first
            new_seconds[bank][state] = new_second
            return carry

        by_blocks(bank, step, 0)

    def update_small(bank, total, weight):
        new_first, new_second = moments(new_firsts[bank][...], new_seconds[bank][...], total, clip[0:1, 0:1])
        new_firsts[bank][...] = new_first
        new_seconds[bank][...] = new_second
        return direction(new_first, new_second, weight)

    update(ATTN, 0)
    exchange(first_tiles, 1, tile_of([lanes_of(0, FIRST)]))
    update(ATTN, 1)
    for half in HALVES:
        update(MLP, half)
    wide_dir = update_small(2, wide_total, wide_weight)
    vec_dir = update_small(3, vec_total, vec_weight)
    row_acc[96:112, 0:HALF] = wide_dir * wide_dir
    exchange(rest_tiles, 2, tile_of([lanes_of(FIRST, LANES), *vec_lanes(vec_dir * vec_dir)]))
    for bank in (ATTN, MLP):
        for half in HALVES:
            store_moments(bank, half)

    own_copies = {}

    def send_own(half, chunk, way):
        place = replica_chunk(half, me, chunk)
        bank = bank_of(half, chunk)
        recv_sem = own_recv.at[half, chunk, way - 1] if way else pair_recv.at[bank]
        own_copies[half, chunk, way] = send(place, place, sent.at[1, bank], recv_sem, flip(me, (PEER, ALONG_X, ALONG_Y)[way]))

    def spread_ratio(first, last, ratio):
        row_acc[first:last, :] = jnp.broadcast_to(
            jnp.sum(jnp.where(eye[first:last, :], ratio[0:1, :], 0.0), axis=1, keepdims=True), (last - first, LANES))

    def new_weight(bank, half, ways):
        rows, columns = SHAPES[bank]

        def step(place, carry):
            first = half * rows + place[0].start
            scale = jnp.concatenate([row_acc[HALF * bank + first:HALF * bank + first + TALL, :]] * (BLOCK // LANES), axis=1)
            state = (pl.ds(first, TALL), place[1])
            value = new_weights[bank][state] - scale * directions[bank].at[half][place]
            new_weights[bank][state] = value
            target = pl.ds(pl.multiple_of(me * columns + place[1].start, BLOCK), BLOCK)
            replicas[bank][pl.ds(first, TALL), target] = value.astype(jnp.bfloat16)
            return carry

        by_blocks(bank, step, 0)
        for way in ways:
            send_own(half, bank, way)

    spread_ratio(0, FIRST, weight_norms / jnp.sqrt(collect(first_tiles, 1)))
    new_weight(ATTN, 0, (1, 2, 0))
    ratio = weight_norms / jnp.sqrt(collect(rest_tiles, 2))
    spread_ratio(FIRST, LANES, ratio)
    new_weight(ATTN, 1, (2, 0))
    for half in HALVES:
        new_weight(MLP, half, (1 + half, 0))
    value = wide_weight - row_acc[96:112, 0:HALF] * wide_dir
    new_weights[2][...] = value
    all_wide[me] = jnp.concatenate([value, value], axis=1).astype(jnp.bfloat16)
    vec_row[0:1, 0:LANES] = ratio[1:2, :]
    vec_row[0:1, LANES:VEC_PAD] = ratio[2:3, :]
    value = vec_weight - vec_row[0:1, 0:VEC] * vec_dir
    new_weights[3][...] = value
    vec_columns[0:TALL, :] = jnp.zeros((TALL, VEC_PAD), jnp.float32)
    vec_columns[0:TALL, 0:VEC] = value
    all_vec[me] = vec_columns[0:TALL, :].astype(jnp.bfloat16)
    for half in HALVES:
        send_own(half, SMALL, 1 + half)
        send_own(half, SMALL, 0)
    send_own(1, ATTN, 1)
    for chunk in (MLP, SMALL):
        for half in HALVES:
            send_own(half, chunk, 2 - half)

    def send_pair(half, owner, chunk):
        place = replica_chunk(half, owner, chunk)
        bank = bank_of(half, chunk)
        send(place, place, sent.at[1, bank], pair_recv.at[bank], flip(me, PEER))

    passed = {}
    for chunk in (SMALL, MLP, ATTN):
        for half in HALVES:
            own_copies[half, chunk, 1 + half].wait_recv()
            owner = flip(me, NEAR[half][0])
            place = replica_chunk(half, owner, chunk)
            passed[half, chunk] = send(place, place, sent.at[1, bank_of(half, chunk)], pass_recv.at[half, chunk],
                                       flip(me, NEAR[half][1]))
            send_pair(half, owner, chunk)
    for chunk in (ATTN, MLP, SMALL):
        for half in HALVES:
            own_copies[half, chunk, 2 - half].wait_recv()
            send_pair(half, flip(me, NEAR[half][1]), chunk)
    for chunk in (SMALL, MLP, ATTN):
        for half in HALVES:
            passed[half, chunk].wait_recv()
            send_pair(half, flip(me, ALONG_X + ALONG_Y), chunk)
        if chunk == SMALL:
            for half, buffer in enumerate((all_wide, all_vec)):
                wait_bytes(buffer.at[pl.ds(0, 4)], pair_recv.at[SMALL + half])
            low_lanes = lax.broadcasted_iota(jnp.int32, (TALL, LANES), 1) < HALF
            for index in range(4):
                left, right = (all_wide[2 * index + k].astype(jnp.float32) for k in range(2))
                replicas[2][:, pl.ds(LANES * index, LANES)] = jnp.where(low_lanes, left, right).astype(jnp.bfloat16)
            for index in range(8):
                vec_columns[pl.ds(TALL * index, TALL), :] = all_vec[index].astype(jnp.float32)
            vec_rows[...] = vec_columns[...].T
            replicas[3][...] = vec_rows[0:VEC, :].astype(jnp.bfloat16)
    for bank in (ATTN, MLP):
        wait_bytes(replicas[bank].at[:, pl.ds(0, LENGTHS[bank] // 2)], pair_recv.at[bank])
        wait_bytes(replicas[bank], sent.at[0, bank])
        wait_bytes(replicas[bank].at[:, pl.ds(0, len(FAR_FIRST) * SHARDS[bank][1])], sent.at[1, bank])
    for half, buffer in enumerate((all_wide, all_vec)):
        wait_bytes(buffer, sent.at[0, SMALL + half])
        wait_bytes(buffer.at[pl.ds(0, len(FAR_FIRST))], sent.at[1, SMALL + half])
    for which, tiles in enumerate((start_tiles, first_tiles, rest_tiles)):
        wait_bytes(tiles.at[pl.ds(0, len(FAR_FIRST))], tile_sent.at[which])


def write_out(*refs):
    count = (len(refs) - 1) // 2
    copies = [pltpu.make_async_copy(refs[k], refs[count + k], refs[-1]) for k in range(count)]
    for copy in copies:
        copy.start()
    for copy in copies:
        copy.wait()


def solution(mesh):
    shards = [jax.ShapeDtypeStruct(shape, jnp.float32) for shape in SHARDS]
    shapes = [jax.ShapeDtypeStruct(shape, jnp.bfloat16) for shape in zip(ROWS, LENGTHS)] + shards * 3
    f32, bf16 = jnp.float32, jnp.bfloat16
    dma = pltpu.SemaphoreType.DMA
    attn, mlp = SHAPES

    def sums(*lead):
        return [pltpu.VMEM((*lead, *attn), f32), pltpu.VMEM((*lead, *mlp), f32)]

    small_sums = [pltpu.VMEM((TALL, LANES), f32), pltpu.VMEM((TALL, VEC_PAD), f32)]
    scratch = [
        pltpu.VMEM((2, 2, 4, *attn), bf16), pltpu.VMEM((2, 2, 4, *mlp), bf16),
        pltpu.VMEM((2, 4, TALL, LANES), bf16), pltpu.VMEM((2, 4, TALL, VEC_PAD), bf16),
        *sums(2), *small_sums, *sums(2), *small_sums, *sums(2), *small_sums, *sums(2),
        pltpu.VMEM((VEC, LANES), bf16), pltpu.VMEM((LANES, VEC_PAD), bf16),
        pltpu.VMEM((VEC_PAD, LANES), f32), pltpu.VMEM((LANES, VEC_PAD), f32), pltpu.VMEM((8, VEC_PAD), f32),
        pltpu.VMEM((8, TALL, LANES), bf16), pltpu.VMEM((8, TALL, VEC_PAD), bf16),
        *[pltpu.VMEM((8, 8, LANES), f32)] * 3, pltpu.VMEM((LANES, LANES), f32),
        dma((9,)), dma((2, 4)), dma((3,)), dma((2, 2, 3)), dma((2, 3)), dma((3,)), dma((2, 3, 2)), dma((2, 3)), dma((4,)),
    ]
    count = len(shapes)
    anywhere = [pl.BlockSpec(memory_space=pl.ANY)] * count
    step = pl.pallas_call(
        kernel,
        out_shape=[pltpu.VMEM(shape.shape, shape.dtype) for shape in shapes],
        in_specs=anywhere,
        out_specs=[pl.BlockSpec(memory_space=pltpu.VMEM)] * count,
        scratch_shapes=scratch,
        compiler_params=pltpu.CompilerParams(collective_id=0, has_side_effects=True, vmem_limit_bytes=36 * MIB),
        name="lamb_step",
    )
    finish = pl.pallas_call(
        write_out,
        out_shape=shapes,
        in_specs=anywhere,
        out_specs=anywhere,
        scratch_shapes=[dma],
        compiler_params=pltpu.CompilerParams(vmem_limit_bytes=MIB),
        name="write_out",
    )

    def local_step(*banks):
        banks = [bank[0] for bank in banks[:4]] + [bank.T if bank.shape == (VEC, TALL) else bank for bank in banks[4:]]
        banks = [pltpu.with_memory_space_constraint(bank, pltpu.HBM) for bank in banks]
        results = finish(*step(*banks))
        return tuple(value.T if value.shape == (TALL, VEC) else value for value in results)

    grad_spec, shard_spec, full_spec = P("data", None, None), P(None, "data"), P(None, None)
    return jax.shard_map(local_step, mesh=mesh, in_specs=(grad_spec,) * 4 + (shard_spec,) * 12,
                         out_specs=(full_spec,) * 4 + (shard_spec,) * 12, check_vma=False)
```

```python
import functools

import jax
import jax.numpy as jnp
from jax import lax
from jax.experimental import pallas as pl
from jax.experimental.pallas import tpu as pltpu
from jax.sharding import PartitionSpec as P

STEP_NUMBER = 10
LEARN_RATE = 0.04
BETA_FIRST = 0.9
BETA_SECOND = 0.999
EPSILON = 1e-6
WEIGHT_DECAY = 0.01
MAX_NORM = 1.0
FIRST_SCALE = 1.0 / (1.0 - BETA_FIRST ** STEP_NUMBER)
SECOND_SCALE = 1.0 / (1.0 - BETA_SECOND ** STEP_NUMBER)

MESH = pl.DeviceIdType.MESH
LANES = 128
TALL = 16
HALF = 64
FIRST = 32
VEC = 146
VEC_PAD = 256
ATTN_SHARD = 2048
MLP_SHARD = 8192
STEP = 1024
BLOCK = 512
MIB = 2 ** 20
ROWS = (HALF, 32, TALL, VEC)
LENGTHS = (16384, 65536, BLOCK, LANES)
SHARDS = ((HALF, ATTN_SHARD), (32, MLP_SHARD), (TALL, HALF), (TALL, VEC))
ATTN, MLP, SMALL = range(3)
BIG = (ATTN, MLP)
HALVES = range(2)
SHAPES = ((32, ATTN_SHARD), (TALL, MLP_SHARD))
PEER, ALONG_X, ALONG_Y = 1, 2, 4
NEAR = ((ALONG_X, ALONG_Y), (ALONG_Y, ALONG_X))
WIDE_LANES = (LANES, LANES + HALF)
FAR_FIRST = tuple(reversed(range(1, 8)))


def flip(index, mask):
    core, x, y = index % 2, (index // 2) % 2, index // 4
    if mask & PEER:
        core = 1 - core
    if mask & ALONG_X:
        x = 1 - x
    if mask & ALONG_Y:
        y = 1 - y
    return y * 4 + x * 2 + core


def aligned(index, size):
    return pl.ds(pl.multiple_of(index * size, size), size)


def moments(first, second, total, clip):
    clipped = clip * total
    new_first = BETA_FIRST * first + (1.0 - BETA_FIRST) * clipped
    new_second = BETA_SECOND * second + (1.0 - BETA_SECOND) * (clipped * clipped)
    return new_first, new_second


def direction(new_first, new_second, weight):
    return (new_first * FIRST_SCALE) / (jnp.sqrt(new_second * SECOND_SCALE) + EPSILON) + WEIGHT_DECAY * weight


def fold(square):
    rows, columns = square.shape
    parts = [square[r:r + 8, k:k + LANES] for r in range(0, rows, 8) for k in range(0, columns, LANES)]
    while len(parts) > 1:
        parts = [a + b for a, b in zip(parts[::2], parts[1::2])] + ([parts[-1]] if len(parts) % 2 else [])
    return parts[0]


def add_all(values):
    return functools.reduce(lambda a, b: a + b, values)


def kernel(*refs):
    grads, weights, firsts, seconds = refs[0:4], refs[4:8], refs[8:12], refs[12:16]
    replicas, new_weights, new_firsts, new_seconds = refs[16:20], refs[20:24], refs[24:28], refs[28:32]
    (recv_attn, recv_mlp, recv_small, part_attn, part_mlp, part_small, last_attn, last_mlp, last_small,
     sum_attn, sum_mlp, sum_small, dir_attn, dir_mlp, vec_in, wide_in, small_out, all_small,
     vec_rows, vec_columns, vec_row, start_tiles, first_tiles, rest_tiles, row_acc,
     load_sems, sent, tile_sent, scatter_recv, small_recv, last_recv, tile_recv, own_recv, pass_recv, pair_recv) = refs[32:]
    recvs, parts, lasts = (recv_attn, recv_mlp), (part_attn, part_mlp), (last_attn, last_mlp)
    me = lax.axis_index("data")
    core = me % 2

    def grad_chunk(half, owner, chunk):
        rows, columns = SHAPES[chunk]
        return grads[chunk].at[pl.ds(rows * half, rows), aligned(owner, columns)]

    def replica_chunk(half, owner, chunk):
        rows, columns = SHAPES[chunk]
        return replicas[chunk].at[pl.ds(rows * half, rows), aligned(owner, columns)]

    along_x, along_y = flip(me, ALONG_X), flip(me, ALONG_Y)
    small_near = (along_x * (1 - core) + along_y * core, along_y * (1 - core) + along_x * core)
    peer = flip(me, PEER)
    peer_next = flip(peer, ALONG_X) * (1 - core) + flip(peer, ALONG_Y) * core

    def send(source, target, send_sem, recv_sem, device):
        copy = pltpu.make_async_remote_copy(src_ref=source, dst_ref=target, send_sem=send_sem, recv_sem=recv_sem,
                                            device_id=(device,), device_id_type=MESH)
        copy.start()
        return copy

    def wait_bytes(ref, sem):
        pltpu.make_async_copy(ref, ref, sem).wait()

    barrier = pltpu.get_barrier_semaphore()
    near = (1, 2, 3, 4, 5)
    for mask in near:
        pl.semaphore_signal(barrier, inc=1, device_id=(flip(me, mask),), device_id_type=MESH)

    small_loads = [pltpu.make_async_copy(grads[2], wide_in, load_sems.at[2]),
                   pltpu.make_async_copy(grads[3], vec_in, load_sems.at[3])]
    for copy in small_loads:
        copy.start()
    for keep in range(2):
        for half in HALVES:
            for chunk in (MLP, ATTN):
                owner = me if keep else flip(me, NEAR[half][1])
                pltpu.make_async_copy(grad_chunk(half, owner, chunk), recvs[chunk].at[half, keep, 0],
                                      scatter_recv.at[half, keep, chunk]).start()
    state_loads = []
    for index, (source, target) in enumerate(((weights, new_weights), (firsts, new_firsts), (seconds, new_seconds))):
        for bank in range(4):
            copy = pltpu.make_async_copy(source[bank], target[bank], load_sems.at[bank if bank < 2 else 2 * index + bank + 2])
            copy.start()
            if bank >= 2:
                state_loads.append(copy)
    pl.semaphore_wait(barrier, len(near))

    def scatter(keep, chunk):
        for slot in (1, 2, 0):
            for half in HALVES:
                target = peer if slot == 0 else flip(me, NEAR[half][0]) // 2 * 2 + slot - 1
                owner = target if keep else flip(target, NEAR[half][1])
                send(grad_chunk(half, owner, chunk), recvs[chunk].at[half, keep, 1 if slot == 0 else 2 + core],
                     sent.at[0, chunk], scatter_recv.at[half, keep, chunk], target)

    scatter(0, MLP)
    scatter(0, ATTN)
    for copy in small_loads:
        copy.wait()
    vec_rows[...] = jnp.zeros_like(vec_rows)
    vec_rows[0:VEC, :] = vec_in[...].astype(jnp.float32)
    vec_columns[...] = vec_rows[...].T

    def small_message(wide, vec):
        pad = jnp.zeros((TALL, VEC_PAD - VEC - HALF), jnp.float32)
        return jnp.concatenate([vec[:, 0:LANES], wide, vec[:, LANES:VEC], pad], axis=1).astype(jnp.bfloat16)

    def small_parts(message):
        vec = jnp.concatenate([message[:, 0:LANES], message[:, WIDE_LANES[1]:HALF + VEC]], axis=1)
        return message[:, slice(*WIDE_LANES)], vec

    wide_grad = wide_in[...].astype(jnp.float32)
    for owner in range(8):
        small_out[owner] = small_message(
            wide_grad[:, HALF * owner:HALF * owner + HALF], vec_columns[TALL * owner:TALL * owner + TALL, 0:VEC])
    for keep in range(2):
        recv_small[keep, 0] = small_out[me if keep else small_near[1]]
        places = [(along_x // 2 * 2, ALONG_Y), (along_y // 2 * 2 + 1, ALONG_X)]
        targets = [(target, target if keep else flip(target, way), 2 + core) for target, way in places]
        for target, owner, slot in [*targets, (peer, peer if keep else peer_next, 1)]:
            send(small_out.at[owner], recv_small.at[keep, slot], sent.at[0, SMALL], small_recv.at[keep], target)
    scatter(1, MLP)
    scatter(1, ATTN)

    row = lax.broadcasted_iota(jnp.int32, (LANES, LANES), 0)
    lane = lax.broadcasted_iota(jnp.int32, (LANES, LANES), 1)
    eye = row == lane
    sub = lax.broadcasted_iota(jnp.int32, (8, LANES), 0)

    def lanes_of(first, last):
        column = jnp.sum(row_acc[first:last, :], axis=1, keepdims=True)
        return jnp.sum(jnp.where(eye[first:last, :], column, 0.0), axis=0, keepdims=True)

    def vec_lanes(square):
        vec_row[...] = jnp.zeros_like(vec_row)
        vec_row[0:1, 0:VEC] = jnp.sum(square, axis=0, keepdims=True)
        return vec_row[0:1, 0:LANES], vec_row[0:1, LANES:VEC_PAD]

    def tile_of(rows):
        tile = jnp.zeros((8, LANES), jnp.float32)
        for index, value in enumerate(rows):
            tile = jnp.where(sub == index, value, tile)
        return tile

    def exchange(tiles, which, value):
        tiles[me] = value
        for mask in FAR_FIRST:
            send(tiles.at[me], tiles.at[me], tile_sent.at[which], tile_recv.at[which], flip(me, mask))

    def collect(tiles, which):
        wait_bytes(tiles.at[pl.ds(0, len(FAR_FIRST))], tile_recv.at[which])
        return add_all([tiles[index] for index in range(8)])

    def by_rows(first, groups, columns, step):
        def group(g, carry):
            def inner(j, acc):
                return acc + step((aligned(g, 8), aligned(j, STEP)))

            row_acc[pl.ds(pl.multiple_of(first + g * 8, 8), 8), :] = lax.fori_loop(
                0, columns // STEP, inner, jnp.zeros((8, LANES), jnp.float32))
            return carry

        lax.fori_loop(0, groups, group, 0)

    def square_of(ref):
        return lambda place: fold(ref[place] * ref[place])

    for buffer, sem in ((recv_attn, load_sems.at[ATTN]), (recv_mlp, load_sems.at[MLP])):
        wait_bytes(buffer.at[:, :, pl.ds(0, 3)], sem)
    for copy in state_loads:
        copy.wait()
    row_acc[...] = jnp.zeros_like(row_acc)
    by_rows(0, 8, ATTN_SHARD, square_of(new_weights[0]))
    by_rows(HALF, 4, MLP_SHARD, square_of(new_weights[1]))
    wide_weight, vec_weight = new_weights[2][...], new_weights[3][...]
    row_acc[96:112, 0:HALF] = wide_weight * wide_weight
    weight_lanes = lanes_of(0, LANES)
    weight_low, weight_high = vec_lanes(vec_weight * vec_weight)

    def by_blocks(chunk, step, init):
        rows, columns = SHAPES[chunk]
        for r in range(0, rows, TALL):
            init = lax.fori_loop(0, columns // BLOCK, functools.partial(
                lambda first, j, carry: step((pl.ds(first, TALL), aligned(j, BLOCK)), carry), r), init)
        return init

    def gather_sum(half, keep, chunk):
        source, target = recvs[chunk].at[half, keep], ((sum_attn, sum_mlp) if keep else parts)[chunk].at[half]
        wait_bytes(source, scatter_recv.at[half, keep, chunk])

        def step(place, carry):
            value = [source[(slot, *place)].astype(jnp.float32) for slot in range(4)]
            target[place] = (value[0] + value[1]) + (value[2] + value[3])
            return carry

        by_blocks(chunk, step, 0)

    def gather_small(keep, target):
        wait_bytes(recv_small.at[keep, pl.ds(1, 3)], small_recv.at[keep])
        target[...] = add_all([recv_small[keep, slot].astype(jnp.float32) for slot in range(4)])

    last = {}
    for chunk in (MLP, ATTN):
        for half in HALVES:
            gather_sum(half, 0, chunk)
    gather_small(0, part_small)
    last_small_copy = send(part_small, last_small, sent.at[0, SMALL], last_recv.at[0, SMALL], small_near[1])
    for chunk in (MLP, ATTN):
        for half in HALVES:
            last[half, chunk] = send(parts[chunk].at[half], lasts[chunk].at[half], sent.at[0, chunk],
                                     last_recv.at[half, chunk], flip(me, NEAR[half][1]))
    for chunk in (MLP, ATTN):
        for half in HALVES:
            gather_sum(half, 1, chunk)
    gather_small(1, sum_small)

    last_small_copy.wait_recv()
    wide_total, vec_total = small_parts(sum_small[...] + last_small[...])
    square = fold(jnp.concatenate([wide_total * wide_total, jnp.zeros((TALL, HALF), jnp.float32)], axis=1))
    low, high = vec_lanes(vec_total * vec_total)
    square = square + tile_of([low, high])
    for chunk in (MLP, ATTN):
        for half in HALVES:
            last[half, chunk].wait_recv()
            total, rest = (sum_attn, sum_mlp)[chunk].at[half], lasts[chunk].at[half]

            def step(place, acc):
                value = total[place] + rest[place]
                total[place] = value
                return acc + fold(value * value)

            square = by_blocks(chunk, step, square)

    exchange(start_tiles, 0, tile_of([weight_lanes, weight_low, weight_high, jnp.sum(square, axis=0, keepdims=True)]))
    start = collect(start_tiles, 0)
    square = jnp.sum(jnp.sum(start[3:4, :], axis=1, keepdims=True), axis=0, keepdims=True)
    clip = jnp.minimum(1.0, (8.0 * MAX_NORM) / jnp.sqrt(jnp.broadcast_to(square, (8, LANES)))) * 0.125
    clip_block = jnp.concatenate([clip] * (STEP // LANES), axis=1)
    weight_norms = LEARN_RATE * jnp.sqrt(start)

    sums, directions = (sum_attn, sum_mlp), (dir_attn, dir_mlp)

    def update(bank, half):
        rows = SHAPES[bank][0]

        def step(place):
            state = (pl.ds(pl.multiple_of(half * rows + place[0].start, 8), 8), place[1])
            new_first, new_second = moments(
                new_firsts[bank][state], new_seconds[bank][state], sums[bank].at[half][place], clip_block)
            value = direction(new_first, new_second, new_weights[bank][state])
            directions[bank].at[half][place] = value
            return fold(value * value)

        by_rows(HALF * bank + half * rows, rows // 8, SHAPES[bank][1], step)

    def store_moments(bank, half):
        rows = SHAPES[bank][0]

        def step(place, carry):
            state = (pl.ds(half * rows + place[0].start, TALL), place[1])
            clip_wide = jnp.concatenate([clip_block[:, 0:BLOCK]] * 2, axis=0)
            new_first, new_second = moments(
                new_firsts[bank][state], new_seconds[bank][state], sums[bank].at[half][place], clip_wide)
            new_firsts[bank][state] = new_first
            new_seconds[bank][state] = new_second
            return carry

        by_blocks(bank, step, 0)

    def update_small(bank, total, weight):
        new_first, new_second = moments(new_firsts[bank][...], new_seconds[bank][...], total, clip[0:1, 0:1])
        new_firsts[bank][...] = new_first
        new_seconds[bank][...] = new_second
        return direction(new_first, new_second, weight)

    update(ATTN, 0)
    exchange(first_tiles, 1, tile_of([lanes_of(0, FIRST)]))
    update(ATTN, 1)
    for half in HALVES:
        update(MLP, half)
    wide_dir = update_small(2, wide_total, wide_weight)
    vec_dir = update_small(3, vec_total, vec_weight)
    row_acc[96:112, 0:HALF] = wide_dir * wide_dir
    exchange(rest_tiles, 2, tile_of([lanes_of(FIRST, LANES), *vec_lanes(vec_dir * vec_dir)]))
    for bank in (ATTN, MLP):
        for half in HALVES:
            store_moments(bank, half)

    own_copies = {}

    def send_own(half, chunk, way):
        place = all_small.at[me] if chunk == SMALL else replica_chunk(half, me, chunk)
        recv_sem = own_recv.at[half, chunk, way - 1] if way else pair_recv.at[chunk]
        own_copies[half, chunk, way] = send(place, place, sent.at[1, chunk], recv_sem, flip(me, (PEER, ALONG_X, ALONG_Y)[way]))

    def spread_ratio(first, last, ratio):
        row_acc[first:last, :] = jnp.broadcast_to(
            jnp.sum(jnp.where(eye[first:last, :], ratio[0:1, :], 0.0), axis=1, keepdims=True), (last - first, LANES))

    def new_weight(bank, half, ways):
        rows, columns = SHAPES[bank]

        def step(place, carry):
            first = half * rows + place[0].start
            scale = jnp.concatenate([row_acc[HALF * bank + first:HALF * bank + first + TALL, :]] * (BLOCK // LANES), axis=1)
            state = (pl.ds(first, TALL), place[1])
            value = new_weights[bank][state] - scale * directions[bank].at[half][place]
            new_weights[bank][state] = value
            target = pl.ds(pl.multiple_of(me * columns + place[1].start, BLOCK), BLOCK)
            replicas[bank][pl.ds(first, TALL), target] = value.astype(jnp.bfloat16)
            return carry

        by_blocks(bank, step, 0)
        for way in ways:
            send_own(half, bank, way)

    spread_ratio(0, FIRST, weight_norms / jnp.sqrt(collect(first_tiles, 1)))
    new_weight(ATTN, 0, (1, 2, 0))
    ratio = weight_norms / jnp.sqrt(collect(rest_tiles, 2))
    spread_ratio(FIRST, LANES, ratio)
    new_weight(ATTN, 1, (2, 0))
    for half in HALVES:
        new_weight(MLP, half, (1 + half, 0))
    value = wide_weight - row_acc[96:112, 0:HALF] * wide_dir
    new_weights[2][...] = value
    wide_value = value
    vec_row[0:1, 0:LANES] = ratio[1:2, :]
    vec_row[0:1, LANES:VEC_PAD] = ratio[2:3, :]
    value = vec_weight - vec_row[0:1, 0:VEC] * vec_dir
    new_weights[3][...] = value
    all_small[me] = small_message(wide_value, value)
    for way in (1, 2, 0):
        send_own(0, SMALL, way)
    send_own(1, ATTN, 1)
    for half in HALVES:
        send_own(half, MLP, 2 - half)

    def send_pair(place, chunk):
        send(place, place, sent.at[1, chunk], pair_recv.at[chunk], peer)

    for way in (1, 2):
        own_copies[0, SMALL, way].wait_recv()
    place = all_small.at[small_near[0]]
    passed_small = send(place, place, sent.at[1, SMALL], pass_recv.at[0, SMALL], small_near[1])
    for owner in small_near:
        send_pair(all_small.at[owner], SMALL)
    passed = {}
    for chunk in (MLP, ATTN):
        for half in HALVES:
            own_copies[half, chunk, 1 + half].wait_recv()
            place = replica_chunk(half, flip(me, NEAR[half][0]), chunk)
            passed[half, chunk] = send(place, place, sent.at[1, chunk], pass_recv.at[half, chunk], flip(me, NEAR[half][1]))
            send_pair(place, chunk)
    for chunk in BIG:
        for half in HALVES:
            own_copies[half, chunk, 2 - half].wait_recv()
            send_pair(replica_chunk(half, flip(me, NEAR[half][1]), chunk), chunk)
    far = flip(me, ALONG_X + ALONG_Y)
    passed_small.wait_recv()
    send_pair(all_small.at[far], SMALL)
    wait_bytes(all_small.at[pl.ds(0, 4)], pair_recv.at[SMALL])
    wides, vecs = zip(*(small_parts(all_small[owner].astype(jnp.float32)) for owner in range(8)))
    replicas[2][...] = jnp.concatenate(wides, axis=1).astype(jnp.bfloat16)
    for owner in range(8):
        vec_columns[TALL * owner:TALL * owner + TALL, 0:VEC] = vecs[owner]
    vec_rows[...] = vec_columns[...].T
    replicas[3][...] = vec_rows[0:VEC, :].astype(jnp.bfloat16)
    for chunk in (MLP, ATTN):
        for half in HALVES:
            passed[half, chunk].wait_recv()
            send_pair(replica_chunk(half, far, chunk), chunk)
    for bank in (ATTN, MLP):
        wait_bytes(replicas[bank].at[:, pl.ds(0, LENGTHS[bank] // 2)], pair_recv.at[bank])
        wait_bytes(replicas[bank], sent.at[0, bank])
        wait_bytes(replicas[bank].at[:, pl.ds(0, len(FAR_FIRST) * SHARDS[bank][1])], sent.at[1, bank])
    wait_bytes(all_small, sent.at[0, SMALL])
    wait_bytes(all_small.at[pl.ds(0, len(FAR_FIRST))], sent.at[1, SMALL])
    for which, tiles in enumerate((start_tiles, first_tiles, rest_tiles)):
        wait_bytes(tiles.at[pl.ds(0, len(FAR_FIRST))], tile_sent.at[which])


def write_out(*refs):
    count = (len(refs) - 1) // 2
    copies = [pltpu.make_async_copy(refs[k], refs[count + k], refs[-1]) for k in range(count)]
    for copy in copies:
        copy.start()
    for copy in copies:
        copy.wait()


def solution(mesh):
    shards = [jax.ShapeDtypeStruct(shape, jnp.float32) for shape in SHARDS]
    shapes = [jax.ShapeDtypeStruct(shape, jnp.bfloat16) for shape in zip(ROWS, LENGTHS)] + shards * 3
    f32, bf16 = jnp.float32, jnp.bfloat16
    dma = pltpu.SemaphoreType.DMA
    attn, mlp = SHAPES

    def sums(*lead):
        return [pltpu.VMEM((*lead, *attn), f32), pltpu.VMEM((*lead, *mlp), f32)]

    small = (TALL, VEC_PAD)
    scratch = [
        pltpu.VMEM((2, 2, 4, *attn), bf16), pltpu.VMEM((2, 2, 4, *mlp), bf16), pltpu.VMEM((2, 4, *small), bf16),
        *sums(2), pltpu.VMEM(small, f32), *sums(2), pltpu.VMEM(small, f32), *sums(2), pltpu.VMEM(small, f32), *sums(2),
        pltpu.VMEM((VEC, LANES), bf16), pltpu.VMEM((TALL, BLOCK), bf16), pltpu.VMEM((8, *small), bf16),
        pltpu.VMEM((8, *small), bf16),
        pltpu.VMEM((VEC_PAD, LANES), f32), pltpu.VMEM((LANES, VEC_PAD), f32), pltpu.VMEM((8, VEC_PAD), f32),
        *[pltpu.VMEM((8, 8, LANES), f32)] * 3, pltpu.VMEM((LANES, LANES), f32),
        dma((10,)), dma((2, 3)), dma((3,)), dma((2, 2, 2)), dma((2,)), dma((2, 3)), dma((3,)), dma((2, 3, 2)), dma((2, 3)),
        dma((3,)),
    ]
    count = len(shapes)
    anywhere = [pl.BlockSpec(memory_space=pl.ANY)] * count
    step = pl.pallas_call(
        kernel,
        out_shape=[pltpu.VMEM(shape.shape, shape.dtype) for shape in shapes],
        in_specs=anywhere,
        out_specs=[pl.BlockSpec(memory_space=pltpu.VMEM)] * count,
        scratch_shapes=scratch,
        compiler_params=pltpu.CompilerParams(collective_id=0, has_side_effects=True, vmem_limit_bytes=36 * MIB),
        name="lamb_step",
    )
    finish = pl.pallas_call(
        write_out,
        out_shape=shapes,
        in_specs=anywhere,
        out_specs=anywhere,
        scratch_shapes=[dma],
        compiler_params=pltpu.CompilerParams(vmem_limit_bytes=MIB),
        name="write_out",
    )

    def local_step(*banks):
        banks = [bank[0] for bank in banks[:4]] + [bank.T if bank.shape == (VEC, TALL) else bank for bank in banks[4:]]
        banks = [pltpu.with_memory_space_constraint(bank, pltpu.HBM) for bank in banks]
        results = finish(*step(*banks))
        return tuple(value.T if value.shape == (TALL, VEC) else value for value in results)

    grad_spec, shard_spec, full_spec = P("data", None, None), P(None, "data"), P(None, None)
    return jax.shard_map(local_step, mesh=mesh, in_specs=(grad_spec,) * 4 + (shard_spec,) * 12,
                         out_specs=(full_spec,) * 4 + (shard_spec,) * 12, check_vma=False)
```

```python
import functools

import jax
import jax.numpy as jnp
from jax import lax
from jax.experimental import pallas as pl
from jax.experimental.pallas import tpu as pltpu
from jax.sharding import PartitionSpec as P

STEP_NUMBER = 10
LEARN_RATE = 0.04
BETA_FIRST = 0.9
BETA_SECOND = 0.999
EPSILON = 1e-6
WEIGHT_DECAY = 0.01
MAX_NORM = 1.0
FIRST_SCALE = 1.0 / (1.0 - BETA_FIRST ** STEP_NUMBER)
SECOND_SCALE = 1.0 / (1.0 - BETA_SECOND ** STEP_NUMBER)

MESH = pl.DeviceIdType.MESH
LANES = 128
TALL = 16
HALF = 64
FIRST = 32
EARLY = 1024
VEC = 146
VEC_PAD = 256
ATTN_SHARD = 2048
MLP_SHARD = 8192
STEP = 1024
BLOCK = 512
MIB = 2 ** 20
ROWS = (HALF, 32, TALL, VEC)
LENGTHS = (16384, 65536, BLOCK, LANES)
SHARDS = ((HALF, ATTN_SHARD), (32, MLP_SHARD), (TALL, HALF), (TALL, VEC))
ATTN, MLP, SMALL = range(3)
BIG = (ATTN, MLP)
HALVES = range(2)
SHAPES = ((32, ATTN_SHARD), (TALL, MLP_SHARD))
PEER, ALONG_X, ALONG_Y = 1, 2, 4
NEAR = ((ALONG_X, ALONG_Y), (ALONG_Y, ALONG_X))
WIDE_LANES = (LANES, LANES + HALF)
FAR_FIRST = tuple(reversed(range(1, 8)))


def flip(index, mask):
    core, x, y = index % 2, (index // 2) % 2, index // 4
    if mask & PEER:
        core = 1 - core
    if mask & ALONG_X:
        x = 1 - x
    if mask & ALONG_Y:
        y = 1 - y
    return y * 4 + x * 2 + core


def aligned(index, size):
    return pl.ds(pl.multiple_of(index * size, size), size)


def moments(first, second, total, clip):
    clipped = clip * total
    new_first = BETA_FIRST * first + (1.0 - BETA_FIRST) * clipped
    new_second = BETA_SECOND * second + (1.0 - BETA_SECOND) * (clipped * clipped)
    return new_first, new_second


def direction(new_first, new_second, weight):
    return (new_first * FIRST_SCALE) / (jnp.sqrt(new_second * SECOND_SCALE) + EPSILON) + WEIGHT_DECAY * weight


def fold(square):
    rows, columns = square.shape
    parts = [square[r:r + 8, k:k + LANES] for r in range(0, rows, 8) for k in range(0, columns, LANES)]
    while len(parts) > 1:
        parts = [a + b for a, b in zip(parts[::2], parts[1::2])] + ([parts[-1]] if len(parts) % 2 else [])
    return parts[0]


def add_all(values):
    return functools.reduce(lambda a, b: a + b, values)


def kernel(*refs):
    grads, weights, firsts, seconds = refs[0:4], refs[4:8], refs[8:12], refs[12:16]
    replicas, new_weights, new_firsts, new_seconds = refs[16:20], refs[20:24], refs[24:28], refs[28:32]
    (recv_attn, recv_mlp, recv_small, part_attn, part_mlp, part_small, last_attn, last_mlp, last_small,
     sum_attn, sum_mlp, sum_small, dir_attn, dir_mlp, early_weight, early_dir, vec_in, wide_in, small_out, all_small,
     vec_rows, vec_columns, vec_row, start_tiles, first_tiles, rest_tiles, row_acc,
     load_sems, sent, tile_sent, scatter_recv, small_recv, last_recv, tile_recv, own_recv, pass_recv, pair_recv,
     early_sent, early_recv) = refs[32:]
    recvs, parts, lasts = (recv_attn, recv_mlp), (part_attn, part_mlp), (last_attn, last_mlp)
    me = lax.axis_index("data")
    core = me % 2

    def grad_chunk(half, owner, chunk):
        rows, columns = SHAPES[chunk]
        return grads[chunk].at[pl.ds(rows * half, rows), aligned(owner, columns)]

    def replica_chunk(half, owner, chunk):
        rows, columns = SHAPES[chunk]
        return replicas[chunk].at[pl.ds(rows * half, rows), aligned(owner, columns)]

    along_x, along_y = flip(me, ALONG_X), flip(me, ALONG_Y)
    small_near = (along_x * (1 - core) + along_y * core, along_y * (1 - core) + along_x * core)
    peer = flip(me, PEER)
    peer_next = flip(peer, ALONG_X) * (1 - core) + flip(peer, ALONG_Y) * core

    def send(source, target, send_sem, recv_sem, device):
        copy = pltpu.make_async_remote_copy(src_ref=source, dst_ref=target, send_sem=send_sem, recv_sem=recv_sem,
                                            device_id=(device,), device_id_type=MESH)
        copy.start()
        return copy

    def wait_bytes(ref, sem):
        pltpu.make_async_copy(ref, ref, sem).wait()

    barrier = pltpu.get_barrier_semaphore()
    near = (1, 2, 3, 4, 5)
    for mask in near:
        pl.semaphore_signal(barrier, inc=1, device_id=(flip(me, mask),), device_id_type=MESH)

    small_loads = [pltpu.make_async_copy(grads[2], wide_in, load_sems.at[2]),
                   pltpu.make_async_copy(grads[3], vec_in, load_sems.at[3])]
    for copy in small_loads:
        copy.start()
    for keep in range(2):
        for half in HALVES:
            for chunk in (MLP, ATTN):
                owner = me if keep else flip(me, NEAR[half][1])
                pltpu.make_async_copy(grad_chunk(half, owner, chunk), recvs[chunk].at[half, keep, 0],
                                      scatter_recv.at[half, keep, chunk]).start()
    state_loads = []
    for index, (source, target) in enumerate(((weights, new_weights), (firsts, new_firsts), (seconds, new_seconds))):
        for bank in range(4):
            copy = pltpu.make_async_copy(source[bank], target[bank], load_sems.at[bank if bank < 2 else 2 * index + bank + 2])
            copy.start()
            if bank >= 2:
                state_loads.append(copy)
    pl.semaphore_wait(barrier, len(near))

    def scatter(keep, chunk):
        for slot in (1, 2, 0):
            for half in HALVES:
                target = peer if slot == 0 else flip(me, NEAR[half][0]) // 2 * 2 + slot - 1
                owner = target if keep else flip(target, NEAR[half][1])
                send(grad_chunk(half, owner, chunk), recvs[chunk].at[half, keep, 1 if slot == 0 else 2 + core],
                     sent.at[0, chunk], scatter_recv.at[half, keep, chunk], target)

    scatter(0, MLP)
    scatter(0, ATTN)
    for copy in small_loads:
        copy.wait()
    vec_rows[...] = jnp.zeros_like(vec_rows)
    vec_rows[0:VEC, :] = vec_in[...].astype(jnp.float32)
    vec_columns[...] = vec_rows[...].T

    def small_message(wide, vec):
        pad = jnp.zeros((TALL, VEC_PAD - VEC - HALF), jnp.float32)
        return jnp.concatenate([vec[:, 0:LANES], wide, vec[:, LANES:VEC], pad], axis=1).astype(jnp.bfloat16)

    def small_parts(message):
        vec = jnp.concatenate([message[:, 0:LANES], message[:, WIDE_LANES[1]:HALF + VEC]], axis=1)
        return message[:, slice(*WIDE_LANES)], vec

    wide_grad = wide_in[...].astype(jnp.float32)
    for owner in range(8):
        small_out[owner] = small_message(
            wide_grad[:, HALF * owner:HALF * owner + HALF], vec_columns[TALL * owner:TALL * owner + TALL, 0:VEC])
    for keep in range(2):
        recv_small[keep, 0] = small_out[me if keep else small_near[1]]
        places = [(along_x // 2 * 2, ALONG_Y), (along_y // 2 * 2 + 1, ALONG_X)]
        targets = [(target, target if keep else flip(target, way), 2 + core) for target, way in places]
        for target, owner, slot in [*targets, (peer, peer if keep else peer_next, 1)]:
            send(small_out.at[owner], recv_small.at[keep, slot], sent.at[0, SMALL], small_recv.at[keep], target)
    scatter(1, MLP)
    scatter(1, ATTN)

    row = lax.broadcasted_iota(jnp.int32, (LANES, LANES), 0)
    lane = lax.broadcasted_iota(jnp.int32, (LANES, LANES), 1)
    eye = row == lane
    sub = lax.broadcasted_iota(jnp.int32, (8, LANES), 0)

    def lanes_of(first, last):
        column = jnp.sum(row_acc[first:last, :], axis=1, keepdims=True)
        return jnp.sum(jnp.where(eye[first:last, :], column, 0.0), axis=0, keepdims=True)

    def vec_lanes(square):
        vec_row[...] = jnp.zeros_like(vec_row)
        vec_row[0:1, 0:VEC] = jnp.sum(square, axis=0, keepdims=True)
        return vec_row[0:1, 0:LANES], vec_row[0:1, LANES:VEC_PAD]

    def tile_of(rows):
        tile = jnp.zeros((8, LANES), jnp.float32)
        for index, value in enumerate(rows):
            tile = jnp.where(sub == index, value, tile)
        return tile

    def exchange(tiles, which, value):
        tiles[me] = value
        for mask in FAR_FIRST:
            send(tiles.at[me], tiles.at[me], tile_sent.at[which], tile_recv.at[which], flip(me, mask))

    def collect(tiles, which):
        wait_bytes(tiles.at[pl.ds(0, len(FAR_FIRST))], tile_recv.at[which])
        return add_all([tiles[index] for index in range(8)])

    def by_rows(first, groups, columns, step):
        def group(g, carry):
            def inner(j, acc):
                return acc + step((aligned(g, 8), aligned(j, STEP)))

            row_acc[pl.ds(pl.multiple_of(first + g * 8, 8), 8), :] = lax.fori_loop(
                0, columns // STEP, inner, jnp.zeros((8, LANES), jnp.float32))
            return carry

        lax.fori_loop(0, groups, group, 0)

    def square_of(ref):
        return lambda place: fold(ref[place] * ref[place])

    for buffer, sem in ((recv_attn, load_sems.at[ATTN]), (recv_mlp, load_sems.at[MLP])):
        wait_bytes(buffer.at[:, :, pl.ds(0, 3)], sem)
    for copy in state_loads:
        copy.wait()
    row_acc[...] = jnp.zeros_like(row_acc)
    by_rows(0, 8, ATTN_SHARD, square_of(new_weights[0]))
    by_rows(HALF, 4, MLP_SHARD, square_of(new_weights[1]))
    wide_weight, vec_weight = new_weights[2][...], new_weights[3][...]
    row_acc[96:112, 0:HALF] = wide_weight * wide_weight
    weight_lanes = lanes_of(0, LANES)
    weight_low, weight_high = vec_lanes(vec_weight * vec_weight)

    def by_blocks(shape, step, init):
        rows, columns = shape
        for r in range(0, rows, TALL):
            init = lax.fori_loop(0, columns // BLOCK, functools.partial(
                lambda first, j, carry: step((pl.ds(first, TALL), aligned(j, BLOCK)), carry), r), init)
        return init

    def gather_sum(half, keep, chunk):
        source, target = recvs[chunk].at[half, keep], ((sum_attn, sum_mlp) if keep else parts)[chunk].at[half]
        wait_bytes(source, scatter_recv.at[half, keep, chunk])

        def step(place, carry):
            value = [source[(slot, *place)].astype(jnp.float32) for slot in range(4)]
            target[place] = (value[0] + value[1]) + (value[2] + value[3])
            return carry

        by_blocks(SHAPES[chunk], step, 0)

    def gather_small(keep, target):
        wait_bytes(recv_small.at[keep, pl.ds(1, 3)], small_recv.at[keep])
        target[...] = add_all([recv_small[keep, slot].astype(jnp.float32) for slot in range(4)])

    last = {}
    for chunk in (MLP, ATTN):
        for half in HALVES:
            gather_sum(half, 0, chunk)
    gather_small(0, part_small)
    last_small_copy = send(part_small, last_small, sent.at[0, SMALL], last_recv.at[0, SMALL], small_near[1])
    for chunk in (MLP, ATTN):
        for half in HALVES:
            last[half, chunk] = send(parts[chunk].at[half], lasts[chunk].at[half], sent.at[0, chunk],
                                     last_recv.at[half, chunk], flip(me, NEAR[half][1]))
    for chunk in (MLP, ATTN):
        for half in HALVES:
            gather_sum(half, 1, chunk)
    gather_small(1, sum_small)

    last_small_copy.wait_recv()
    wide_total, vec_total = small_parts(sum_small[...] + last_small[...])
    square = fold(jnp.concatenate([wide_total * wide_total, jnp.zeros((TALL, HALF), jnp.float32)], axis=1))
    low, high = vec_lanes(vec_total * vec_total)
    square = square + tile_of([low, high])
    for chunk in (MLP, ATTN):
        for half in HALVES:
            last[half, chunk].wait_recv()
            total, rest = (sum_attn, sum_mlp)[chunk].at[half], lasts[chunk].at[half]

            def step(place, acc):
                value = total[place] + rest[place]
                total[place] = value
                return acc + fold(value * value)

            square = by_blocks(SHAPES[chunk], step, square)

    exchange(start_tiles, 0, tile_of([weight_lanes, weight_low, weight_high, jnp.sum(square, axis=0, keepdims=True)]))
    late_rows = pl.ds(FIRST, FIRST)
    early_columns = pl.ds(0, EARLY)

    def send_early(kind, source, buffer):
        for way, mask in enumerate((ALONG_X, ALONG_Y)):
            send(source, buffer.at[way], early_sent.at[kind], early_recv.at[kind, way], flip(me, mask))

    send_early(0, new_weights[ATTN].at[late_rows, early_columns], early_weight)
    start = collect(start_tiles, 0)
    square = jnp.sum(jnp.sum(start[3:4, :], axis=1, keepdims=True), axis=0, keepdims=True)
    clip = jnp.minimum(1.0, (8.0 * MAX_NORM) / jnp.sqrt(jnp.broadcast_to(square, (8, LANES)))) * 0.125
    clip_block = jnp.concatenate([clip] * (STEP // LANES), axis=1)
    weight_norms = LEARN_RATE * jnp.sqrt(start)

    sums, directions = (sum_attn, sum_mlp), (dir_attn, dir_mlp)

    def update(bank, half):
        rows = SHAPES[bank][0]

        def step(place):
            state = (pl.ds(pl.multiple_of(half * rows + place[0].start, 8), 8), place[1])
            new_first, new_second = moments(
                new_firsts[bank][state], new_seconds[bank][state], sums[bank].at[half][place], clip_block)
            value = direction(new_first, new_second, new_weights[bank][state])
            directions[bank].at[half][place] = value
            return fold(value * value)

        by_rows(HALF * bank + half * rows, rows // 8, SHAPES[bank][1], step)

    def store_moments(bank, half):
        rows = SHAPES[bank][0]

        def step(place, carry):
            state = (pl.ds(half * rows + place[0].start, TALL), place[1])
            clip_wide = jnp.concatenate([clip_block[:, 0:BLOCK]] * 2, axis=0)
            new_first, new_second = moments(
                new_firsts[bank][state], new_seconds[bank][state], sums[bank].at[half][place], clip_wide)
            new_firsts[bank][state] = new_first
            new_seconds[bank][state] = new_second
            return carry

        by_blocks(SHAPES[bank], step, 0)

    def update_small(bank, total, weight):
        new_first, new_second = moments(new_firsts[bank][...], new_seconds[bank][...], total, clip[0:1, 0:1])
        new_firsts[bank][...] = new_first
        new_seconds[bank][...] = new_second
        return direction(new_first, new_second, weight)

    update(ATTN, 0)
    exchange(first_tiles, 1, tile_of([lanes_of(0, FIRST)]))
    update(ATTN, 1)
    send_early(1, dir_attn.at[1, :, early_columns], early_dir)
    for half in HALVES:
        update(MLP, half)
    wide_dir = update_small(2, wide_total, wide_weight)
    vec_dir = update_small(3, vec_total, vec_weight)
    row_acc[96:112, 0:HALF] = wide_dir * wide_dir
    exchange(rest_tiles, 2, tile_of([lanes_of(FIRST, LANES), *vec_lanes(vec_dir * vec_dir)]))
    for bank in (ATTN, MLP):
        for half in HALVES:
            store_moments(bank, half)

    own_copies = {}

    def send_own(half, chunk, way):
        place = all_small.at[me] if chunk == SMALL else replica_chunk(half, me, chunk)
        if (half, chunk) == (1, ATTN) and way:
            place = replicas[ATTN].at[late_rows, pl.ds(pl.multiple_of(me * ATTN_SHARD + EARLY, BLOCK), ATTN_SHARD - EARLY)]
        recv_sem = own_recv.at[half, chunk, way - 1] if way else pair_recv.at[chunk]
        own_copies[half, chunk, way] = send(place, place, sent.at[1, chunk], recv_sem, flip(me, (PEER, ALONG_X, ALONG_Y)[way]))

    def spread_ratio(first, last, ratio):
        row_acc[first:last, :] = jnp.broadcast_to(
            jnp.sum(jnp.where(eye[first:last, :], ratio[0:1, :], 0.0), axis=1, keepdims=True), (last - first, LANES))

    def form_weights(bank, half, owner, shape, weight, direct, result):
        rows = SHAPES[bank][0]

        def step(place, carry):
            first = half * rows + place[0].start
            scale = jnp.concatenate([row_acc[HALF * bank + first:HALF * bank + first + TALL, :]] * (BLOCK // LANES), axis=1)
            value = weight[place] - scale * direct[place]
            if result is not None:
                result[place] = value
            target = pl.ds(pl.multiple_of(owner * SHAPES[bank][1] + place[1].start, BLOCK), BLOCK)
            replicas[bank][pl.ds(first, TALL), target] = value.astype(jnp.bfloat16)
            return carry

        by_blocks(shape, step, 0)

    def new_weight(bank, half, ways):
        rows = SHAPES[bank][0]
        mine = new_weights[bank].at[pl.ds(half * rows, rows)]
        form_weights(bank, half, me, SHAPES[bank], mine, directions[bank].at[half], mine)
        for way in ways:
            send_own(half, bank, way)

    spread_ratio(0, FIRST, weight_norms / jnp.sqrt(collect(first_tiles, 1)))
    new_weight(ATTN, 0, (1, 2, 0))
    ratio = weight_norms / jnp.sqrt(collect(rest_tiles, 2))
    spread_ratio(FIRST, LANES, ratio)
    wait_bytes(early_weight, early_sent.at[0])
    new_weight(ATTN, 1, (2, 0))
    for half in HALVES:
        new_weight(MLP, half, (1 + half, 0))
    value = wide_weight - row_acc[96:112, 0:HALF] * wide_dir
    new_weights[2][...] = value
    wide_value = value
    vec_row[0:1, 0:LANES] = ratio[1:2, :]
    vec_row[0:1, LANES:VEC_PAD] = ratio[2:3, :]
    value = vec_weight - vec_row[0:1, 0:VEC] * vec_dir
    new_weights[3][...] = value
    all_small[me] = small_message(wide_value, value)
    for way in (1, 2, 0):
        send_own(0, SMALL, way)
    send_own(1, ATTN, 1)
    for half in HALVES:
        send_own(half, MLP, 2 - half)

    for way, owner in enumerate((along_x, along_y)):
        for kind, buffer in enumerate((early_weight, early_dir)):
            wait_bytes(buffer.at[way], early_recv.at[kind, way])
        form_weights(ATTN, 1, owner, (FIRST, EARLY), early_weight.at[way], early_dir.at[way], None)

    def send_pair(place, chunk):
        send(place, place, sent.at[1, chunk], pair_recv.at[chunk], peer)

    for way in (1, 2):
        own_copies[0, SMALL, way].wait_recv()
    place = all_small.at[small_near[0]]
    passed_small = send(place, place, sent.at[1, SMALL], pass_recv.at[0, SMALL], small_near[1])
    for owner in small_near:
        send_pair(all_small.at[owner], SMALL)
    passed = {}
    for chunk in (MLP, ATTN):
        for half in HALVES:
            own_copies[half, chunk, 1 + half].wait_recv()
            place = replica_chunk(half, flip(me, NEAR[half][0]), chunk)
            passed[half, chunk] = send(place, place, sent.at[1, chunk], pass_recv.at[half, chunk], flip(me, NEAR[half][1]))
            send_pair(place, chunk)
    for chunk in BIG:
        for half in HALVES:
            own_copies[half, chunk, 2 - half].wait_recv()
            send_pair(replica_chunk(half, flip(me, NEAR[half][1]), chunk), chunk)
    far = flip(me, ALONG_X + ALONG_Y)
    passed_small.wait_recv()
    send_pair(all_small.at[far], SMALL)
    wait_bytes(all_small.at[pl.ds(0, 4)], pair_recv.at[SMALL])
    wides, vecs = zip(*(small_parts(all_small[owner].astype(jnp.float32)) for owner in range(8)))
    replicas[2][...] = jnp.concatenate(wides, axis=1).astype(jnp.bfloat16)
    for owner in range(8):
        vec_columns[TALL * owner:TALL * owner + TALL, 0:VEC] = vecs[owner]
    vec_rows[...] = vec_columns[...].T
    replicas[3][...] = vec_rows[0:VEC, :].astype(jnp.bfloat16)
    for chunk in (MLP, ATTN):
        for half in HALVES:
            passed[half, chunk].wait_recv()
            send_pair(replica_chunk(half, far, chunk), chunk)
    for bank in (ATTN, MLP):
        wait_bytes(replicas[bank].at[:, pl.ds(0, LENGTHS[bank] // 2)], pair_recv.at[bank])
        wait_bytes(replicas[bank], sent.at[0, bank])
        columns = len(FAR_FIRST) * SHARDS[bank][1] - (EARLY if bank == ATTN else 0)
        wait_bytes(replicas[bank].at[:, pl.ds(0, columns)], sent.at[1, bank])
    wait_bytes(all_small, sent.at[0, SMALL])
    wait_bytes(all_small.at[pl.ds(0, len(FAR_FIRST))], sent.at[1, SMALL])
    wait_bytes(early_dir, early_sent.at[1])
    for which, tiles in enumerate((start_tiles, first_tiles, rest_tiles)):
        wait_bytes(tiles.at[pl.ds(0, len(FAR_FIRST))], tile_sent.at[which])


def write_out(*refs):
    count = (len(refs) - 1) // 2
    copies = [pltpu.make_async_copy(refs[k], refs[count + k], refs[-1]) for k in range(count)]
    for copy in copies:
        copy.start()
    for copy in copies:
        copy.wait()


def solution(mesh):
    shards = [jax.ShapeDtypeStruct(shape, jnp.float32) for shape in SHARDS]
    shapes = [jax.ShapeDtypeStruct(shape, jnp.bfloat16) for shape in zip(ROWS, LENGTHS)] + shards * 3
    f32, bf16 = jnp.float32, jnp.bfloat16
    dma = pltpu.SemaphoreType.DMA
    attn, mlp = SHAPES

    def sums(*lead):
        return [pltpu.VMEM((*lead, *attn), f32), pltpu.VMEM((*lead, *mlp), f32)]

    small = (TALL, VEC_PAD)
    scratch = [
        pltpu.VMEM((2, 2, 4, *attn), bf16), pltpu.VMEM((2, 2, 4, *mlp), bf16), pltpu.VMEM((2, 4, *small), bf16),
        *sums(2), pltpu.VMEM(small, f32), *sums(2), pltpu.VMEM(small, f32), *sums(2), pltpu.VMEM(small, f32), *sums(2),
        *[pltpu.VMEM((2, FIRST, EARLY), f32)] * 2, pltpu.VMEM((VEC, LANES), bf16), pltpu.VMEM((TALL, BLOCK), bf16), pltpu.VMEM((8, *small), bf16),
        pltpu.VMEM((8, *small), bf16),
        pltpu.VMEM((VEC_PAD, LANES), f32), pltpu.VMEM((LANES, VEC_PAD), f32), pltpu.VMEM((8, VEC_PAD), f32),
        *[pltpu.VMEM((8, 8, LANES), f32)] * 3, pltpu.VMEM((LANES, LANES), f32),
        dma((10,)), dma((2, 3)), dma((3,)), dma((2, 2, 2)), dma((2,)), dma((2, 3)), dma((3,)), dma((2, 3, 2)), dma((2, 3)),
        dma((3,)), dma((2,)), dma((2, 2)),
    ]
    count = len(shapes)
    anywhere = [pl.BlockSpec(memory_space=pl.ANY)] * count
    step = pl.pallas_call(
        kernel,
        out_shape=[pltpu.VMEM(shape.shape, shape.dtype) for shape in shapes],
        in_specs=anywhere,
        out_specs=[pl.BlockSpec(memory_space=pltpu.VMEM)] * count,
        scratch_shapes=scratch,
        compiler_params=pltpu.CompilerParams(collective_id=0, has_side_effects=True, vmem_limit_bytes=36 * MIB),
        name="lamb_step",
    )
    finish = pl.pallas_call(
        write_out,
        out_shape=shapes,
        in_specs=anywhere,
        out_specs=anywhere,
        scratch_shapes=[dma],
        compiler_params=pltpu.CompilerParams(vmem_limit_bytes=MIB),
        name="write_out",
    )

    def local_step(*banks):
        banks = [bank[0] for bank in banks[:4]] + [bank.T if bank.shape == (VEC, TALL) else bank for bank in banks[4:]]
        banks = [pltpu.with_memory_space_constraint(bank, pltpu.HBM) for bank in banks]
        results = finish(*step(*banks))
        return tuple(value.T if value.shape == (TALL, VEC) else value for value in results)

    grad_spec, shard_spec, full_spec = P("data", None, None), P(None, "data"), P(None, None)
    return jax.shard_map(local_step, mesh=mesh, in_specs=(grad_spec,) * 4 + (shard_spec,) * 12,
                         out_specs=(full_spec,) * 4 + (shard_spec,) * 12, check_vma=False)
```

```python
import functools

import jax
import jax.numpy as jnp
from jax import lax
from jax.experimental import pallas as pl
from jax.experimental.pallas import tpu as pltpu
from jax.sharding import PartitionSpec as P

STEP_NUMBER = 10
LEARN_RATE = 0.04
BETA_FIRST = 0.9
BETA_SECOND = 0.999
EPSILON = 1e-6
WEIGHT_DECAY = 0.01
MAX_NORM = 1.0
FIRST_SCALE = 1.0 / (1.0 - BETA_FIRST ** STEP_NUMBER)
SECOND_SCALE = 1.0 / (1.0 - BETA_SECOND ** STEP_NUMBER)

MESH = pl.DeviceIdType.MESH
LANES = 128
TALL = 16
HALF = 64
FIRST = 32
EARLY = 1024
VEC = 146
VEC_PAD = 256
ATTN_SHARD = 2048
MLP_SHARD = 8192
STEP = 2048
BLOCK = 1024
WIDE = 512
TAIL = 640
MIB = 2 ** 20
ROWS = (HALF, 32, TALL, VEC)
LENGTHS = (16384, 65536, WIDE, LANES)
SHARDS = ((HALF, ATTN_SHARD), (32, MLP_SHARD), (TALL, HALF), (TALL, VEC))
ATTN, MLP, SMALL = range(3)
BIG = (ATTN, MLP)
HALVES = range(2)
SHAPES = ((32, ATTN_SHARD), (TALL, MLP_SHARD))
PEER, ALONG_X, ALONG_Y = 1, 2, 4
NEAR = ((ALONG_X, ALONG_Y), (ALONG_Y, ALONG_X))
WIDE_LANES = (LANES, LANES + HALF)
FAR_FIRST = (6, 7, 4, 2, 5, 3, 1)


def flip(index, mask):
    core, x, y = index % 2, (index // 2) % 2, index // 4
    if mask & PEER:
        core = 1 - core
    if mask & ALONG_X:
        x = 1 - x
    if mask & ALONG_Y:
        y = 1 - y
    return y * 4 + x * 2 + core


def aligned(index, size):
    return pl.ds(pl.multiple_of(index * size, size), size)


def moments(first, second, total, clip):
    clipped = clip * total
    new_first = BETA_FIRST * first + (1.0 - BETA_FIRST) * clipped
    new_second = BETA_SECOND * second + (1.0 - BETA_SECOND) * (clipped * clipped)
    return new_first, new_second


def direction(new_first, new_second, weight):
    return (new_first * FIRST_SCALE) / (jnp.sqrt(new_second * SECOND_SCALE) + EPSILON) + WEIGHT_DECAY * weight


def fold(square):
    rows, columns = square.shape
    parts = [square[r:r + 8, k:k + LANES] for r in range(0, rows, 8) for k in range(0, columns, LANES)]
    while len(parts) > 1:
        parts = [a + b for a, b in zip(parts[::2], parts[1::2])] + ([parts[-1]] if len(parts) % 2 else [])
    return parts[0]


def add_all(values):
    return functools.reduce(lambda a, b: a + b, values)


def kernel(*refs):
    grads, weights, firsts, seconds = refs[0:4], refs[4:8], refs[8:12], refs[12:16]
    replicas, new_weights, new_firsts, new_seconds = refs[16:20], refs[20:24], refs[24:28], refs[28:32]
    (recv_attn, recv_mlp, recv_small, part_attn, part_mlp, part_small, last_attn, last_mlp, last_small,
     sum_attn, sum_mlp, sum_small, dir_attn, dir_mlp, early_weight, early_dir, vec_in, wide_in, small_out, all_small,
     vec_rows, vec_columns, vec_row, start_tiles, first_tiles, rest_tiles, row_acc,
     load_sems, sent, tile_sent, scatter_recv, small_recv, last_recv, tile_recv, own_recv, pass_recv, pair_recv,
     early_sent, early_recv, tail_recv) = refs[32:]
    recvs, parts, lasts = (recv_attn, recv_mlp), (part_attn, part_mlp), (last_attn, last_mlp)
    me = lax.axis_index("data")
    core = me % 2

    def grad_chunk(half, owner, chunk):
        rows, columns = SHAPES[chunk]
        return grads[chunk].at[pl.ds(rows * half, rows), aligned(owner, columns)]

    def replica_chunk(half, owner, chunk):
        rows, columns = SHAPES[chunk]
        return replicas[chunk].at[pl.ds(rows * half, rows), aligned(owner, columns)]

    def replica_part(half, owner, first, last):
        rows, columns = SHAPES[ATTN]
        start = pl.multiple_of(owner * columns + first, LANES)
        return replicas[ATTN].at[pl.ds(rows * half, rows), pl.ds(start, last - first)]

    along_x, along_y = flip(me, ALONG_X), flip(me, ALONG_Y)
    small_near = (along_x * (1 - core) + along_y * core, along_y * (1 - core) + along_x * core)
    peer = flip(me, PEER)
    peer_next = flip(peer, ALONG_X) * (1 - core) + flip(peer, ALONG_Y) * core

    def send(source, target, send_sem, recv_sem, device):
        copy = pltpu.make_async_remote_copy(src_ref=source, dst_ref=target, send_sem=send_sem, recv_sem=recv_sem,
                                            device_id=(device,), device_id_type=MESH)
        copy.start()
        return copy

    def wait_bytes(ref, sem):
        pltpu.make_async_copy(ref, ref, sem).wait()

    barrier = pltpu.get_barrier_semaphore()
    near = (1, 2, 3, 4, 5)
    for mask in near:
        pl.semaphore_signal(barrier, inc=1, device_id=(flip(me, mask),), device_id_type=MESH)

    small_loads = [pltpu.make_async_copy(grads[2], wide_in, load_sems.at[2]),
                   pltpu.make_async_copy(grads[3], vec_in, load_sems.at[3])]
    for copy in small_loads:
        copy.start()
    for keep in range(2):
        for half in HALVES:
            for chunk in (MLP, ATTN):
                owner = me if keep else flip(me, NEAR[half][1])
                pltpu.make_async_copy(grad_chunk(half, owner, chunk), recvs[chunk].at[half, keep, 0],
                                      scatter_recv.at[half, keep, chunk]).start()
    state_loads = []
    for index, (source, target) in enumerate(((weights, new_weights), (firsts, new_firsts), (seconds, new_seconds))):
        for bank in range(4):
            copy = pltpu.make_async_copy(source[bank], target[bank], load_sems.at[bank if bank < 2 else 2 * index + bank + 2])
            copy.start()
            if bank >= 2:
                state_loads.append(copy)
    pl.semaphore_wait(barrier, len(near))

    def scatter(keep, chunk):
        for slot in (1, 2, 0):
            for half in HALVES:
                target = peer if slot == 0 else flip(me, NEAR[half][0]) // 2 * 2 + slot - 1
                owner = target if keep else flip(target, NEAR[half][1])
                send(grad_chunk(half, owner, chunk), recvs[chunk].at[half, keep, 1 if slot == 0 else 2 + core],
                     sent.at[0, chunk], scatter_recv.at[half, keep, chunk], target)

    scatter(0, MLP)
    scatter(0, ATTN)
    for copy in small_loads:
        copy.wait()
    vec_rows[...] = jnp.zeros_like(vec_rows)
    vec_rows[0:VEC, :] = vec_in[...].astype(jnp.float32)
    vec_columns[...] = vec_rows[...].T

    def small_message(wide, vec):
        pad = jnp.zeros((TALL, VEC_PAD - VEC - HALF), jnp.float32)
        return jnp.concatenate([vec[:, 0:LANES], wide, vec[:, LANES:VEC], pad], axis=1).astype(jnp.bfloat16)

    def small_parts(message):
        vec = jnp.concatenate([message[:, 0:LANES], message[:, WIDE_LANES[1]:HALF + VEC]], axis=1)
        return message[:, slice(*WIDE_LANES)], vec

    wide_grad = wide_in[...].astype(jnp.float32)
    for owner in range(8):
        small_out[owner] = small_message(
            wide_grad[:, HALF * owner:HALF * owner + HALF], vec_columns[TALL * owner:TALL * owner + TALL, 0:VEC])
    for keep in range(2):
        recv_small[keep, 0] = small_out[me if keep else small_near[1]]
        places = [(along_x // 2 * 2, ALONG_Y), (along_y // 2 * 2 + 1, ALONG_X)]
        targets = [(target, target if keep else flip(target, way), 2 + core) for target, way in places]
        for target, owner, slot in [*targets, (peer, peer if keep else peer_next, 1)]:
            send(small_out.at[owner], recv_small.at[keep, slot], sent.at[0, SMALL], small_recv.at[keep], target)
    scatter(1, MLP)
    scatter(1, ATTN)

    row = lax.broadcasted_iota(jnp.int32, (LANES, LANES), 0)
    lane = lax.broadcasted_iota(jnp.int32, (LANES, LANES), 1)
    eye = row == lane
    sub = lax.broadcasted_iota(jnp.int32, (8, LANES), 0)

    def lanes_of(first, last):
        column = jnp.sum(row_acc[first:last, :], axis=1, keepdims=True)
        return jnp.sum(jnp.where(eye[first:last, :], column, 0.0), axis=0, keepdims=True)

    def vec_lanes(square):
        vec_row[...] = jnp.zeros_like(vec_row)
        vec_row[0:1, 0:VEC] = jnp.sum(square, axis=0, keepdims=True)
        return vec_row[0:1, 0:LANES], vec_row[0:1, LANES:VEC_PAD]

    def tile_of(rows):
        tile = jnp.zeros((8, LANES), jnp.float32)
        for index, value in enumerate(rows):
            tile = jnp.where(sub == index, value, tile)
        return tile

    def exchange(tiles, which, value):
        tiles[me] = value
        for mask in FAR_FIRST:
            send(tiles.at[me], tiles.at[me], tile_sent.at[which], tile_recv.at[which], flip(me, mask))

    def collect(tiles, which):
        wait_bytes(tiles.at[pl.ds(0, len(FAR_FIRST))], tile_recv.at[which])
        return add_all([tiles[index] for index in range(8)])

    def by_rows(first, groups, columns, step):
        def group(g, carry):
            def inner(j, acc):
                return acc + step((aligned(g, 8), aligned(j, STEP)))

            row_acc[pl.ds(pl.multiple_of(first + g * 8, 8), 8), :] = lax.fori_loop(
                0, columns // STEP, inner, jnp.zeros((8, LANES), jnp.float32))
            return carry

        lax.fori_loop(0, groups, group, 0)

    def square_of(ref):
        return lambda place: fold(ref[place] * ref[place])

    for buffer, sem in ((recv_attn, load_sems.at[ATTN]), (recv_mlp, load_sems.at[MLP])):
        wait_bytes(buffer.at[:, :, pl.ds(0, 3)], sem)
    for copy in state_loads:
        copy.wait()
    row_acc[...] = jnp.zeros_like(row_acc)
    by_rows(0, 8, ATTN_SHARD, square_of(new_weights[0]))
    by_rows(HALF, 4, MLP_SHARD, square_of(new_weights[1]))
    wide_weight, vec_weight = new_weights[2][...], new_weights[3][...]
    row_acc[96:112, 0:HALF] = wide_weight * wide_weight
    weight_lanes = lanes_of(0, LANES)
    weight_low, weight_high = vec_lanes(vec_weight * vec_weight)

    def by_blocks(shape, step, init):
        rows, columns = shape
        for r in range(0, rows, TALL):
            init = lax.fori_loop(0, columns // BLOCK, functools.partial(
                lambda first, j, carry: step((pl.ds(first, TALL), aligned(j, BLOCK)), carry), r), init)
        return init

    def gather_sum(half, keep, chunk):
        source, target = recvs[chunk].at[half, keep], ((sum_attn, sum_mlp) if keep else parts)[chunk].at[half]
        wait_bytes(source, scatter_recv.at[half, keep, chunk])

        def step(place, carry):
            value = [source[(slot, *place)].astype(jnp.float32) for slot in range(4)]
            target[place] = (value[0] + value[1]) + (value[2] + value[3])
            return carry

        by_blocks(SHAPES[chunk], step, 0)

    def gather_small(keep, target):
        wait_bytes(recv_small.at[keep, pl.ds(1, 3)], small_recv.at[keep])
        target[...] = add_all([recv_small[keep, slot].astype(jnp.float32) for slot in range(4)])

    last = {}
    for chunk in (MLP, ATTN):
        for half in HALVES:
            gather_sum(half, 0, chunk)
    gather_small(0, part_small)
    last_small_copy = send(part_small, last_small, sent.at[0, SMALL], last_recv.at[0, SMALL], small_near[1])
    for chunk in (MLP, ATTN):
        for half in HALVES:
            last[half, chunk] = send(parts[chunk].at[half], lasts[chunk].at[half], sent.at[0, chunk],
                                     last_recv.at[half, chunk], flip(me, NEAR[half][1]))
    for chunk in (MLP, ATTN):
        for half in HALVES:
            gather_sum(half, 1, chunk)
    gather_small(1, sum_small)

    last_small_copy.wait_recv()
    wide_total, vec_total = small_parts(sum_small[...] + last_small[...])
    square = fold(jnp.concatenate([wide_total * wide_total, jnp.zeros((TALL, HALF), jnp.float32)], axis=1))
    low, high = vec_lanes(vec_total * vec_total)
    square = square + tile_of([low, high])
    for chunk in (MLP, ATTN):
        for half in HALVES:
            last[half, chunk].wait_recv()
            total, rest = (sum_attn, sum_mlp)[chunk].at[half], lasts[chunk].at[half]

            def step(place, acc):
                value = total[place] + rest[place]
                total[place] = value
                return acc + fold(value * value)

            square = by_blocks(SHAPES[chunk], step, square)

    exchange(start_tiles, 0, tile_of([weight_lanes, weight_low, weight_high, jnp.sum(square, axis=0, keepdims=True)]))
    late_rows = pl.ds(FIRST, FIRST)
    early_columns = pl.ds(0, EARLY)

    def send_early(kind, source, buffer):
        for way, mask in enumerate((ALONG_X, ALONG_Y)):
            send(source, buffer.at[way], early_sent.at[kind], early_recv.at[kind, way], flip(me, mask))

    send_early(0, new_weights[ATTN].at[late_rows, early_columns], early_weight)
    start = collect(start_tiles, 0)
    square = jnp.sum(jnp.sum(start[3:4, :], axis=1, keepdims=True), axis=0, keepdims=True)
    clip = jnp.minimum(1.0, (8.0 * MAX_NORM) / jnp.sqrt(jnp.broadcast_to(square, (8, LANES)))) * 0.125
    clip_block = jnp.concatenate([clip] * (STEP // LANES), axis=1)
    weight_norms = LEARN_RATE * jnp.sqrt(start)

    sums, directions = (sum_attn, sum_mlp), (dir_attn, dir_mlp)

    def update(bank, half):
        rows = SHAPES[bank][0]

        def step(place):
            state = (pl.ds(pl.multiple_of(half * rows + place[0].start, 8), 8), place[1])
            new_first, new_second = moments(
                new_firsts[bank][state], new_seconds[bank][state], sums[bank].at[half][place], clip_block)
            value = direction(new_first, new_second, new_weights[bank][state])
            directions[bank].at[half][place] = value
            return fold(value * value)

        by_rows(HALF * bank + half * rows, rows // 8, SHAPES[bank][1], step)

    def store_moments(bank, half):
        rows = SHAPES[bank][0]

        def step(place, carry):
            state = (pl.ds(half * rows + place[0].start, TALL), place[1])
            clip_wide = jnp.concatenate([clip_block[:, 0:BLOCK]] * 2, axis=0)
            new_first, new_second = moments(
                new_firsts[bank][state], new_seconds[bank][state], sums[bank].at[half][place], clip_wide)
            new_firsts[bank][state] = new_first
            new_seconds[bank][state] = new_second
            return carry

        by_blocks(SHAPES[bank], step, 0)

    def update_small(bank, total, weight):
        new_first, new_second = moments(new_firsts[bank][...], new_seconds[bank][...], total, clip[0:1, 0:1])
        new_firsts[bank][...] = new_first
        new_seconds[bank][...] = new_second
        return direction(new_first, new_second, weight)

    update(ATTN, 0)
    exchange(first_tiles, 1, tile_of([lanes_of(0, FIRST)]))
    update(ATTN, 1)
    send_early(1, dir_attn.at[1, :, early_columns], early_dir)
    for half in HALVES:
        update(MLP, half)
    wide_dir = update_small(2, wide_total, wide_weight)
    vec_dir = update_small(3, vec_total, vec_weight)
    row_acc[96:112, 0:HALF] = wide_dir * wide_dir
    exchange(rest_tiles, 2, tile_of([lanes_of(FIRST, LANES), *vec_lanes(vec_dir * vec_dir)]))
    for bank in (ATTN, MLP):
        for half in HALVES:
            store_moments(bank, half)

    own_copies = {}

    def send_own(half, chunk, way):
        place = all_small.at[me] if chunk == SMALL else replica_chunk(half, me, chunk)
        if (half, chunk) == (1, ATTN) and way:
            place = replica_part(1, me, EARLY, ATTN_SHARD)
        recv_sem = own_recv.at[half, chunk, way - 1] if way else pair_recv.at[chunk]
        own_copies[half, chunk, way] = send(place, place, sent.at[1, chunk], recv_sem, flip(me, (PEER, ALONG_X, ALONG_Y)[way]))

    def spread_ratio(first, last, ratio):
        row_acc[first:last, :] = jnp.broadcast_to(
            jnp.sum(jnp.where(eye[first:last, :], ratio[0:1, :], 0.0), axis=1, keepdims=True), (last - first, LANES))

    def form_weights(bank, half, owner, shape, weight, direct, result):
        rows = SHAPES[bank][0]

        def step(place, carry):
            first = half * rows + place[0].start
            scale = jnp.concatenate([row_acc[HALF * bank + first:HALF * bank + first + TALL, :]] * (BLOCK // LANES), axis=1)
            value = weight[place] - scale * direct[place]
            if result is not None:
                result[place] = value
            target = pl.ds(pl.multiple_of(owner * SHAPES[bank][1] + place[1].start, BLOCK), BLOCK)
            replicas[bank][pl.ds(first, TALL), target] = value.astype(jnp.bfloat16)
            return carry

        by_blocks(shape, step, 0)

    def new_weight(bank, half, ways):
        rows = SHAPES[bank][0]
        mine = new_weights[bank].at[pl.ds(half * rows, rows)]
        form_weights(bank, half, me, SHAPES[bank], mine, directions[bank].at[half], mine)
        for way in ways:
            send_own(half, bank, way)

    spread_ratio(0, FIRST, weight_norms / jnp.sqrt(collect(first_tiles, 1)))
    new_weight(ATTN, 0, (1, 2, 0))
    ratio = weight_norms / jnp.sqrt(collect(rest_tiles, 2))
    spread_ratio(FIRST, LANES, ratio)
    wait_bytes(early_weight, early_sent.at[0])
    new_weight(ATTN, 1, (2, 0))
    for half in HALVES:
        new_weight(MLP, half, (1 + half, 0))
    value = wide_weight - row_acc[96:112, 0:HALF] * wide_dir
    new_weights[2][...] = value
    wide_value = value
    vec_row[0:1, 0:LANES] = ratio[1:2, :]
    vec_row[0:1, LANES:VEC_PAD] = ratio[2:3, :]
    value = vec_weight - vec_row[0:1, 0:VEC] * vec_dir
    new_weights[3][...] = value
    all_small[me] = small_message(wide_value, value)
    for way in (1, 2, 0):
        send_own(0, SMALL, way)
    send_own(1, ATTN, 1)
    for half in HALVES:
        send_own(half, MLP, 2 - half)

    for way, owner in enumerate((along_x, along_y)):
        for kind, buffer in enumerate((early_weight, early_dir)):
            wait_bytes(buffer.at[way], early_recv.at[kind, way])
        form_weights(ATTN, 1, owner, (FIRST, EARLY), early_weight.at[way], early_dir.at[way], None)

    def send_pair(place, chunk):
        send(place, place, sent.at[1, chunk], pair_recv.at[chunk], peer)

    for way in (1, 2):
        own_copies[0, SMALL, way].wait_recv()
    place = all_small.at[small_near[0]]
    passed_small = send(place, place, sent.at[1, SMALL], pass_recv.at[0, SMALL], small_near[1])
    for owner in small_near:
        send_pair(all_small.at[owner], SMALL)
    passed = {}
    for chunk in (MLP, ATTN):
        for half in HALVES:
            own_copies[half, chunk, 1 + half].wait_recv()
            owner, target = flip(me, NEAR[half][0]), flip(me, NEAR[half][1])
            place = replica_chunk(half, owner, chunk)
            send_pair(place, chunk)
            if chunk == ATTN:
                place = replica_part(half, owner, 0, ATTN_SHARD - TAIL)
            passed[half, chunk] = send(place, place, sent.at[1, chunk], pass_recv.at[half, chunk], target)
    for target_core in (0, 1):
        for half in HALVES:
            place = replica_part(half, flip(me, NEAR[half][0]), ATTN_SHARD - TAIL, ATTN_SHARD)
            send(place, place, sent.at[1, ATTN], tail_recv, flip(me, NEAR[half][1] + (PEER if target_core else 0)))
    for chunk in BIG:
        for half in HALVES:
            own_copies[half, chunk, 2 - half].wait_recv()
            send_pair(replica_chunk(half, flip(me, NEAR[half][1]), chunk), chunk)
    far = flip(me, ALONG_X + ALONG_Y)
    passed_small.wait_recv()
    send_pair(all_small.at[far], SMALL)
    wait_bytes(all_small.at[pl.ds(0, 4)], pair_recv.at[SMALL])
    wides, vecs = zip(*(small_parts(all_small[owner].astype(jnp.float32)) for owner in range(8)))
    replicas[2][...] = jnp.concatenate(wides, axis=1).astype(jnp.bfloat16)
    for owner in range(8):
        vec_columns[TALL * owner:TALL * owner + TALL, 0:VEC] = vecs[owner]
    vec_rows[...] = vec_columns[...].T
    replicas[3][...] = vec_rows[0:VEC, :].astype(jnp.bfloat16)
    wait_bytes(all_small, sent.at[0, SMALL])
    wait_bytes(all_small.at[pl.ds(0, len(FAR_FIRST))], sent.at[1, SMALL])
    wait_bytes(early_dir, early_sent.at[1])
    for which, tiles in enumerate((start_tiles, first_tiles, rest_tiles)):
        wait_bytes(tiles.at[pl.ds(0, len(FAR_FIRST))], tile_sent.at[which])
    for bank in BIG:
        wait_bytes(replicas[bank], sent.at[0, bank])
    for chunk in (MLP, ATTN):
        for half in HALVES:
            passed[half, chunk].wait_recv()
            send_pair(replica_part(half, far, 0, ATTN_SHARD - TAIL) if chunk == ATTN else replica_chunk(half, far, chunk), chunk)
    for bank, received, gone in ((MLP, 0, 0), (ATTN, TAIL, EARLY)):
        columns = SHAPES[bank][1]
        wait_bytes(replicas[bank].at[:, pl.ds(0, 4 * columns - received)], pair_recv.at[bank])
        wait_bytes(replicas[bank].at[:, pl.ds(0, len(FAR_FIRST) * columns - gone)], sent.at[1, bank])
    wait_bytes(replicas[ATTN].at[:, pl.ds(0, 2 * TAIL)], tail_recv)


def write_out(*refs):
    count = (len(refs) - 1) // 2
    copies = [pltpu.make_async_copy(refs[k], refs[count + k], refs[-1]) for k in range(count)]
    for copy in copies:
        copy.start()
    for copy in copies:
        copy.wait()


def solution(mesh):
    shards = [jax.ShapeDtypeStruct(shape, jnp.float32) for shape in SHARDS]
    shapes = [jax.ShapeDtypeStruct(shape, jnp.bfloat16) for shape in zip(ROWS, LENGTHS)] + shards * 3
    f32, bf16 = jnp.float32, jnp.bfloat16
    dma = pltpu.SemaphoreType.DMA
    attn, mlp = SHAPES

    def sums(*lead):
        return [pltpu.VMEM((*lead, *attn), f32), pltpu.VMEM((*lead, *mlp), f32)]

    small = (TALL, VEC_PAD)
    scratch = [
        pltpu.VMEM((2, 2, 4, *attn), bf16), pltpu.VMEM((2, 2, 4, *mlp), bf16), pltpu.VMEM((2, 4, *small), bf16),
        *sums(2), pltpu.VMEM(small, f32), *sums(2), pltpu.VMEM(small, f32), *sums(2), pltpu.VMEM(small, f32), *sums(2),
        *[pltpu.VMEM((2, FIRST, EARLY), f32)] * 2, pltpu.VMEM((VEC, LANES), bf16), pltpu.VMEM((TALL, WIDE), bf16), pltpu.VMEM((8, *small), bf16),
        pltpu.VMEM((8, *small), bf16),
        pltpu.VMEM((VEC_PAD, LANES), f32), pltpu.VMEM((LANES, VEC_PAD), f32), pltpu.VMEM((8, VEC_PAD), f32),
        *[pltpu.VMEM((8, 8, LANES), f32)] * 3, pltpu.VMEM((LANES, LANES), f32),
        dma((10,)), dma((2, 3)), dma((3,)), dma((2, 2, 2)), dma((2,)), dma((2, 3)), dma((3,)), dma((2, 3, 2)), dma((2, 3)),
        dma((3,)), dma((2,)), dma((2, 2)), dma,
    ]
    count = len(shapes)
    anywhere = [pl.BlockSpec(memory_space=pl.ANY)] * count
    step = pl.pallas_call(
        kernel,
        out_shape=[pltpu.VMEM(shape.shape, shape.dtype) for shape in shapes],
        in_specs=anywhere,
        out_specs=[pl.BlockSpec(memory_space=pltpu.VMEM)] * count,
        scratch_shapes=scratch,
        compiler_params=pltpu.CompilerParams(collective_id=0, has_side_effects=True, vmem_limit_bytes=36 * MIB),
        name="lamb_step",
    )
    finish = pl.pallas_call(
        write_out,
        out_shape=shapes,
        in_specs=anywhere,
        out_specs=anywhere,
        scratch_shapes=[dma],
        compiler_params=pltpu.CompilerParams(vmem_limit_bytes=MIB),
        name="write_out",
    )

    def local_step(*banks):
        banks = [bank[0] for bank in banks[:4]] + [bank.T if bank.shape == (VEC, TALL) else bank for bank in banks[4:]]
        banks = [pltpu.with_memory_space_constraint(bank, pltpu.HBM) for bank in banks]
        results = finish(*step(*banks))
        return tuple(value.T if value.shape == (TALL, VEC) else value for value in results)

    grad_spec, shard_spec, full_spec = P("data", None, None), P(None, "data"), P(None, None)
    return jax.shard_map(local_step, mesh=mesh, in_specs=(grad_spec,) * 4 + (shard_spec,) * 12,
                         out_specs=(full_spec,) * 4 + (shard_spec,) * 12, check_vma=False)
```

```python
import functools

import jax
import jax.numpy as jnp
from jax import lax
from jax.experimental import pallas as pl
from jax.experimental.pallas import tpu as pltpu
from jax.sharding import PartitionSpec as P

STEP_NUMBER = 10
LEARN_RATE = 0.04
BETA_FIRST = 0.9
BETA_SECOND = 0.999
EPSILON = 1e-6
WEIGHT_DECAY = 0.01
MAX_NORM = 1.0
FIRST_SCALE = 1.0 / (1.0 - BETA_FIRST ** STEP_NUMBER)
SECOND_SCALE = 1.0 / (1.0 - BETA_SECOND ** STEP_NUMBER)

MESH = pl.DeviceIdType.MESH
LANES = 128
TALL = 16
HALF = 64
FIRST = 32
EARLY = 1024
VEC = 146
VEC_PAD = 256
ATTN_SHARD = 2048
MLP_SHARD = 8192
STEP = 2048
BLOCK = 1024
WIDE = 512
TAIL = 640
MIB = 2 ** 20
ROWS = (HALF, 32, TALL, VEC)
LENGTHS = (16384, 65536, WIDE, LANES)
SHARDS = ((HALF, ATTN_SHARD), (32, MLP_SHARD), (TALL, HALF), (TALL, VEC))
ATTN, MLP, SMALL = range(3)
BIG = (ATTN, MLP)
HALVES = range(2)
SHAPES = ((32, ATTN_SHARD), (TALL, MLP_SHARD))
PEER, ALONG_X, ALONG_Y = 1, 2, 4
NEAR = ((ALONG_X, ALONG_Y), (ALONG_Y, ALONG_X))
WIDE_LANES = (LANES, LANES + HALF)
FAR_FIRST = (6, 7, 4, 2, 5, 3, 1)


def flip(index, mask):
    core, x, y = index % 2, (index // 2) % 2, index // 4
    if mask & PEER:
        core = 1 - core
    if mask & ALONG_X:
        x = 1 - x
    if mask & ALONG_Y:
        y = 1 - y
    return y * 4 + x * 2 + core


def aligned(index, size):
    return pl.ds(pl.multiple_of(index * size, size), size)


def moments(first, second, total, clip):
    clipped = clip * total
    new_first = BETA_FIRST * first + (1.0 - BETA_FIRST) * clipped
    new_second = BETA_SECOND * second + (1.0 - BETA_SECOND) * (clipped * clipped)
    return new_first, new_second


def direction(new_first, new_second, weight):
    return (new_first * FIRST_SCALE) / (jnp.sqrt(new_second * SECOND_SCALE) + EPSILON) + WEIGHT_DECAY * weight


def fold(square):
    rows, columns = square.shape
    parts = [square[r:r + 8, k:k + LANES] for r in range(0, rows, 8) for k in range(0, columns, LANES)]
    while len(parts) > 1:
        parts = [a + b for a, b in zip(parts[::2], parts[1::2])] + ([parts[-1]] if len(parts) % 2 else [])
    return parts[0]


def add_all(values):
    return functools.reduce(lambda a, b: a + b, values)


def kernel(*refs):
    grads, weights, firsts, seconds = refs[0:4], refs[4:8], refs[8:12], refs[12:16]
    replicas, new_weights, new_firsts, new_seconds = refs[16:20], refs[20:24], refs[24:28], refs[28:32]
    (recv_attn, recv_mlp, recv_small, part_attn, part_mlp, part_small, last_attn, last_mlp, last_small,
     sum_attn, sum_mlp, sum_small, dir_attn, dir_mlp, early_weight, early_dir, vec_in, wide_in, small_out, all_small,
     vec_rows, vec_columns, vec_row, start_tiles, first_tiles, rest_tiles, row_acc,
     load_sems, sent, tile_sent, scatter_recv, small_recv, last_recv, tile_recv, own_recv, pass_recv, pair_recv,
     early_sent, early_recv, tail_recv, ready) = refs[32:]
    recvs, parts, lasts = (recv_attn, recv_mlp), (part_attn, part_mlp), (last_attn, last_mlp)
    me = lax.axis_index("data")
    core = me % 2

    def grad_chunk(half, owner, chunk):
        rows, columns = SHAPES[chunk]
        return grads[chunk].at[pl.ds(rows * half, rows), aligned(owner, columns)]

    def replica_chunk(half, owner, chunk):
        rows, columns = SHAPES[chunk]
        return replicas[chunk].at[pl.ds(rows * half, rows), aligned(owner, columns)]

    def replica_part(half, owner, first, last):
        rows, columns = SHAPES[ATTN]
        start = pl.multiple_of(owner * columns + first, LANES)
        return replicas[ATTN].at[pl.ds(rows * half, rows), pl.ds(start, last - first)]

    along_x, along_y = flip(me, ALONG_X), flip(me, ALONG_Y)
    small_near = (along_x * (1 - core) + along_y * core, along_y * (1 - core) + along_x * core)
    peer = flip(me, PEER)
    peer_next = flip(peer, ALONG_X) * (1 - core) + flip(peer, ALONG_Y) * core

    def send(source, target, send_sem, recv_sem, device):
        copy = pltpu.make_async_remote_copy(src_ref=source, dst_ref=target, send_sem=send_sem, recv_sem=recv_sem,
                                            device_id=(device,), device_id_type=MESH)
        copy.start()
        return copy

    def wait_bytes(ref, sem):
        pltpu.make_async_copy(ref, ref, sem).wait()

    barrier = pltpu.get_barrier_semaphore()

    def signal(semaphore, device):
        pl.semaphore_signal(semaphore, inc=1, device_id=(device,), device_id_type=MESH)

    signal(barrier, peer)

    @pl.when(core == 1)
    def _():
        for mask in (ALONG_X, ALONG_Y):
            for device in (flip(me, mask), flip(peer, mask)):
                signal(barrier, device)


    small_loads = [pltpu.make_async_copy(grads[2], wide_in, load_sems.at[2]),
                   pltpu.make_async_copy(grads[3], vec_in, load_sems.at[3])]
    for copy in small_loads:
        copy.start()
    for keep in range(2):
        for half in HALVES:
            for chunk in (MLP, ATTN):
                owner = me if keep else flip(me, NEAR[half][1])
                pltpu.make_async_copy(grad_chunk(half, owner, chunk), recvs[chunk].at[half, keep, 0],
                                      scatter_recv.at[half, keep, chunk]).start()
    state_loads = []
    for index, (source, target) in enumerate(((weights, new_weights), (firsts, new_firsts), (seconds, new_seconds))):
        for bank in range(4):
            copy = pltpu.make_async_copy(source[bank], target[bank], load_sems.at[bank if bank < 2 else 2 * index + bank + 2])
            copy.start()
            if bank >= 2:
                state_loads.append(copy)
    pl.semaphore_wait(barrier, 3)

    def scatter(keep, chunk, slots):
        for slot in slots:
            for half in HALVES:
                target = peer if slot == 0 else flip(me, NEAR[half][0]) // 2 * 2 + slot - 1
                owner = target if keep else flip(target, NEAR[half][1])
                send(grad_chunk(half, owner, chunk), recvs[chunk].at[half, keep, 1 if slot == 0 else 2 + core],
                     sent.at[0, chunk], scatter_recv.at[half, keep, chunk], target)

    for chunk in (MLP, ATTN):
        scatter(0, chunk, (2, 0))

    @pl.when(core == 1)
    def _():
        signal(ready, along_x)
        signal(ready, along_y)
        pl.semaphore_wait(ready, 2)
        signal(ready, peer)

    @pl.when(core == 0)
    def _():
        pl.semaphore_wait(ready, 1)

    for chunk in (MLP, ATTN):
        scatter(0, chunk, (1,))
    for copy in small_loads:
        copy.wait()
    vec_rows[...] = jnp.zeros_like(vec_rows)
    vec_rows[0:VEC, :] = vec_in[...].astype(jnp.float32)
    vec_columns[...] = vec_rows[...].T

    def small_message(wide, vec):
        pad = jnp.zeros((TALL, VEC_PAD - VEC - HALF), jnp.float32)
        return jnp.concatenate([vec[:, 0:LANES], wide, vec[:, LANES:VEC], pad], axis=1).astype(jnp.bfloat16)

    def small_parts(message):
        vec = jnp.concatenate([message[:, 0:LANES], message[:, WIDE_LANES[1]:HALF + VEC]], axis=1)
        return message[:, slice(*WIDE_LANES)], vec

    wide_grad = wide_in[...].astype(jnp.float32)
    for owner in range(8):
        small_out[owner] = small_message(
            wide_grad[:, HALF * owner:HALF * owner + HALF], vec_columns[TALL * owner:TALL * owner + TALL, 0:VEC])
    for keep in range(2):
        recv_small[keep, 0] = small_out[me if keep else small_near[1]]
        places = [(along_x // 2 * 2, ALONG_Y), (along_y // 2 * 2 + 1, ALONG_X)]
        targets = [(target, target if keep else flip(target, way), 2 + core) for target, way in places]
        for target, owner, slot in [*targets, (peer, peer if keep else peer_next, 1)]:
            send(small_out.at[owner], recv_small.at[keep, slot], sent.at[0, SMALL], small_recv.at[keep], target)
    for chunk in (MLP, ATTN):
        scatter(1, chunk, (1, 2, 0))

    row = lax.broadcasted_iota(jnp.int32, (LANES, LANES), 0)
    lane = lax.broadcasted_iota(jnp.int32, (LANES, LANES), 1)
    eye = row == lane
    sub = lax.broadcasted_iota(jnp.int32, (8, LANES), 0)

    def lanes_of(first, last):
        column = jnp.sum(row_acc[first:last, :], axis=1, keepdims=True)
        return jnp.sum(jnp.where(eye[first:last, :], column, 0.0), axis=0, keepdims=True)

    def vec_lanes(square):
        vec_row[...] = jnp.zeros_like(vec_row)
        vec_row[0:1, 0:VEC] = jnp.sum(square, axis=0, keepdims=True)
        return vec_row[0:1, 0:LANES], vec_row[0:1, LANES:VEC_PAD]

    def tile_of(rows):
        tile = jnp.zeros((8, LANES), jnp.float32)
        for index, value in enumerate(rows):
            tile = jnp.where(sub == index, value, tile)
        return tile

    def exchange(tiles, which, value):
        tiles[me] = value
        for mask in FAR_FIRST:
            send(tiles.at[me], tiles.at[me], tile_sent.at[which], tile_recv.at[which], flip(me, mask))

    def collect(tiles, which):
        wait_bytes(tiles.at[pl.ds(0, len(FAR_FIRST))], tile_recv.at[which])
        return add_all([tiles[index] for index in range(8)])

    def by_rows(first, groups, columns, step):
        def group(g, carry):
            def inner(j, acc):
                return acc + step((aligned(g, 8), aligned(j, STEP)))

            row_acc[pl.ds(pl.multiple_of(first + g * 8, 8), 8), :] = lax.fori_loop(
                0, columns // STEP, inner, jnp.zeros((8, LANES), jnp.float32))
            return carry

        lax.fori_loop(0, groups, group, 0)

    def square_of(ref):
        return lambda place: fold(ref[place] * ref[place])

    for buffer, sem in ((recv_attn, load_sems.at[ATTN]), (recv_mlp, load_sems.at[MLP])):
        wait_bytes(buffer.at[:, :, pl.ds(0, 3)], sem)
    for copy in state_loads:
        copy.wait()
    row_acc[...] = jnp.zeros_like(row_acc)
    by_rows(0, 8, ATTN_SHARD, square_of(new_weights[0]))
    by_rows(HALF, 4, MLP_SHARD, square_of(new_weights[1]))
    wide_weight, vec_weight = new_weights[2][...], new_weights[3][...]
    row_acc[96:112, 0:HALF] = wide_weight * wide_weight
    weight_lanes = lanes_of(0, LANES)
    weight_low, weight_high = vec_lanes(vec_weight * vec_weight)

    def by_blocks(shape, step, init):
        rows, columns = shape
        for r in range(0, rows, TALL):
            init = lax.fori_loop(0, columns // BLOCK, functools.partial(
                lambda first, j, carry: step((pl.ds(first, TALL), aligned(j, BLOCK)), carry), r), init)
        return init

    def gather_sum(half, keep, chunk):
        source, target = recvs[chunk].at[half, keep], ((sum_attn, sum_mlp) if keep else parts)[chunk].at[half]
        wait_bytes(source, scatter_recv.at[half, keep, chunk])

        def step(place, carry):
            value = [source[(slot, *place)].astype(jnp.float32) for slot in range(4)]
            target[place] = (value[0] + value[1]) + (value[2] + value[3])
            return carry

        by_blocks(SHAPES[chunk], step, 0)

    def gather_small(keep, target):
        wait_bytes(recv_small.at[keep, pl.ds(1, 3)], small_recv.at[keep])
        target[...] = add_all([recv_small[keep, slot].astype(jnp.float32) for slot in range(4)])

    last = {}
    for chunk in (MLP, ATTN):
        for half in HALVES:
            gather_sum(half, 0, chunk)
    gather_small(0, part_small)
    last_small_copy = send(part_small, last_small, sent.at[0, SMALL], last_recv.at[0, SMALL], small_near[1])
    for chunk in (MLP, ATTN):
        for half in HALVES:
            last[half, chunk] = send(parts[chunk].at[half], lasts[chunk].at[half], sent.at[0, chunk],
                                     last_recv.at[half, chunk], flip(me, NEAR[half][1]))
    for chunk in (MLP, ATTN):
        for half in HALVES:
            gather_sum(half, 1, chunk)
    gather_small(1, sum_small)

    last_small_copy.wait_recv()
    wide_total, vec_total = small_parts(sum_small[...] + last_small[...])
    square = fold(jnp.concatenate([wide_total * wide_total, jnp.zeros((TALL, HALF), jnp.float32)], axis=1))
    low, high = vec_lanes(vec_total * vec_total)
    square = square + tile_of([low, high])
    for chunk in (MLP, ATTN):
        for half in HALVES:
            last[half, chunk].wait_recv()
            total, rest = (sum_attn, sum_mlp)[chunk].at[half], lasts[chunk].at[half]

            def step(place, acc):
                value = total[place] + rest[place]
                total[place] = value
                return acc + fold(value * value)

            square = by_blocks(SHAPES[chunk], step, square)

    exchange(start_tiles, 0, tile_of([weight_lanes, weight_low, weight_high, jnp.sum(square, axis=0, keepdims=True)]))
    late_rows = pl.ds(FIRST, FIRST)
    early_columns = pl.ds(0, EARLY)

    def send_early(kind, source, buffer):
        for way, mask in enumerate((ALONG_X, ALONG_Y)):
            send(source, buffer.at[way], early_sent.at[kind], early_recv.at[kind, way], flip(me, mask))

    send_early(0, new_weights[ATTN].at[late_rows, early_columns], early_weight)
    start = collect(start_tiles, 0)
    square = jnp.sum(jnp.sum(start[3:4, :], axis=1, keepdims=True), axis=0, keepdims=True)
    clip = jnp.minimum(1.0, (8.0 * MAX_NORM) / jnp.sqrt(jnp.broadcast_to(square, (8, LANES)))) * 0.125
    clip_block = jnp.concatenate([clip] * (STEP // LANES), axis=1)
    weight_norms = LEARN_RATE * jnp.sqrt(start)

    sums, directions = (sum_attn, sum_mlp), (dir_attn, dir_mlp)

    def update(bank, half):
        rows = SHAPES[bank][0]

        def step(place):
            state = (pl.ds(pl.multiple_of(half * rows + place[0].start, 8), 8), place[1])
            new_first, new_second = moments(
                new_firsts[bank][state], new_seconds[bank][state], sums[bank].at[half][place], clip_block)
            value = direction(new_first, new_second, new_weights[bank][state])
            directions[bank].at[half][place] = value
            return fold(value * value)

        by_rows(HALF * bank + half * rows, rows // 8, SHAPES[bank][1], step)

    def store_moments(bank, half):
        rows = SHAPES[bank][0]

        def step(place, carry):
            state = (pl.ds(half * rows + place[0].start, TALL), place[1])
            clip_wide = jnp.concatenate([clip_block[:, 0:BLOCK]] * 2, axis=0)
            new_first, new_second = moments(
                new_firsts[bank][state], new_seconds[bank][state], sums[bank].at[half][place], clip_wide)
            new_firsts[bank][state] = new_first
            new_seconds[bank][state] = new_second
            return carry

        by_blocks(SHAPES[bank], step, 0)

    def update_small(bank, total, weight):
        new_first, new_second = moments(new_firsts[bank][...], new_seconds[bank][...], total, clip[0:1, 0:1])
        new_firsts[bank][...] = new_first
        new_seconds[bank][...] = new_second
        return direction(new_first, new_second, weight)

    update(ATTN, 0)
    exchange(first_tiles, 1, tile_of([lanes_of(0, FIRST)]))
    update(ATTN, 1)
    send_early(1, dir_attn.at[1, :, early_columns], early_dir)
    for half in HALVES:
        update(MLP, half)
    wide_dir = update_small(2, wide_total, wide_weight)
    vec_dir = update_small(3, vec_total, vec_weight)
    row_acc[96:112, 0:HALF] = wide_dir * wide_dir
    exchange(rest_tiles, 2, tile_of([lanes_of(FIRST, LANES), *vec_lanes(vec_dir * vec_dir)]))
    for bank in (ATTN, MLP):
        for half in HALVES:
            store_moments(bank, half)

    own_copies = {}

    def send_own(half, chunk, way):
        place = all_small.at[me] if chunk == SMALL else replica_chunk(half, me, chunk)
        if (half, chunk) == (1, ATTN) and way:
            place = replica_part(1, me, EARLY, ATTN_SHARD)
        recv_sem = own_recv.at[half, chunk, way - 1] if way else pair_recv.at[chunk]
        own_copies[half, chunk, way] = send(place, place, sent.at[1, chunk], recv_sem, flip(me, (PEER, ALONG_X, ALONG_Y)[way]))

    def spread_ratio(first, last, ratio):
        row_acc[first:last, :] = jnp.broadcast_to(
            jnp.sum(jnp.where(eye[first:last, :], ratio[0:1, :], 0.0), axis=1, keepdims=True), (last - first, LANES))

    def form_weights(bank, half, owner, shape, weight, direct, result):
        rows = SHAPES[bank][0]

        def step(place, carry):
            first = half * rows + place[0].start
            scale = jnp.concatenate([row_acc[HALF * bank + first:HALF * bank + first + TALL, :]] * (BLOCK // LANES), axis=1)
            value = weight[place] - scale * direct[place]
            if result is not None:
                result[place] = value
            target = pl.ds(pl.multiple_of(owner * SHAPES[bank][1] + place[1].start, BLOCK), BLOCK)
            replicas[bank][pl.ds(first, TALL), target] = value.astype(jnp.bfloat16)
            return carry

        by_blocks(shape, step, 0)

    def new_weight(bank, half, ways):
        rows = SHAPES[bank][0]
        mine = new_weights[bank].at[pl.ds(half * rows, rows)]
        form_weights(bank, half, me, SHAPES[bank], mine, directions[bank].at[half], mine)
        for way in ways:
            send_own(half, bank, way)

    spread_ratio(0, FIRST, weight_norms / jnp.sqrt(collect(first_tiles, 1)))
    new_weight(ATTN, 0, (1, 2, 0))
    ratio = weight_norms / jnp.sqrt(collect(rest_tiles, 2))
    spread_ratio(FIRST, LANES, ratio)
    wait_bytes(early_weight, early_sent.at[0])
    new_weight(ATTN, 1, (2, 0))
    for half in HALVES:
        new_weight(MLP, half, (1 + half, 0))
    value = wide_weight - row_acc[96:112, 0:HALF] * wide_dir
    new_weights[2][...] = value
    wide_value = value
    vec_row[0:1, 0:LANES] = ratio[1:2, :]
    vec_row[0:1, LANES:VEC_PAD] = ratio[2:3, :]
    value = vec_weight - vec_row[0:1, 0:VEC] * vec_dir
    new_weights[3][...] = value
    all_small[me] = small_message(wide_value, value)
    for way in (1, 2, 0):
        send_own(0, SMALL, way)
    send_own(1, ATTN, 1)
    for half in HALVES:
        send_own(half, MLP, 2 - half)

    for way, owner in enumerate((along_x, along_y)):
        for kind, buffer in enumerate((early_weight, early_dir)):
            wait_bytes(buffer.at[way], early_recv.at[kind, way])
        form_weights(ATTN, 1, owner, (FIRST, EARLY), early_weight.at[way], early_dir.at[way], None)

    def send_pair(place, chunk):
        send(place, place, sent.at[1, chunk], pair_recv.at[chunk], peer)

    for way in (1, 2):
        own_copies[0, SMALL, way].wait_recv()
    place = all_small.at[small_near[0]]
    passed_small = send(place, place, sent.at[1, SMALL], pass_recv.at[0, SMALL], small_near[1])
    for owner in small_near:
        send_pair(all_small.at[owner], SMALL)
    passed = {}
    for chunk in (MLP, ATTN):
        for half in HALVES:
            own_copies[half, chunk, 1 + half].wait_recv()
            owner, target = flip(me, NEAR[half][0]), flip(me, NEAR[half][1])
            place = replica_chunk(half, owner, chunk)
            send_pair(place, chunk)
            if chunk == ATTN:
                place = replica_part(half, owner, 0, ATTN_SHARD - TAIL)
            passed[half, chunk] = send(place, place, sent.at[1, chunk], pass_recv.at[half, chunk], target)
    for target_core in (0, 1):
        for half in HALVES:
            place = replica_part(half, flip(me, NEAR[half][0]), ATTN_SHARD - TAIL, ATTN_SHARD)
            send(place, place, sent.at[1, ATTN], tail_recv, flip(me, NEAR[half][1] + (PEER if target_core else 0)))
    for chunk in BIG:
        for half in HALVES:
            own_copies[half, chunk, 2 - half].wait_recv()
            send_pair(replica_chunk(half, flip(me, NEAR[half][1]), chunk), chunk)
    far = flip(me, ALONG_X + ALONG_Y)
    passed_small.wait_recv()
    send_pair(all_small.at[far], SMALL)
    wait_bytes(all_small.at[pl.ds(0, 4)], pair_recv.at[SMALL])
    wides, vecs = zip(*(small_parts(all_small[owner].astype(jnp.float32)) for owner in range(8)))
    replicas[2][...] = jnp.concatenate(wides, axis=1).astype(jnp.bfloat16)
    for owner in range(8):
        vec_columns[TALL * owner:TALL * owner + TALL, 0:VEC] = vecs[owner]
    vec_rows[...] = vec_columns[...].T
    replicas[3][...] = vec_rows[0:VEC, :].astype(jnp.bfloat16)
    wait_bytes(all_small, sent.at[0, SMALL])
    wait_bytes(all_small.at[pl.ds(0, len(FAR_FIRST))], sent.at[1, SMALL])
    wait_bytes(early_dir, early_sent.at[1])
    for which, tiles in enumerate((start_tiles, first_tiles, rest_tiles)):
        wait_bytes(tiles.at[pl.ds(0, len(FAR_FIRST))], tile_sent.at[which])
    for bank in BIG:
        wait_bytes(replicas[bank], sent.at[0, bank])
    for chunk in (MLP, ATTN):
        for half in HALVES:
            passed[half, chunk].wait_recv()
            send_pair(replica_part(half, far, 0, ATTN_SHARD - TAIL) if chunk == ATTN else replica_chunk(half, far, chunk), chunk)
    for bank, received, gone in ((MLP, 0, 0), (ATTN, TAIL, EARLY)):
        columns = SHAPES[bank][1]
        wait_bytes(replicas[bank].at[:, pl.ds(0, 4 * columns - received)], pair_recv.at[bank])
        wait_bytes(replicas[bank].at[:, pl.ds(0, len(FAR_FIRST) * columns - gone)], sent.at[1, bank])
    wait_bytes(replicas[ATTN].at[:, pl.ds(0, 2 * TAIL)], tail_recv)


def write_out(*refs):
    count = (len(refs) - 1) // 2
    largest_first = sorted(range(count), key=lambda k: -refs[k].size)
    copies = [pltpu.make_async_copy(refs[k], refs[count + k], refs[-1]) for k in largest_first]
    for copy in copies:
        copy.start()
    for copy in copies:
        copy.wait()


def solution(mesh):
    shards = [jax.ShapeDtypeStruct(shape, jnp.float32) for shape in SHARDS]
    shapes = [jax.ShapeDtypeStruct(shape, jnp.bfloat16) for shape in zip(ROWS, LENGTHS)] + shards * 3
    f32, bf16 = jnp.float32, jnp.bfloat16
    dma = pltpu.SemaphoreType.DMA
    attn, mlp = SHAPES

    def sums(*lead):
        return [pltpu.VMEM((*lead, *attn), f32), pltpu.VMEM((*lead, *mlp), f32)]

    small = (TALL, VEC_PAD)
    scratch = [
        pltpu.VMEM((2, 2, 4, *attn), bf16), pltpu.VMEM((2, 2, 4, *mlp), bf16), pltpu.VMEM((2, 4, *small), bf16),
        *sums(2), pltpu.VMEM(small, f32), *sums(2), pltpu.VMEM(small, f32), *sums(2), pltpu.VMEM(small, f32), *sums(2),
        *[pltpu.VMEM((2, FIRST, EARLY), f32)] * 2, pltpu.VMEM((VEC, LANES), bf16), pltpu.VMEM((TALL, WIDE), bf16), pltpu.VMEM((8, *small), bf16),
        pltpu.VMEM((8, *small), bf16),
        pltpu.VMEM((VEC_PAD, LANES), f32), pltpu.VMEM((LANES, VEC_PAD), f32), pltpu.VMEM((8, VEC_PAD), f32),
        *[pltpu.VMEM((8, 8, LANES), f32)] * 3, pltpu.VMEM((LANES, LANES), f32),
        dma((10,)), dma((2, 3)), dma((3,)), dma((2, 2, 2)), dma((2,)), dma((2, 3)), dma((3,)), dma((2, 3, 2)), dma((2, 3)),
        dma((3,)), dma((2,)), dma((2, 2)), dma, pltpu.SemaphoreType.REGULAR,
    ]
    count = len(shapes)
    anywhere = [pl.BlockSpec(memory_space=pl.ANY)] * count
    step = pl.pallas_call(
        kernel,
        out_shape=[pltpu.VMEM(shape.shape, shape.dtype) for shape in shapes],
        in_specs=anywhere,
        out_specs=[pl.BlockSpec(memory_space=pltpu.VMEM)] * count,
        scratch_shapes=scratch,
        compiler_params=pltpu.CompilerParams(collective_id=0, has_side_effects=True, vmem_limit_bytes=36 * MIB),
        name="lamb_step",
    )
    finish = pl.pallas_call(
        write_out,
        out_shape=shapes,
        in_specs=anywhere,
        out_specs=anywhere,
        scratch_shapes=[dma],
        compiler_params=pltpu.CompilerParams(vmem_limit_bytes=MIB),
        name="write_out",
    )

    def local_step(*banks):
        banks = [bank[0] for bank in banks[:4]] + [bank.T if bank.shape == (VEC, TALL) else bank for bank in banks[4:]]
        banks = [pltpu.with_memory_space_constraint(bank, pltpu.HBM) for bank in banks]
        results = finish(*step(*banks))
        return tuple(value.T if value.shape == (TALL, VEC) else value for value in results)

    grad_spec, shard_spec, full_spec = P("data", None, None), P(None, "data"), P(None, None)
    return jax.shard_map(local_step, mesh=mesh, in_specs=(grad_spec,) * 4 + (shard_spec,) * 12,
                         out_specs=(full_spec,) * 4 + (shard_spec,) * 12, check_vma=False)
```

```python
import functools

import jax
import jax.numpy as jnp
from jax import lax
from jax.experimental import pallas as pl
from jax.experimental.pallas import tpu as pltpu
from jax.sharding import PartitionSpec as P

STEP_NUMBER = 10
LEARN_RATE = 0.04
BETA_FIRST = 0.9
BETA_SECOND = 0.999
EPSILON = 1e-6
WEIGHT_DECAY = 0.01
MAX_NORM = 1.0
FIRST_SCALE = 1.0 / (1.0 - BETA_FIRST ** STEP_NUMBER)
SECOND_SCALE = 1.0 / (1.0 - BETA_SECOND ** STEP_NUMBER)

MESH = pl.DeviceIdType.MESH
LANES = 128
TALL = 16
HALF = 64
FIRST = 32
EARLY = 1024
VEC = 146
VEC_PAD = 256
ATTN_SHARD = 2048
MLP_SHARD = 8192
STEP = 2048
BLOCK = 1024
WIDE = 512
TAIL = 640
MIB = 2 ** 20
ROWS = (HALF, 32, TALL, VEC)
LENGTHS = (16384, 65536, WIDE, LANES)
SHARDS = ((HALF, ATTN_SHARD), (32, MLP_SHARD), (TALL, HALF), (TALL, VEC))
ATTN, MLP, SMALL = range(3)
BIG = (ATTN, MLP)
HALVES = range(2)
SHAPES = ((32, ATTN_SHARD), (TALL, MLP_SHARD))
PEER, ALONG_X, ALONG_Y = 1, 2, 4
NEAR = ((ALONG_X, ALONG_Y), (ALONG_Y, ALONG_X))
WIDE_LANES = (LANES, LANES + HALF)
FAR_FIRST = (6, 7, 4, 2, 5, 3, 1)


def flip(index, mask):
    core, x, y = index % 2, (index // 2) % 2, index // 4
    if mask & PEER:
        core = 1 - core
    if mask & ALONG_X:
        x = 1 - x
    if mask & ALONG_Y:
        y = 1 - y
    return y * 4 + x * 2 + core


def aligned(index, size):
    return pl.ds(pl.multiple_of(index * size, size), size)


def moments(first, second, total, clip):
    clipped = clip * total
    new_first = BETA_FIRST * first + (1.0 - BETA_FIRST) * clipped
    new_second = BETA_SECOND * second + (1.0 - BETA_SECOND) * (clipped * clipped)
    return new_first, new_second


def direction(new_first, new_second, weight):
    return (new_first * FIRST_SCALE) / (jnp.sqrt(new_second * SECOND_SCALE) + EPSILON) + WEIGHT_DECAY * weight


def fold(square):
    rows, columns = square.shape
    parts = [square[r:r + 8, k:k + LANES] for r in range(0, rows, 8) for k in range(0, columns, LANES)]
    while len(parts) > 1:
        parts = [a + b for a, b in zip(parts[::2], parts[1::2])] + ([parts[-1]] if len(parts) % 2 else [])
    return parts[0]


def add_all(values):
    return functools.reduce(lambda a, b: a + b, values)


def kernel(*refs):
    grads, weights, firsts, seconds = refs[0:4], refs[4:8], refs[8:12], refs[12:16]
    replicas, new_weights, new_firsts, new_seconds = refs[16:20], refs[20:24], refs[24:28], refs[28:32]
    (recv_attn, recv_mlp, recv_small, part_attn, part_mlp, part_small, last_attn, last_mlp, last_small,
     sum_attn, sum_mlp, sum_small, dir_attn, dir_mlp, early, state_wide, state_vec, vec_in, wide_in, small_out, all_small,
     vec_rows, vec_columns, vec_row, all_tiles, row_acc,
     load_sems, sent, tile_sent, scatter_recv, small_recv, last_recv, tile_recv, own_recv, own_small, pass_recv, pair_recv,
     early_sent, early_recv, tail_recv, ready) = refs[32:]
    recvs, parts, lasts = (recv_attn, recv_mlp), (part_attn, part_mlp), (last_attn, last_mlp)
    me = lax.axis_index("data")
    core = me % 2

    def grad_chunk(half, owner, chunk):
        rows, columns = SHAPES[chunk]
        return grads[chunk].at[pl.ds(rows * half, rows), aligned(owner, columns)]

    def replica_chunk(half, owner, chunk):
        rows, columns = SHAPES[chunk]
        return replicas[chunk].at[pl.ds(rows * half, rows), aligned(owner, columns)]

    def replica_part(half, owner, first, last):
        rows, columns = SHAPES[ATTN]
        start = pl.multiple_of(owner * columns + first, LANES)
        return replicas[ATTN].at[pl.ds(rows * half, rows), pl.ds(start, last - first)]

    along_x, along_y = flip(me, ALONG_X), flip(me, ALONG_Y)
    small_near = (along_x * (1 - core) + along_y * core, along_y * (1 - core) + along_x * core)
    peer = flip(me, PEER)
    peer_next = flip(peer, ALONG_X) * (1 - core) + flip(peer, ALONG_Y) * core

    def send(source, target, send_sem, recv_sem, device):
        copy = pltpu.make_async_remote_copy(src_ref=source, dst_ref=target, send_sem=send_sem, recv_sem=recv_sem,
                                            device_id=(device,), device_id_type=MESH)
        copy.start()
        return copy

    def wait_bytes(ref, sem):
        pltpu.make_async_copy(ref, ref, sem).wait()

    barrier = pltpu.get_barrier_semaphore()

    def signal(semaphore, device):
        pl.semaphore_signal(semaphore, inc=1, device_id=(device,), device_id_type=MESH)

    signal(barrier, peer)

    @pl.when(core == 1)
    def _():
        for mask in (ALONG_X, ALONG_Y):
            for device in (flip(me, mask), flip(peer, mask)):
                signal(barrier, device)


    small_loads = [pltpu.make_async_copy(grads[2], wide_in, load_sems.at[4]),
                   pltpu.make_async_copy(grads[3], vec_in, load_sems.at[5])]
    for copy in small_loads:
        copy.start()
    for keep in range(2):
        for half in HALVES:
            for chunk in (MLP, ATTN):
                owner = me if keep else flip(me, NEAR[half][1])
                pltpu.make_async_copy(grad_chunk(half, owner, chunk), recvs[chunk].at[half, keep, 0],
                                      scatter_recv.at[keep, chunk]).start()
    for index, (source, target) in enumerate(((weights, new_weights), (firsts, new_firsts), (seconds, new_seconds))):
        for bank, place in enumerate((target[0], target[1], state_wide.at[index], state_vec.at[index])):
            pltpu.make_async_copy(source[bank], place, load_sems.at[bank]).start()
    pl.semaphore_wait(barrier, 3)

    def scatter(keep, chunk, slots):
        for slot in slots:
            for half in HALVES:
                target = peer if slot == 0 else flip(me, NEAR[half][0]) // 2 * 2 + slot - 1
                owner = target if keep else flip(target, NEAR[half][1])
                send(grad_chunk(half, owner, chunk), recvs[chunk].at[half, keep, 1 if slot == 0 else 2 + core],
                     sent.at[0, chunk], scatter_recv.at[keep, chunk], target)

    for chunk in (MLP, ATTN):
        scatter(0, chunk, (2, 0))

    @pl.when(core == 1)
    def _():
        signal(ready, along_x)
        signal(ready, along_y)
        pl.semaphore_wait(ready, 2)
        signal(ready, peer)

    @pl.when(core == 0)
    def _():
        pl.semaphore_wait(ready, 1)

    for chunk in (MLP, ATTN):
        scatter(0, chunk, (1,))
    for copy in small_loads:
        copy.wait()
    vec_rows[...] = jnp.zeros_like(vec_rows)
    vec_rows[0:VEC, :] = vec_in[...].astype(jnp.float32)
    vec_columns[...] = vec_rows[...].T

    def small_message(wide, vec):
        pad = jnp.zeros((TALL, VEC_PAD - VEC - HALF), jnp.float32)
        return jnp.concatenate([vec[:, 0:LANES], wide, vec[:, LANES:VEC], pad], axis=1).astype(jnp.bfloat16)

    def small_parts(message):
        vec = jnp.concatenate([message[:, 0:LANES], message[:, WIDE_LANES[1]:HALF + VEC]], axis=1)
        return message[:, slice(*WIDE_LANES)], vec

    wide_grad = wide_in[...].astype(jnp.float32)
    for owner in range(8):
        small_out[owner] = small_message(
            wide_grad[:, HALF * owner:HALF * owner + HALF], vec_columns[TALL * owner:TALL * owner + TALL, 0:VEC])
    for keep in range(2):
        recv_small[keep, 0] = small_out[me if keep else small_near[1]]
        places = [(along_x // 2 * 2, ALONG_Y), (along_y // 2 * 2 + 1, ALONG_X)]
        targets = [(target, target if keep else flip(target, way), 2 + core) for target, way in places]
        for target, owner, slot in [*targets, (peer, peer if keep else peer_next, 1)]:
            send(small_out.at[owner], recv_small.at[keep, slot], sent.at[0, SMALL], small_recv.at[keep], target)
    for chunk in (MLP, ATTN):
        scatter(1, chunk, (1, 2, 0))

    row = lax.broadcasted_iota(jnp.int32, (LANES, LANES), 0)
    lane = lax.broadcasted_iota(jnp.int32, (LANES, LANES), 1)
    eye = row == lane
    sub = lax.broadcasted_iota(jnp.int32, (8, LANES), 0)

    def lanes_of(first, last):
        column = jnp.sum(row_acc[first:last, :], axis=1, keepdims=True)
        return jnp.sum(jnp.where(eye[first:last, :], column, 0.0), axis=0, keepdims=True)

    def vec_lanes(square):
        vec_row[...] = jnp.zeros_like(vec_row)
        vec_row[0:1, 0:VEC] = jnp.sum(square, axis=0, keepdims=True)
        return vec_row[0:1, 0:LANES], vec_row[0:1, LANES:VEC_PAD]

    def tile_of(rows):
        tile = jnp.zeros((8, LANES), jnp.float32)
        for index, value in enumerate(rows):
            tile = jnp.where(sub == index, value, tile)
        return tile

    def exchange(which, value):
        all_tiles[which, me] = value
        place = all_tiles.at[which, me]
        for mask in FAR_FIRST:
            send(place, place, tile_sent, tile_recv.at[which], flip(me, mask))

    def collect(which):
        wait_bytes(all_tiles.at[which, pl.ds(0, len(FAR_FIRST))], tile_recv.at[which])
        return add_all([all_tiles[which, index] for index in range(8)])

    def by_rows(first, groups, columns, step):
        def group(g, carry):
            def inner(j, acc):
                return acc + step((aligned(g, 8), aligned(j, STEP)))

            row_acc[pl.ds(pl.multiple_of(first + g * 8, 8), 8), :] = lax.fori_loop(
                0, columns // STEP, inner, jnp.zeros((8, LANES), jnp.float32))
            return carry

        lax.fori_loop(0, groups, group, 0)

    def square_of(ref):
        return lambda place: fold(ref[place] * ref[place])

    for buffer, sem in ((recv_attn, load_sems.at[ATTN]), (recv_mlp, load_sems.at[MLP])):
        wait_bytes(buffer.at[:, :, pl.ds(0, 3)], sem)
    for bank, buffer in ((2, state_wide), (3, state_vec)):
        wait_bytes(buffer, load_sems.at[bank])
    row_acc[...] = jnp.zeros_like(row_acc)
    by_rows(0, 8, ATTN_SHARD, square_of(new_weights[0]))
    by_rows(HALF, 4, MLP_SHARD, square_of(new_weights[1]))
    wide_weight, vec_weight = state_wide[0], state_vec[0]
    row_acc[96:112, 0:HALF] = wide_weight * wide_weight
    weight_lanes = lanes_of(0, LANES)
    weight_low, weight_high = vec_lanes(vec_weight * vec_weight)

    def by_blocks(shape, step, init):
        rows, columns = shape
        for r in range(0, rows, TALL):
            init = lax.fori_loop(0, columns // BLOCK, functools.partial(
                lambda first, j, carry: step((pl.ds(first, TALL), aligned(j, BLOCK)), carry), r), init)
        return init

    def gather_sum(keep, chunk):
        wait_bytes(recvs[chunk].at[:, keep], scatter_recv.at[keep, chunk])
        for half in HALVES:
            source, target = recvs[chunk].at[half, keep], ((sum_attn, sum_mlp) if keep else parts)[chunk].at[half]

            def step(place, carry):
                value = [source[(slot, *place)].astype(jnp.float32) for slot in range(4)]
                target[place] = (value[0] + value[1]) + (value[2] + value[3])
                return carry

            by_blocks(SHAPES[chunk], step, 0)

    def gather_small(keep, target):
        wait_bytes(recv_small.at[keep, pl.ds(1, 3)], small_recv.at[keep])
        target[...] = add_all([recv_small[keep, slot].astype(jnp.float32) for slot in range(4)])

    for chunk in (MLP, ATTN):
        gather_sum(0, chunk)
    gather_small(0, part_small)
    send(part_small, last_small, sent.at[0, SMALL], last_recv.at[SMALL], small_near[1])
    for chunk in (MLP, ATTN):
        for half in HALVES:
            send(parts[chunk].at[half], lasts[chunk].at[half], sent.at[0, chunk], last_recv.at[chunk], flip(me, NEAR[half][1]))
    for chunk in (MLP, ATTN):
        gather_sum(1, chunk)
    gather_small(1, sum_small)

    wait_bytes(last_small, last_recv.at[SMALL])
    wide_total, vec_total = small_parts(sum_small[...] + last_small[...])
    square = fold(jnp.concatenate([wide_total * wide_total, jnp.zeros((TALL, HALF), jnp.float32)], axis=1))
    low, high = vec_lanes(vec_total * vec_total)
    square = square + tile_of([low, high])
    for chunk in (MLP, ATTN):
        wait_bytes(lasts[chunk], last_recv.at[chunk])
        for half in HALVES:
            total, rest = (sum_attn, sum_mlp)[chunk].at[half], lasts[chunk].at[half]

            def step(place, acc):
                value = total[place] + rest[place]
                total[place] = value
                return acc + fold(value * value)

            square = by_blocks(SHAPES[chunk], step, square)

    exchange(0, tile_of([weight_lanes, weight_low, weight_high, jnp.sum(square, axis=0, keepdims=True)]))
    late_rows = pl.ds(FIRST, FIRST)
    early_columns = pl.ds(0, EARLY)

    def send_early(kind, source):
        for way, mask in enumerate((ALONG_X, ALONG_Y)):
            send(source, early.at[kind, way], early_sent.at[kind], early_recv, flip(me, mask))

    send_early(0, new_weights[ATTN].at[late_rows, early_columns])
    start = collect(0)
    square = jnp.sum(jnp.sum(start[3:4, :], axis=1, keepdims=True), axis=0, keepdims=True)
    clip = jnp.minimum(1.0, (8.0 * MAX_NORM) / jnp.sqrt(jnp.broadcast_to(square, (8, LANES)))) * 0.125
    clip_block = jnp.concatenate([clip] * (STEP // LANES), axis=1)
    weight_norms = LEARN_RATE * jnp.sqrt(start)

    sums, directions = (sum_attn, sum_mlp), (dir_attn, dir_mlp)

    def update(bank, half):
        rows = SHAPES[bank][0]

        def step(place):
            state = (pl.ds(pl.multiple_of(half * rows + place[0].start, 8), 8), place[1])
            new_first, new_second = moments(
                new_firsts[bank][state], new_seconds[bank][state], sums[bank].at[half][place], clip_block)
            value = direction(new_first, new_second, new_weights[bank][state])
            directions[bank].at[half][place] = value
            return fold(value * value)

        by_rows(HALF * bank + half * rows, rows // 8, SHAPES[bank][1], step)

    def store_moments(bank, half):
        rows = SHAPES[bank][0]

        def step(place, carry):
            state = (pl.ds(half * rows + place[0].start, TALL), place[1])
            clip_wide = jnp.concatenate([clip_block[:, 0:BLOCK]] * 2, axis=0)
            new_first, new_second = moments(
                new_firsts[bank][state], new_seconds[bank][state], sums[bank].at[half][place], clip_wide)
            new_firsts[bank][state] = new_first
            new_seconds[bank][state] = new_second
            return carry

        by_blocks(SHAPES[bank], step, 0)

    def update_small(bank, total, state):
        new_first, new_second = moments(state[1], state[2], total, clip[0:1, 0:1])
        new_firsts[bank][...] = new_first
        new_seconds[bank][...] = new_second
        return direction(new_first, new_second, state[0])

    update(ATTN, 0)
    exchange(1, tile_of([lanes_of(0, FIRST)]))
    update(ATTN, 1)
    send_early(1, dir_attn.at[1, :, early_columns])
    for half in HALVES:
        update(MLP, half)
    wide_dir = update_small(2, wide_total, state_wide)
    vec_dir = update_small(3, vec_total, state_vec)
    row_acc[96:112, 0:HALF] = wide_dir * wide_dir
    exchange(2, tile_of([lanes_of(FIRST, LANES), *vec_lanes(vec_dir * vec_dir)]))
    for bank in (ATTN, MLP):
        for half in HALVES:
            store_moments(bank, half)

    def send_own(half, chunk, way):
        place = all_small.at[me] if chunk == SMALL else replica_chunk(half, me, chunk)
        if (half, chunk) == (1, ATTN) and way:
            place = replica_part(1, me, EARLY, ATTN_SHARD)
        recv_sem = pair_recv.at[chunk] if not way else own_small if chunk == SMALL else own_recv.at[(way - 1 + half) % 2, chunk]
        send(place, place, sent.at[1, chunk], recv_sem, flip(me, (PEER, ALONG_X, ALONG_Y)[way]))

    def wait_own(kind, chunk):
        columns = SHAPES[chunk][1] - (EARLY // 2 if chunk == ATTN else 0)
        wait_bytes(replicas[chunk].at[:, pl.ds(0, columns)], own_recv.at[kind, chunk])

    def spread_ratio(first, last, ratio):
        row_acc[first:last, :] = jnp.broadcast_to(
            jnp.sum(jnp.where(eye[first:last, :], ratio[0:1, :], 0.0), axis=1, keepdims=True), (last - first, LANES))

    def form_weights(bank, half, owner, shape, weight, direct, result):
        rows = SHAPES[bank][0]

        def step(place, carry):
            first = half * rows + place[0].start
            scale = jnp.concatenate([row_acc[HALF * bank + first:HALF * bank + first + TALL, :]] * (BLOCK // LANES), axis=1)
            value = weight[place] - scale * direct[place]
            if result is not None:
                result[place] = value
            target = pl.ds(pl.multiple_of(owner * SHAPES[bank][1] + place[1].start, BLOCK), BLOCK)
            replicas[bank][pl.ds(first, TALL), target] = value.astype(jnp.bfloat16)
            return carry

        by_blocks(shape, step, 0)

    def new_weight(bank, half, ways):
        rows = SHAPES[bank][0]
        mine = new_weights[bank].at[pl.ds(half * rows, rows)]
        form_weights(bank, half, me, SHAPES[bank], mine, directions[bank].at[half], mine)
        for way in ways:
            send_own(half, bank, way)

    spread_ratio(0, FIRST, weight_norms / jnp.sqrt(collect(1)))
    new_weight(ATTN, 0, (1, 2, 0))
    ratio = weight_norms / jnp.sqrt(collect(2))
    spread_ratio(FIRST, LANES, ratio)
    wait_bytes(early.at[0], early_sent.at[0])
    new_weight(ATTN, 1, (2, 0))
    for half in HALVES:
        new_weight(MLP, half, (1 + half, 0))
    value = wide_weight - row_acc[96:112, 0:HALF] * wide_dir
    new_weights[2][...] = value
    wide_value = value
    vec_row[0:1, 0:LANES] = ratio[1:2, :]
    vec_row[0:1, LANES:VEC_PAD] = ratio[2:3, :]
    value = vec_weight - vec_row[0:1, 0:VEC] * vec_dir
    new_weights[3][...] = value
    all_small[me] = small_message(wide_value, value)
    for way in (1, 2, 0):
        send_own(0, SMALL, way)
    send_own(1, ATTN, 1)
    for half in HALVES:
        send_own(half, MLP, 2 - half)

    wait_bytes(early, early_recv)
    for way, owner in enumerate((along_x, along_y)):
        form_weights(ATTN, 1, owner, (FIRST, EARLY), early.at[0, way], early.at[1, way], None)

    def send_pair(place, chunk):
        send(place, place, sent.at[1, chunk], pair_recv.at[chunk], peer)

    wait_bytes(all_small.at[pl.ds(0, 2)], own_small)
    place = all_small.at[small_near[0]]
    send(place, place, sent.at[1, SMALL], pass_recv.at[SMALL], small_near[1])
    for owner in small_near:
        send_pair(all_small.at[owner], SMALL)
    for chunk in (MLP, ATTN):
        wait_own(0, chunk)
        for half in HALVES:
            owner, target = flip(me, NEAR[half][0]), flip(me, NEAR[half][1])
            place = replica_chunk(half, owner, chunk)
            send_pair(place, chunk)
            if chunk == ATTN:
                place = replica_part(half, owner, 0, ATTN_SHARD - TAIL)
            send(place, place, sent.at[1, chunk], pass_recv.at[chunk], target)
    for target_core in (0, 1):
        for half in HALVES:
            place = replica_part(half, flip(me, NEAR[half][0]), ATTN_SHARD - TAIL, ATTN_SHARD)
            send(place, place, sent.at[1, ATTN], tail_recv, flip(me, NEAR[half][1] + (PEER if target_core else 0)))
    for chunk in BIG:
        wait_own(1, chunk)
        for half in HALVES:
            send_pair(replica_chunk(half, flip(me, NEAR[half][1]), chunk), chunk)
    far = flip(me, ALONG_X + ALONG_Y)
    wait_bytes(all_small.at[pl.ds(0, 1)], pass_recv.at[SMALL])
    send_pair(all_small.at[far], SMALL)
    wait_bytes(all_small.at[pl.ds(0, 4)], pair_recv.at[SMALL])
    wides, vecs = zip(*(small_parts(all_small[owner].astype(jnp.float32)) for owner in range(8)))
    replicas[2][...] = jnp.concatenate(wides, axis=1).astype(jnp.bfloat16)
    for owner in range(8):
        vec_columns[TALL * owner:TALL * owner + TALL, 0:VEC] = vecs[owner]
    vec_rows[...] = vec_columns[...].T
    replicas[3][...] = vec_rows[0:VEC, :].astype(jnp.bfloat16)
    wait_bytes(all_small, sent.at[0, SMALL])
    wait_bytes(all_small.at[pl.ds(0, len(FAR_FIRST))], sent.at[1, SMALL])
    wait_bytes(early.at[1], early_sent.at[1])
    wait_bytes(all_tiles.at[:, pl.ds(0, len(FAR_FIRST))], tile_sent)
    for bank in BIG:
        wait_bytes(replicas[bank], sent.at[0, bank])
    for chunk, gone in ((MLP, 0), (ATTN, TAIL)):
        wait_bytes(replicas[chunk].at[:, pl.ds(0, SHAPES[chunk][1] - gone)], pass_recv.at[chunk])
        for half in HALVES:
            send_pair(replica_part(half, far, 0, ATTN_SHARD - TAIL) if chunk == ATTN else replica_chunk(half, far, chunk), chunk)
    for bank, received, gone in ((MLP, 0, 0), (ATTN, TAIL, EARLY)):
        columns = SHAPES[bank][1]
        wait_bytes(replicas[bank].at[:, pl.ds(0, 4 * columns - received)], pair_recv.at[bank])
        wait_bytes(replicas[bank].at[:, pl.ds(0, len(FAR_FIRST) * columns - gone)], sent.at[1, bank])
    wait_bytes(replicas[ATTN].at[:, pl.ds(0, 2 * TAIL)], tail_recv)


def write_out(*refs):
    count = (len(refs) - 1) // 2
    largest_first = sorted(range(count), key=lambda k: -refs[k].size)
    copies = [pltpu.make_async_copy(refs[k], refs[count + k], refs[-1]) for k in largest_first]
    for copy in copies:
        copy.start()
    for copy in copies:
        copy.wait()


def solution(mesh):
    shards = [jax.ShapeDtypeStruct(shape, jnp.float32) for shape in SHARDS]
    shapes = [jax.ShapeDtypeStruct(shape, jnp.bfloat16) for shape in zip(ROWS, LENGTHS)] + shards * 3
    f32, bf16 = jnp.float32, jnp.bfloat16
    dma = pltpu.SemaphoreType.DMA
    attn, mlp = SHAPES

    def sums(*lead):
        return [pltpu.VMEM((*lead, *attn), f32), pltpu.VMEM((*lead, *mlp), f32)]

    small = (TALL, VEC_PAD)
    scratch = [
        pltpu.VMEM((2, 2, 4, *attn), bf16), pltpu.VMEM((2, 2, 4, *mlp), bf16), pltpu.VMEM((2, 4, *small), bf16),
        *sums(2), pltpu.VMEM(small, f32), *sums(2), pltpu.VMEM(small, f32), *sums(2), pltpu.VMEM(small, f32), *sums(2),
        pltpu.VMEM((2, 2, FIRST, EARLY), f32), pltpu.VMEM((3, *SHARDS[2]), f32), pltpu.VMEM((3, *SHARDS[3]), f32),
        pltpu.VMEM((VEC, LANES), bf16), pltpu.VMEM((TALL, WIDE), bf16), pltpu.VMEM((8, *small), bf16),
        pltpu.VMEM((8, *small), bf16),
        pltpu.VMEM((VEC_PAD, LANES), f32), pltpu.VMEM((LANES, VEC_PAD), f32), pltpu.VMEM((8, VEC_PAD), f32),
        pltpu.VMEM((3, 8, 8, LANES), f32), pltpu.VMEM((LANES, LANES), f32),
        dma((6,)), dma((2, 3)), dma, dma((2, 2)), dma((2,)), dma((3,)), dma((3,)), dma((2, 2)), dma, dma((3,)), dma((3,)),
        dma((2,)), dma, dma, pltpu.SemaphoreType.REGULAR,
    ]
    count = len(shapes)
    anywhere = [pl.BlockSpec(memory_space=pl.ANY)] * count
    step = pl.pallas_call(
        kernel,
        out_shape=[pltpu.VMEM(shape.shape, shape.dtype) for shape in shapes],
        in_specs=anywhere,
        out_specs=[pl.BlockSpec(memory_space=pltpu.VMEM)] * count,
        scratch_shapes=scratch,
        compiler_params=pltpu.CompilerParams(collective_id=0, has_side_effects=True, vmem_limit_bytes=36 * MIB),
        name="lamb_step",
    )
    finish = pl.pallas_call(
        write_out,
        out_shape=shapes,
        in_specs=anywhere,
        out_specs=anywhere,
        scratch_shapes=[dma],
        compiler_params=pltpu.CompilerParams(vmem_limit_bytes=MIB),
        name="write_out",
    )

    def local_step(*banks):
        banks = [bank[0] for bank in banks[:4]] + [bank.T if bank.shape == (VEC, TALL) else bank for bank in banks[4:]]
        banks = [pltpu.with_memory_space_constraint(bank, pltpu.HBM) for bank in banks]
        results = finish(*step(*banks))
        return tuple(value.T if value.shape == (TALL, VEC) else value for value in results)

    grad_spec, shard_spec, full_spec = P("data", None, None), P(None, "data"), P(None, None)
    return jax.shard_map(local_step, mesh=mesh, in_specs=(grad_spec,) * 4 + (shard_spec,) * 12,
                         out_specs=(full_spec,) * 4 + (shard_spec,) * 12, check_vma=False)
```

```python
import functools

import jax
import jax.numpy as jnp
from jax import lax
from jax.experimental import pallas as pl
from jax.experimental.pallas import tpu as pltpu
from jax.sharding import PartitionSpec as P

STEP_NUMBER = 10
LEARN_RATE = 0.04
BETA_FIRST = 0.9
BETA_SECOND = 0.999
EPSILON = 1e-6
WEIGHT_DECAY = 0.01
MAX_NORM = 1.0
FIRST_SCALE = 1.0 / (1.0 - BETA_FIRST ** STEP_NUMBER)
SECOND_SCALE = 1.0 / (1.0 - BETA_SECOND ** STEP_NUMBER)

MESH = pl.DeviceIdType.MESH
LANES = 128
TALL = 16
HALF = 64
FIRST = 32
EARLY = 1024
VEC = 146
VEC_PAD = 256
ATTN_SHARD = 2048
MLP_SHARD = 8192
STEP = 2048
BLOCK = 1024
WIDE = 512
TAIL = 640
PASSED = ((0, 1024), (1024, ATTN_SHARD - TAIL))
MIB = 2 ** 20
ROWS = (HALF, 32, TALL, VEC)
LENGTHS = (16384, 65536, WIDE, LANES)
SHARDS = ((HALF, ATTN_SHARD), (32, MLP_SHARD), (TALL, HALF), (TALL, VEC))
ATTN, MLP, SMALL = range(3)
BIG = (ATTN, MLP)
HALVES = range(2)
SHAPES = ((32, ATTN_SHARD), (TALL, MLP_SHARD))
PEER, ALONG_X, ALONG_Y = 1, 2, 4
NEAR = ((ALONG_X, ALONG_Y), (ALONG_Y, ALONG_X))
WIDE_LANES = (LANES, LANES + HALF)
FAR_FIRST = (6, 7, 4, 2, 5, 3, 1)
TILE_ROWS = (4, 1, 3)


def flip(index, mask):
    core, x, y = index % 2, (index // 2) % 2, index // 4
    if mask & PEER:
        core = 1 - core
    if mask & ALONG_X:
        x = 1 - x
    if mask & ALONG_Y:
        y = 1 - y
    return y * 4 + x * 2 + core


def aligned(index, size):
    return pl.ds(pl.multiple_of(index * size, size), size)


def moments(first, second, total, clip):
    clipped = clip * total
    new_first = BETA_FIRST * first + (1.0 - BETA_FIRST) * clipped
    new_second = BETA_SECOND * second + (1.0 - BETA_SECOND) * (clipped * clipped)
    return new_first, new_second


def direction(new_first, new_second, weight):
    return (new_first * FIRST_SCALE) / (jnp.sqrt(new_second * SECOND_SCALE) + EPSILON) + WEIGHT_DECAY * weight


def fold(square):
    rows, columns = square.shape
    parts = [square[r:r + 8, k:k + LANES] for r in range(0, rows, 8) for k in range(0, columns, LANES)]
    while len(parts) > 1:
        parts = [a + b for a, b in zip(parts[::2], parts[1::2])] + ([parts[-1]] if len(parts) % 2 else [])
    return parts[0]


def add_all(values):
    return functools.reduce(lambda a, b: a + b, values)


def kernel(*refs):
    grads, weights, firsts, seconds = refs[0:4], refs[4:8], refs[8:12], refs[12:16]
    replicas, new_weights, new_firsts, new_seconds = refs[16:20], refs[20:24], refs[24:28], refs[28:32]
    (recv_attn, recv_mlp, recv_small, part_attn, part_mlp, part_small, last_attn, last_mlp, last_small,
     sum_attn, sum_mlp, sum_small, dir_attn, dir_mlp, early, state_wide, state_vec, vec_in, wide_in, small_out, all_small,
     vec_rows, vec_columns, vec_row, all_tiles, row_acc,
     load_sems, sent, tile_sent, scatter_recv, small_recv, last_recv, tile_recv, own_recv, own_small, pass_recv, pair_recv,
     early_sent, early_recv, tail_recv, attn_pass_recv, ready) = refs[32:]
    recvs, parts, lasts = (recv_attn, recv_mlp), (part_attn, part_mlp), (last_attn, last_mlp)
    me = lax.axis_index("data")
    core = me % 2

    def grad_chunk(half, owner, chunk):
        rows, columns = SHAPES[chunk]
        return grads[chunk].at[pl.ds(rows * half, rows), aligned(owner, columns)]

    def replica_chunk(half, owner, chunk):
        rows, columns = SHAPES[chunk]
        return replicas[chunk].at[pl.ds(rows * half, rows), aligned(owner, columns)]

    def replica_part(half, owner, first, last):
        rows, columns = SHAPES[ATTN]
        start = pl.multiple_of(owner * columns + first, LANES)
        return replicas[ATTN].at[pl.ds(rows * half, rows), pl.ds(start, last - first)]

    along_x, along_y = flip(me, ALONG_X), flip(me, ALONG_Y)
    small_near = (along_x * (1 - core) + along_y * core, along_y * (1 - core) + along_x * core)
    peer = flip(me, PEER)
    peer_next = flip(peer, ALONG_X) * (1 - core) + flip(peer, ALONG_Y) * core

    def send(source, target, send_sem, recv_sem, device):
        copy = pltpu.make_async_remote_copy(src_ref=source, dst_ref=target, send_sem=send_sem, recv_sem=recv_sem,
                                            device_id=(device,), device_id_type=MESH)
        copy.start()
        return copy

    def wait_bytes(ref, sem):
        pltpu.make_async_copy(ref, ref, sem).wait()

    barrier = pltpu.get_barrier_semaphore()

    def signal(semaphore, device):
        pl.semaphore_signal(semaphore, inc=1, device_id=(device,), device_id_type=MESH)

    signal(barrier, peer)

    @pl.when(core == 1)
    def _():
        for mask in (ALONG_X, ALONG_Y):
            for device in (flip(me, mask), flip(peer, mask)):
                signal(barrier, device)


    small_loads = [pltpu.make_async_copy(grads[2], wide_in, load_sems.at[4]),
                   pltpu.make_async_copy(grads[3], vec_in, load_sems.at[5])]
    for copy in small_loads:
        copy.start()
    for keep in range(2):
        for half in HALVES:
            for chunk in (MLP, ATTN):
                owner = me if keep else flip(me, NEAR[half][1])
                pltpu.make_async_copy(grad_chunk(half, owner, chunk), recvs[chunk].at[half, keep, 0],
                                      scatter_recv.at[keep, chunk]).start()
    for index, (source, target) in enumerate(((weights, new_weights), (firsts, new_firsts), (seconds, new_seconds))):
        for bank, place in enumerate((target[0], target[1], state_wide.at[index], state_vec.at[index])):
            pltpu.make_async_copy(source[bank], place, load_sems.at[bank]).start()
    pl.semaphore_wait(barrier, 3)

    def scatter(keep, chunk, slots):
        for slot in slots:
            for half in HALVES:
                target = peer if slot == 0 else flip(me, NEAR[half][0]) // 2 * 2 + slot - 1
                owner = target if keep else flip(target, NEAR[half][1])
                send(grad_chunk(half, owner, chunk), recvs[chunk].at[half, keep, 1 if slot == 0 else 2 + core],
                     sent.at[0, chunk], scatter_recv.at[keep, chunk], target)

    for chunk in (MLP, ATTN):
        scatter(0, chunk, (2, 0))

    @pl.when(core == 1)
    def _():
        signal(ready, along_x)
        signal(ready, along_y)
        pl.semaphore_wait(ready, 2)
        signal(ready, peer)

    @pl.when(core == 0)
    def _():
        pl.semaphore_wait(ready, 1)

    for chunk in (MLP, ATTN):
        scatter(0, chunk, (1,))
    for copy in small_loads:
        copy.wait()
    vec_rows[...] = jnp.zeros_like(vec_rows)
    vec_rows[0:VEC, :] = vec_in[...].astype(jnp.float32)
    vec_columns[...] = vec_rows[...].T

    def small_message(wide, vec):
        pad = jnp.zeros((TALL, VEC_PAD - VEC - HALF), jnp.float32)
        return jnp.concatenate([vec[:, 0:LANES], wide, vec[:, LANES:VEC], pad], axis=1).astype(jnp.bfloat16)

    def small_parts(message):
        vec = jnp.concatenate([message[:, 0:LANES], message[:, WIDE_LANES[1]:HALF + VEC]], axis=1)
        return message[:, slice(*WIDE_LANES)], vec

    wide_grad = wide_in[...].astype(jnp.float32)
    for owner in range(8):
        small_out[owner] = small_message(
            wide_grad[:, HALF * owner:HALF * owner + HALF], vec_columns[TALL * owner:TALL * owner + TALL, 0:VEC])
    for keep in range(2):
        recv_small[keep, 0] = small_out[me if keep else small_near[1]]
        places = [(along_x // 2 * 2, ALONG_Y), (along_y // 2 * 2 + 1, ALONG_X)]
        targets = [(target, target if keep else flip(target, way), 2 + core) for target, way in places]
        for target, owner, slot in [*targets, (peer, peer if keep else peer_next, 1)]:
            send(small_out.at[owner], recv_small.at[keep, slot], sent.at[0, SMALL], small_recv.at[keep], target)
    for chunk in (MLP, ATTN):
        scatter(1, chunk, (1, 2, 0))

    row = lax.broadcasted_iota(jnp.int32, (LANES, LANES), 0)
    lane = lax.broadcasted_iota(jnp.int32, (LANES, LANES), 1)
    eye = row == lane
    sub = lax.broadcasted_iota(jnp.int32, (8, LANES), 0)

    def lanes_of(first, last):
        column = jnp.sum(row_acc[first:last, :], axis=1, keepdims=True)
        return jnp.sum(jnp.where(eye[first:last, :], column, 0.0), axis=0, keepdims=True)

    def vec_lanes(square):
        vec_row[...] = jnp.zeros_like(vec_row)
        vec_row[0:1, 0:VEC] = jnp.sum(square, axis=0, keepdims=True)
        return vec_row[0:1, 0:LANES], vec_row[0:1, LANES:VEC_PAD]

    def tile_of(rows):
        tile = jnp.zeros((8, LANES), jnp.float32)
        for index, value in enumerate(rows):
            tile = jnp.where(sub == index, value, tile)
        return tile

    def exchange(which, value):
        all_tiles[which, me] = value
        place = all_tiles.at[which, me, pl.ds(0, TILE_ROWS[which])]
        for mask in FAR_FIRST:
            send(place, place, tile_sent, tile_recv.at[which], flip(me, mask))

    def collect(which):
        rows = TILE_ROWS[which]
        wait_bytes(all_tiles.at[which, pl.ds(0, len(FAR_FIRST)), pl.ds(0, rows)], tile_recv.at[which])
        return add_all([all_tiles[which, index, 0:rows] for index in range(8)])

    def by_rows(first, groups, columns, step):
        def group(g, carry):
            def inner(j, acc):
                return acc + step((aligned(g, 8), aligned(j, STEP)))

            row_acc[pl.ds(pl.multiple_of(first + g * 8, 8), 8), :] = lax.fori_loop(
                0, columns // STEP, inner, jnp.zeros((8, LANES), jnp.float32))
            return carry

        lax.fori_loop(0, groups, group, 0, unroll=4)

    def square_of(ref):
        return lambda place: fold(ref[place] * ref[place])

    for buffer, sem in ((recv_attn, load_sems.at[ATTN]), (recv_mlp, load_sems.at[MLP])):
        wait_bytes(buffer.at[:, :, pl.ds(0, 3)], sem)
    for bank, buffer in ((2, state_wide), (3, state_vec)):
        wait_bytes(buffer, load_sems.at[bank])
    row_acc[...] = jnp.zeros_like(row_acc)
    by_rows(0, 8, ATTN_SHARD, square_of(new_weights[0]))
    by_rows(HALF, 4, MLP_SHARD, square_of(new_weights[1]))
    wide_weight, vec_weight = state_wide[0], state_vec[0]
    row_acc[96:112, 0:HALF] = wide_weight * wide_weight
    weight_lanes = lanes_of(0, LANES)
    weight_low, weight_high = vec_lanes(vec_weight * vec_weight)

    def by_blocks(shape, step, init):
        rows, columns = shape
        for r in range(0, rows, TALL):
            init = lax.fori_loop(0, columns // BLOCK, functools.partial(
                lambda first, j, carry: step((pl.ds(first, TALL), aligned(j, BLOCK)), carry), r), init, unroll=2)
        return init

    def gather_sum(keep, chunk):
        wait_bytes(recvs[chunk].at[:, keep], scatter_recv.at[keep, chunk])
        for half in HALVES:
            source, target = recvs[chunk].at[half, keep], ((sum_attn, sum_mlp) if keep else parts)[chunk].at[half]

            def step(place, carry):
                value = [source[(slot, *place)].astype(jnp.float32) for slot in range(4)]
                target[place] = (value[0] + value[1]) + (value[2] + value[3])
                return carry

            by_blocks(SHAPES[chunk], step, 0)

    def gather_small(keep, target):
        wait_bytes(recv_small.at[keep, pl.ds(1, 3)], small_recv.at[keep])
        target[...] = add_all([recv_small[keep, slot].astype(jnp.float32) for slot in range(4)])

    for chunk in (MLP, ATTN):
        gather_sum(0, chunk)
    gather_small(0, part_small)
    send(part_small, last_small, sent.at[0, SMALL], last_recv.at[SMALL], small_near[1])
    for chunk in (MLP, ATTN):
        for half in HALVES:
            send(parts[chunk].at[half], lasts[chunk].at[half], sent.at[0, chunk], last_recv.at[chunk], flip(me, NEAR[half][1]))
    for chunk in (MLP, ATTN):
        gather_sum(1, chunk)
    gather_small(1, sum_small)

    wait_bytes(last_small, last_recv.at[SMALL])
    wide_total, vec_total = small_parts(sum_small[...] + last_small[...])
    square = fold(jnp.concatenate([wide_total * wide_total, jnp.zeros((TALL, HALF), jnp.float32)], axis=1))
    low, high = vec_lanes(vec_total * vec_total)
    square = square + tile_of([low, high])
    for chunk in (MLP, ATTN):
        wait_bytes(lasts[chunk], last_recv.at[chunk])
        for half in HALVES:
            total, rest = (sum_attn, sum_mlp)[chunk].at[half], lasts[chunk].at[half]

            def step(place, acc):
                value = total[place] + rest[place]
                total[place] = value
                return acc + fold(value * value)

            square = by_blocks(SHAPES[chunk], step, square)

    exchange(0, tile_of([weight_lanes, weight_low, weight_high, jnp.sum(square, axis=0, keepdims=True)]))
    late_rows = pl.ds(FIRST, FIRST)
    early_columns = pl.ds(0, EARLY)

    def send_early(kind, source):
        for way, mask in enumerate((ALONG_X, ALONG_Y)):
            send(source, early.at[kind, way], early_sent.at[kind], early_recv, flip(me, mask))

    send_early(0, new_weights[ATTN].at[late_rows, early_columns])
    start = collect(0)
    square = jnp.sum(jnp.sum(start[3:4, :], axis=1, keepdims=True), axis=0, keepdims=True)
    clip = jnp.minimum(1.0, (8.0 * MAX_NORM) / jnp.sqrt(jnp.broadcast_to(square, (8, LANES)))) * 0.125
    clip_block = jnp.concatenate([clip] * (STEP // LANES), axis=1)
    weight_norms = LEARN_RATE * jnp.sqrt(start)

    sums, directions = (sum_attn, sum_mlp), (dir_attn, dir_mlp)

    def update(bank, half):
        rows = SHAPES[bank][0]

        def step(place):
            state = (pl.ds(pl.multiple_of(half * rows + place[0].start, 8), 8), place[1])
            new_first, new_second = moments(
                new_firsts[bank][state], new_seconds[bank][state], sums[bank].at[half][place], clip_block)
            value = direction(new_first, new_second, new_weights[bank][state])
            directions[bank].at[half][place] = value
            return fold(value * value)

        by_rows(HALF * bank + half * rows, rows // 8, SHAPES[bank][1], step)

    def store_moments(bank, half):
        rows = SHAPES[bank][0]

        def step(place, carry):
            state = (pl.ds(half * rows + place[0].start, TALL), place[1])
            clip_wide = jnp.concatenate([clip_block[:, 0:BLOCK]] * 2, axis=0)
            new_first, new_second = moments(
                new_firsts[bank][state], new_seconds[bank][state], sums[bank].at[half][place], clip_wide)
            new_firsts[bank][state] = new_first
            new_seconds[bank][state] = new_second
            return carry

        by_blocks(SHAPES[bank], step, 0)

    def update_small(bank, total, state):
        new_first, new_second = moments(state[1], state[2], total, clip[0:1, 0:1])
        new_firsts[bank][...] = new_first
        new_seconds[bank][...] = new_second
        return direction(new_first, new_second, state[0])

    update(ATTN, 0)
    exchange(1, tile_of([lanes_of(0, FIRST)]))
    update(ATTN, 1)
    send_early(1, dir_attn.at[1, :, early_columns])
    for half in HALVES:
        update(MLP, half)
    wide_dir = update_small(2, wide_total, state_wide)
    vec_dir = update_small(3, vec_total, state_vec)
    row_acc[96:112, 0:HALF] = wide_dir * wide_dir
    exchange(2, tile_of([lanes_of(FIRST, LANES), *vec_lanes(vec_dir * vec_dir)]))
    for bank in (ATTN, MLP):
        for half in HALVES:
            store_moments(bank, half)

    def send_own(half, chunk, way):
        place = all_small.at[me] if chunk == SMALL else replica_chunk(half, me, chunk)
        if (half, chunk) == (1, ATTN) and way:
            place = replica_part(1, me, EARLY, ATTN_SHARD)
        recv_sem = pair_recv.at[chunk] if not way else own_small if chunk == SMALL else own_recv.at[(way - 1 + half) % 2, chunk]
        send(place, place, sent.at[1, chunk], recv_sem, flip(me, (PEER, ALONG_X, ALONG_Y)[way]))

    def wait_own(kind, chunk):
        columns = SHAPES[chunk][1] - (EARLY // 2 if chunk == ATTN else 0)
        wait_bytes(replicas[chunk].at[:, pl.ds(0, columns)], own_recv.at[kind, chunk])

    def spread_ratio(first, last, ratio):
        row_acc[first:last, :] = jnp.broadcast_to(
            jnp.sum(jnp.where(eye[first:last, :], ratio[0:1, :], 0.0), axis=1, keepdims=True), (last - first, LANES))

    def form_weights(bank, half, owner, shape, weight, direct, result):
        rows = SHAPES[bank][0]

        def step(place, carry):
            first = half * rows + place[0].start
            scale = jnp.concatenate([row_acc[HALF * bank + first:HALF * bank + first + TALL, :]] * (BLOCK // LANES), axis=1)
            value = weight[place] - scale * direct[place]
            if result is not None:
                result[place] = value
            target = pl.ds(pl.multiple_of(owner * SHAPES[bank][1] + place[1].start, BLOCK), BLOCK)
            replicas[bank][pl.ds(first, TALL), target] = value.astype(jnp.bfloat16)
            return carry

        by_blocks(shape, step, 0)

    def new_weight(bank, half, ways):
        rows = SHAPES[bank][0]
        mine = new_weights[bank].at[pl.ds(half * rows, rows)]
        form_weights(bank, half, me, SHAPES[bank], mine, directions[bank].at[half], mine)
        for way in ways:
            send_own(half, bank, way)

    spread_ratio(0, FIRST, weight_norms[0:1, :] / jnp.sqrt(collect(1)))
    new_weight(ATTN, 0, (1, 2, 0))
    ratio = weight_norms[0:3, :] / jnp.sqrt(collect(2))
    spread_ratio(FIRST, LANES, ratio)
    wait_bytes(early.at[0], early_sent.at[0])
    new_weight(ATTN, 1, (2, 0))
    for half in HALVES:
        new_weight(MLP, half, (1 + half, 0))
    value = wide_weight - row_acc[96:112, 0:HALF] * wide_dir
    new_weights[2][...] = value
    wide_value = value
    vec_row[0:1, 0:LANES] = ratio[1:2, :]
    vec_row[0:1, LANES:VEC_PAD] = ratio[2:3, :]
    value = vec_weight - vec_row[0:1, 0:VEC] * vec_dir
    new_weights[3][...] = value
    all_small[me] = small_message(wide_value, value)
    for way in (1, 2, 0):
        send_own(0, SMALL, way)
    send_own(1, ATTN, 1)
    for half in HALVES:
        send_own(half, MLP, 2 - half)

    wait_bytes(early, early_recv)
    for way, owner in enumerate((along_x, along_y)):
        form_weights(ATTN, 1, owner, (FIRST, EARLY), early.at[0, way], early.at[1, way], None)

    def send_pair(place, chunk):
        send(place, place, sent.at[1, chunk], pair_recv.at[chunk], peer)

    wait_bytes(all_small.at[pl.ds(0, 2)], own_small)
    place = all_small.at[small_near[0]]
    send(place, place, sent.at[1, SMALL], pass_recv.at[SMALL], small_near[1])
    for owner in small_near:
        send_pair(all_small.at[owner], SMALL)
    for chunk in (MLP, ATTN):
        wait_own(0, chunk)
        for half in HALVES:
            owner, target = flip(me, NEAR[half][0]), flip(me, NEAR[half][1])
            place = replica_chunk(half, owner, chunk)
            send_pair(place, chunk)
            if chunk == MLP:
                send(place, place, sent.at[1, MLP], pass_recv.at[MLP], target)
    for index, (first, last) in enumerate(PASSED):
        for half in HALVES:
            place = replica_part(half, flip(me, NEAR[half][0]), first, last)
            send(place, place, sent.at[1, ATTN], attn_pass_recv.at[index], flip(me, NEAR[half][1]))
    for target_core in (0, 1):
        for half in HALVES:
            place = replica_part(half, flip(me, NEAR[half][0]), ATTN_SHARD - TAIL, ATTN_SHARD)
            send(place, place, sent.at[1, ATTN], tail_recv, flip(me, NEAR[half][1] + (PEER if target_core else 0)))
    for chunk in BIG:
        wait_own(1, chunk)
        for half in HALVES:
            send_pair(replica_chunk(half, flip(me, NEAR[half][1]), chunk), chunk)
    far = flip(me, ALONG_X + ALONG_Y)
    wait_bytes(all_small.at[pl.ds(0, 1)], pass_recv.at[SMALL])
    send_pair(all_small.at[far], SMALL)
    wait_bytes(all_small.at[pl.ds(0, 4)], pair_recv.at[SMALL])
    wides, vecs = zip(*(small_parts(all_small[owner].astype(jnp.float32)) for owner in range(8)))
    replicas[2][...] = jnp.concatenate(wides, axis=1).astype(jnp.bfloat16)
    for owner in range(8):
        vec_columns[TALL * owner:TALL * owner + TALL, 0:VEC] = vecs[owner]
    vec_rows[...] = vec_columns[...].T
    replicas[3][...] = vec_rows[0:VEC, :].astype(jnp.bfloat16)
    wait_bytes(all_small, sent.at[0, SMALL])
    wait_bytes(all_small.at[pl.ds(0, len(FAR_FIRST))], sent.at[1, SMALL])
    wait_bytes(early.at[1], early_sent.at[1])
    wait_bytes(all_tiles.at[0, pl.ds(0, len(FAR_FIRST))], tile_sent)
    for bank in BIG:
        wait_bytes(replicas[bank], sent.at[0, bank])
    wait_bytes(replicas[MLP].at[:, pl.ds(0, MLP_SHARD)], pass_recv.at[MLP])
    for half in HALVES:
        send_pair(replica_chunk(half, far, MLP), MLP)
    for index, (first, last) in enumerate(PASSED):
        wait_bytes(replicas[ATTN].at[:, pl.ds(0, last - first)], attn_pass_recv.at[index])
        for half in HALVES:
            send_pair(replica_part(half, far, first, last), ATTN)
    for bank, received, gone in ((MLP, 0, 0), (ATTN, TAIL, EARLY)):
        columns = SHAPES[bank][1]
        wait_bytes(replicas[bank].at[:, pl.ds(0, 4 * columns - received)], pair_recv.at[bank])
        wait_bytes(replicas[bank].at[:, pl.ds(0, len(FAR_FIRST) * columns - gone)], sent.at[1, bank])
    wait_bytes(replicas[ATTN].at[:, pl.ds(0, 2 * TAIL)], tail_recv)


def write_out(*refs):
    count = (len(refs) - 1) // 2
    largest_first = sorted(range(count), key=lambda k: -refs[k].size)
    copies = [pltpu.make_async_copy(refs[k], refs[count + k], refs[-1]) for k in largest_first]
    for copy in copies:
        copy.start()
    for copy in copies:
        copy.wait()


def solution(mesh):
    shards = [jax.ShapeDtypeStruct(shape, jnp.float32) for shape in SHARDS]
    shapes = [jax.ShapeDtypeStruct(shape, jnp.bfloat16) for shape in zip(ROWS, LENGTHS)] + shards * 3
    f32, bf16 = jnp.float32, jnp.bfloat16
    dma = pltpu.SemaphoreType.DMA
    attn, mlp = SHAPES

    def sums(*lead):
        return [pltpu.VMEM((*lead, *attn), f32), pltpu.VMEM((*lead, *mlp), f32)]

    small = (TALL, VEC_PAD)
    scratch = [
        pltpu.VMEM((2, 2, 4, *attn), bf16), pltpu.VMEM((2, 2, 4, *mlp), bf16), pltpu.VMEM((2, 4, *small), bf16),
        *sums(2), pltpu.VMEM(small, f32), *sums(2), pltpu.VMEM(small, f32), *sums(2), pltpu.VMEM(small, f32), *sums(2),
        pltpu.VMEM((2, 2, FIRST, EARLY), f32), pltpu.VMEM((3, *SHARDS[2]), f32), pltpu.VMEM((3, *SHARDS[3]), f32),
        pltpu.VMEM((VEC, LANES), bf16), pltpu.VMEM((TALL, WIDE), bf16), pltpu.VMEM((8, *small), bf16),
        pltpu.VMEM((8, *small), bf16),
        pltpu.VMEM((VEC_PAD, LANES), f32), pltpu.VMEM((LANES, VEC_PAD), f32), pltpu.VMEM((8, VEC_PAD), f32),
        pltpu.VMEM((3, 8, 8, LANES), f32), pltpu.VMEM((LANES, LANES), f32),
        dma((6,)), dma((2, 3)), dma, dma((2, 2)), dma((2,)), dma((3,)), dma((3,)), dma((2, 2)), dma, dma((3,)), dma((3,)),
        dma((2,)), dma, dma, dma((len(PASSED),)), pltpu.SemaphoreType.REGULAR,
    ]
    count = len(shapes)
    anywhere = [pl.BlockSpec(memory_space=pl.ANY)] * count
    step = pl.pallas_call(
        kernel,
        out_shape=[pltpu.VMEM(shape.shape, shape.dtype) for shape in shapes],
        in_specs=anywhere,
        out_specs=[pl.BlockSpec(memory_space=pltpu.VMEM)] * count,
        scratch_shapes=scratch,
        compiler_params=pltpu.CompilerParams(collective_id=0, has_side_effects=True, vmem_limit_bytes=36 * MIB),
        name="lamb_step",
    )
    finish = pl.pallas_call(
        write_out,
        out_shape=shapes,
        in_specs=anywhere,
        out_specs=anywhere,
        scratch_shapes=[dma],
        compiler_params=pltpu.CompilerParams(vmem_limit_bytes=MIB),
        name="write_out",
    )

    def local_step(*banks):
        banks = [bank[0] for bank in banks[:4]] + [bank.T if bank.shape == (VEC, TALL) else bank for bank in banks[4:]]
        banks = [pltpu.with_memory_space_constraint(bank, pltpu.HBM) for bank in banks]
        results = finish(*step(*banks))
        return tuple(value.T if value.shape == (TALL, VEC) else value for value in results)

    grad_spec, shard_spec, full_spec = P("data", None, None), P(None, "data"), P(None, None)
    return jax.shard_map(local_step, mesh=mesh, in_specs=(grad_spec,) * 4 + (shard_spec,) * 12,
                         out_specs=(full_spec,) * 4 + (shard_spec,) * 12, check_vma=False)
```

```python
import functools

import jax
import jax.numpy as jnp
from jax import lax
from jax.experimental import pallas as pl
from jax.experimental.pallas import tpu as pltpu
from jax.sharding import PartitionSpec as P

STEP_NUMBER = 10
LEARN_RATE = 0.04
BETA_FIRST = 0.9
BETA_SECOND = 0.999
EPSILON = 1e-6
WEIGHT_DECAY = 0.01
MAX_NORM = 1.0
FIRST_SCALE = 1.0 / (1.0 - BETA_FIRST ** STEP_NUMBER)
SECOND_SCALE = 1.0 / (1.0 - BETA_SECOND ** STEP_NUMBER)
FIRST_FACTOR = FIRST_SCALE / SECOND_SCALE ** 0.5
EPSILON_TERM = EPSILON / SECOND_SCALE ** 0.5

MESH = pl.DeviceIdType.MESH
LANES = 128
TALL = 16
HALF = 64
FIRST = 32
EARLY = 1024
VEC = 146
VEC_PAD = 256
ATTN_SHARD = 2048
MLP_SHARD = 8192
STEP = 2048
BLOCK = 1024
WIDE = 512
TAIL = 640
PASSED = ((0, 1152), (1152, ATTN_SHARD - TAIL))
MIB = 2 ** 20
ROWS = (HALF, 32, TALL, VEC)
LENGTHS = (16384, 65536, WIDE, LANES)
SHARDS = ((HALF, ATTN_SHARD), (32, MLP_SHARD), (TALL, HALF), (TALL, VEC))
ATTN, MLP, SMALL = range(3)
BIG = (ATTN, MLP)
HALVES = range(2)
SHAPES = ((32, ATTN_SHARD), (TALL, MLP_SHARD))
PEER, ALONG_X, ALONG_Y = 1, 2, 4
NEAR = ((ALONG_X, ALONG_Y), (ALONG_Y, ALONG_X))
WIDE_LANES = (LANES, LANES + HALF)
FAR_FIRST = (6, 4, 2, 7, 5, 3, 1)
TILE_ROWS = (4, 1, 3)


def flip(index, mask):
    core, x, y = index % 2, (index // 2) % 2, index // 4
    if mask & PEER:
        core = 1 - core
    if mask & ALONG_X:
        x = 1 - x
    if mask & ALONG_Y:
        y = 1 - y
    return y * 4 + x * 2 + core


def aligned(index, size):
    return pl.ds(pl.multiple_of(index * size, size), size)


def moments(first, second, total, factors):
    new_first = BETA_FIRST * first + factors[0] * total
    new_second = BETA_SECOND * second + factors[1] * (total * total)
    return new_first, new_second


def direction(new_first, new_second, weight):
    return (new_first * FIRST_FACTOR) / (jnp.sqrt(new_second) + EPSILON_TERM) + WEIGHT_DECAY * weight


def fold(square):
    rows, columns = square.shape
    parts = [square[r:r + 8, k:k + LANES] for r in range(0, rows, 8) for k in range(0, columns, LANES)]
    while len(parts) > 1:
        parts = [a + b for a, b in zip(parts[::2], parts[1::2])] + ([parts[-1]] if len(parts) % 2 else [])
    return parts[0]


def add_all(values):
    return functools.reduce(lambda a, b: a + b, values)


def kernel(*refs):
    grads, weights, firsts, seconds = refs[0:4], refs[4:8], refs[8:12], refs[12:16]
    replicas, new_weights, new_firsts, new_seconds = refs[16:20], refs[20:24], refs[24:28], refs[28:32]
    (recv_attn, recv_mlp, recv_small, part_attn, part_mlp, part_small, last_attn, last_mlp, last_small,
     sum_attn, sum_mlp, sum_small, dir_attn, dir_mlp, early, state_wide, state_vec, vec_in, wide_in, small_out, all_small,
     vec_rows, vec_columns, vec_row, all_tiles, row_acc,
     load_sems, sent, tile_sent, scatter_recv, small_recv, last_recv, tile_recv, own_recv, own_small, pass_recv, pair_recv,
     early_sent, early_recv, tail_recv, attn_pass_recv, ready) = refs[32:]
    recvs, parts, lasts = (recv_attn, recv_mlp), (part_attn, part_mlp), (last_attn, last_mlp)
    me = lax.axis_index("data")
    core = me % 2

    def grad_chunk(half, owner, chunk):
        rows, columns = SHAPES[chunk]
        return grads[chunk].at[pl.ds(rows * half, rows), aligned(owner, columns)]

    def replica_chunk(half, owner, chunk):
        rows, columns = SHAPES[chunk]
        return replicas[chunk].at[pl.ds(rows * half, rows), aligned(owner, columns)]

    def replica_part(half, owner, first, last):
        rows, columns = SHAPES[ATTN]
        start = pl.multiple_of(owner * columns + first, LANES)
        return replicas[ATTN].at[pl.ds(rows * half, rows), pl.ds(start, last - first)]

    along_x, along_y = flip(me, ALONG_X), flip(me, ALONG_Y)
    small_near = (along_x * (1 - core) + along_y * core, along_y * (1 - core) + along_x * core)
    peer = flip(me, PEER)
    peer_next = flip(peer, ALONG_X) * (1 - core) + flip(peer, ALONG_Y) * core

    def send(source, target, send_sem, recv_sem, device):
        copy = pltpu.make_async_remote_copy(src_ref=source, dst_ref=target, send_sem=send_sem, recv_sem=recv_sem,
                                            device_id=(device,), device_id_type=MESH)
        copy.start()
        return copy

    def wait_bytes(ref, sem):
        pltpu.make_async_copy(ref, ref, sem).wait()

    barrier = pltpu.get_barrier_semaphore()

    def signal(semaphore, device):
        pl.semaphore_signal(semaphore, inc=1, device_id=(device,), device_id_type=MESH)

    signal(barrier, peer)

    @pl.when(core == 1)
    def _():
        for mask in (ALONG_X, ALONG_Y):
            for device in (flip(me, mask), flip(peer, mask)):
                signal(barrier, device)


    small_loads = [pltpu.make_async_copy(grads[2], wide_in, load_sems.at[4]),
                   pltpu.make_async_copy(grads[3], vec_in, load_sems.at[5])]
    for copy in small_loads:
        copy.start()
    for keep in range(2):
        for half in HALVES:
            for chunk in (MLP, ATTN):
                owner = me if keep else flip(me, NEAR[half][1])
                pltpu.make_async_copy(grad_chunk(half, owner, chunk), recvs[chunk].at[half, keep, 0],
                                      scatter_recv.at[keep, chunk]).start()
    for index, (source, target) in enumerate(((weights, new_weights), (firsts, new_firsts), (seconds, new_seconds))):
        for bank, place in enumerate((target[0], target[1], state_wide.at[index], state_vec.at[index])):
            pltpu.make_async_copy(source[bank], place, load_sems.at[bank]).start()
    pl.semaphore_wait(barrier, 3)

    def scatter(keep, chunk, slots):
        for slot in slots:
            for half in HALVES:
                target = peer if slot == 0 else flip(me, NEAR[half][0]) // 2 * 2 + slot - 1
                owner = target if keep else flip(target, NEAR[half][1])
                send(grad_chunk(half, owner, chunk), recvs[chunk].at[half, keep, 1 if slot == 0 else 2 + core],
                     sent.at[0, chunk], scatter_recv.at[keep, chunk], target)

    for chunk in (MLP, ATTN):
        scatter(0, chunk, (2, 0))

    @pl.when(core == 1)
    def _():
        signal(ready, along_x)
        signal(ready, along_y)
        pl.semaphore_wait(ready, 2)
        signal(ready, peer)

    @pl.when(core == 0)
    def _():
        pl.semaphore_wait(ready, 1)

    for chunk in (MLP, ATTN):
        scatter(0, chunk, (1,))
    for copy in small_loads:
        copy.wait()
    vec_rows[...] = jnp.zeros_like(vec_rows)
    vec_rows[0:VEC, :] = vec_in[...].astype(jnp.float32)
    vec_columns[...] = vec_rows[...].T

    def small_message(wide, vec):
        pad = jnp.zeros((TALL, VEC_PAD - VEC - HALF), jnp.float32)
        return jnp.concatenate([vec[:, 0:LANES], wide, vec[:, LANES:VEC], pad], axis=1).astype(jnp.bfloat16)

    def small_parts(message):
        vec = jnp.concatenate([message[:, 0:LANES], message[:, WIDE_LANES[1]:HALF + VEC]], axis=1)
        return message[:, slice(*WIDE_LANES)], vec

    wide_grad = wide_in[...].astype(jnp.float32)
    for owner in range(8):
        small_out[owner] = small_message(
            wide_grad[:, HALF * owner:HALF * owner + HALF], vec_columns[TALL * owner:TALL * owner + TALL, 0:VEC])
    for keep in range(2):
        recv_small[keep, 0] = small_out[me if keep else small_near[1]]
        places = [(along_x // 2 * 2, ALONG_Y), (along_y // 2 * 2 + 1, ALONG_X)]
        targets = [(target, target if keep else flip(target, way), 2 + core) for target, way in places]
        for target, owner, slot in [*targets, (peer, peer if keep else peer_next, 1)]:
            send(small_out.at[owner], recv_small.at[keep, slot], sent.at[0, SMALL], small_recv.at[keep], target)
    for chunk in (MLP, ATTN):
        scatter(1, chunk, (1, 2, 0))

    row = lax.broadcasted_iota(jnp.int32, (LANES, LANES), 0)
    lane = lax.broadcasted_iota(jnp.int32, (LANES, LANES), 1)
    eye = row == lane
    sub = lax.broadcasted_iota(jnp.int32, (8, LANES), 0)

    def lanes_of(first, last):
        column = jnp.sum(row_acc[first:last, :], axis=1, keepdims=True)
        return jnp.sum(jnp.where(eye[first:last, :], column, 0.0), axis=0, keepdims=True)

    def vec_lanes(square):
        vec_row[...] = jnp.zeros_like(vec_row)
        vec_row[0:1, 0:VEC] = jnp.sum(square, axis=0, keepdims=True)
        return vec_row[0:1, 0:LANES], vec_row[0:1, LANES:VEC_PAD]

    def tile_of(rows):
        tile = jnp.zeros((8, LANES), jnp.float32)
        for index, value in enumerate(rows):
            tile = jnp.where(sub == index, value, tile)
        return tile

    def exchange(which, value):
        all_tiles[which, me] = value
        place = all_tiles.at[which, me, pl.ds(0, TILE_ROWS[which])]
        for mask in FAR_FIRST:
            send(place, place, tile_sent, tile_recv.at[which], flip(me, mask))

    def collect(which):
        rows = TILE_ROWS[which]
        wait_bytes(all_tiles.at[which, pl.ds(0, len(FAR_FIRST)), pl.ds(0, rows)], tile_recv.at[which])
        return add_all([all_tiles[which, index, 0:rows] for index in range(8)])

    def by_rows(first, groups, columns, step):
        def group(g, carry):
            def inner(j, acc):
                return acc + step((aligned(g, 8), aligned(j, STEP)))

            row_acc[pl.ds(pl.multiple_of(first + g * 8, 8), 8), :] = lax.fori_loop(
                0, columns // STEP, inner, jnp.zeros((8, LANES), jnp.float32))
            return carry

        lax.fori_loop(0, groups, group, 0, unroll=4)

    def square_of(ref):
        return lambda place: fold(ref[place] * ref[place])

    for buffer, sem in ((recv_attn, load_sems.at[ATTN]), (recv_mlp, load_sems.at[MLP])):
        wait_bytes(buffer.at[:, :, pl.ds(0, 3)], sem)
    for bank, buffer in ((2, state_wide), (3, state_vec)):
        wait_bytes(buffer, load_sems.at[bank])
    row_acc[...] = jnp.zeros_like(row_acc)
    by_rows(0, 8, ATTN_SHARD, square_of(new_weights[0]))
    by_rows(HALF, 4, MLP_SHARD, square_of(new_weights[1]))
    wide_weight, vec_weight = state_wide[0], state_vec[0]
    row_acc[96:112, 0:HALF] = wide_weight * wide_weight
    weight_lanes = lanes_of(0, LANES)
    weight_low, weight_high = vec_lanes(vec_weight * vec_weight)

    def by_blocks(shape, step, init):
        rows, columns = shape
        for r in range(0, rows, TALL):
            init = lax.fori_loop(0, columns // BLOCK, functools.partial(
                lambda first, j, carry: step((pl.ds(first, TALL), aligned(j, BLOCK)), carry), r), init, unroll=2)
        return init

    def gather_sum(keep, chunk):
        wait_bytes(recvs[chunk].at[:, keep], scatter_recv.at[keep, chunk])
        for half in HALVES:
            source, target = recvs[chunk].at[half, keep], ((sum_attn, sum_mlp) if keep else parts)[chunk].at[half]

            def step(place, carry):
                value = [source[(slot, *place)].astype(jnp.float32) for slot in range(4)]
                target[place] = (value[0] + value[1]) + (value[2] + value[3])
                return carry

            by_blocks(SHAPES[chunk], step, 0)

    def gather_small(keep, target):
        wait_bytes(recv_small.at[keep, pl.ds(1, 3)], small_recv.at[keep])
        target[...] = add_all([recv_small[keep, slot].astype(jnp.float32) for slot in range(4)])

    for chunk in (MLP, ATTN):
        gather_sum(0, chunk)
    gather_small(0, part_small)
    send(part_small, last_small, sent.at[0, SMALL], last_recv.at[SMALL], small_near[1])
    for chunk in (MLP, ATTN):
        for half in HALVES:
            send(parts[chunk].at[half], lasts[chunk].at[half], sent.at[0, chunk], last_recv.at[chunk], flip(me, NEAR[half][1]))
    for chunk in (MLP, ATTN):
        gather_sum(1, chunk)
    gather_small(1, sum_small)

    wait_bytes(last_small, last_recv.at[SMALL])
    wide_total, vec_total = small_parts(sum_small[...] + last_small[...])
    square = fold(jnp.concatenate([wide_total * wide_total, jnp.zeros((TALL, HALF), jnp.float32)], axis=1))
    low, high = vec_lanes(vec_total * vec_total)
    square = square + tile_of([low, high])
    for chunk in (MLP, ATTN):
        wait_bytes(lasts[chunk], last_recv.at[chunk])
        for half in HALVES:
            total, rest = (sum_attn, sum_mlp)[chunk].at[half], lasts[chunk].at[half]

            def step(place, acc):
                value = total[place] + rest[place]
                total[place] = value
                return acc + fold(value * value)

            square = by_blocks(SHAPES[chunk], step, square)

    exchange(0, tile_of([weight_lanes, weight_low, weight_high, jnp.sum(square, axis=0, keepdims=True)]))
    late_rows = pl.ds(FIRST, FIRST)
    early_columns = pl.ds(0, EARLY)

    def send_early(kind, source):
        for way, mask in enumerate((ALONG_X, ALONG_Y)):
            send(source, early.at[kind, way], early_sent.at[kind], early_recv, flip(me, mask))

    send_early(0, new_weights[ATTN].at[late_rows, early_columns])
    start = collect(0)
    square = jnp.sum(jnp.sum(start[3:4, :], axis=1, keepdims=True), axis=0, keepdims=True)
    clip = jnp.minimum(1.0, (8.0 * MAX_NORM) / jnp.sqrt(jnp.broadcast_to(square, (8, LANES)))) * 0.125
    factors = ((1.0 - BETA_FIRST) * clip, (1.0 - BETA_SECOND) * (clip * clip))
    factor_blocks = [jnp.concatenate([factor] * (STEP // LANES), axis=1) for factor in factors]
    weight_norms = LEARN_RATE * jnp.sqrt(start)

    sums, directions = (sum_attn, sum_mlp), (dir_attn, dir_mlp)

    def update(bank, half):
        rows = SHAPES[bank][0]

        def step(place):
            state = (pl.ds(pl.multiple_of(half * rows + place[0].start, 8), 8), place[1])
            new_first, new_second = moments(
                new_firsts[bank][state], new_seconds[bank][state], sums[bank].at[half][place], factor_blocks)
            value = direction(new_first, new_second, new_weights[bank][state])
            directions[bank].at[half][place] = value
            return fold(value * value)

        by_rows(HALF * bank + half * rows, rows // 8, SHAPES[bank][1], step)

    def store_moments(bank, half):
        rows = SHAPES[bank][0]

        def step(place, carry):
            state = (pl.ds(half * rows + place[0].start, TALL), place[1])
            wide_factors = [jnp.concatenate([block[:, 0:BLOCK]] * 2, axis=0) for block in factor_blocks]
            new_first, new_second = moments(
                new_firsts[bank][state], new_seconds[bank][state], sums[bank].at[half][place], wide_factors)
            new_firsts[bank][state] = new_first
            new_seconds[bank][state] = new_second
            return carry

        by_blocks(SHAPES[bank], step, 0)

    def update_small(bank, total, state):
        new_first, new_second = moments(state[1], state[2], total, [factor[0:1, 0:1] for factor in factors])
        new_firsts[bank][...] = new_first
        new_seconds[bank][...] = new_second
        return direction(new_first, new_second, state[0])

    update(ATTN, 0)
    exchange(1, tile_of([lanes_of(0, FIRST)]))
    update(ATTN, 1)
    send_early(1, dir_attn.at[1, :, early_columns])
    for half in HALVES:
        update(MLP, half)
    wide_dir = update_small(2, wide_total, state_wide)
    vec_dir = update_small(3, vec_total, state_vec)
    row_acc[96:112, 0:HALF] = wide_dir * wide_dir
    exchange(2, tile_of([lanes_of(FIRST, LANES), *vec_lanes(vec_dir * vec_dir)]))
    for bank in (ATTN, MLP):
        for half in HALVES:
            store_moments(bank, half)

    def send_own(half, chunk, way):
        place = all_small.at[me] if chunk == SMALL else replica_chunk(half, me, chunk)
        if (half, chunk) == (1, ATTN) and way:
            place = replica_part(1, me, EARLY, ATTN_SHARD)
        recv_sem = pair_recv.at[chunk] if not way else own_small if chunk == SMALL else own_recv.at[(way - 1 + half) % 2, chunk]
        send(place, place, sent.at[1, chunk], recv_sem, flip(me, (PEER, ALONG_X, ALONG_Y)[way]))

    def wait_own(kind, chunk):
        columns = SHAPES[chunk][1] - (EARLY // 2 if chunk == ATTN else 0)
        wait_bytes(replicas[chunk].at[:, pl.ds(0, columns)], own_recv.at[kind, chunk])

    def spread_ratio(first, last, ratio):
        row_acc[first:last, :] = jnp.broadcast_to(
            jnp.sum(jnp.where(eye[first:last, :], ratio[0:1, :], 0.0), axis=1, keepdims=True), (last - first, LANES))

    def form_weights(bank, half, owner, shape, weight, direct, result):
        rows = SHAPES[bank][0]

        def step(place, carry):
            first = half * rows + place[0].start
            scale = jnp.concatenate([row_acc[HALF * bank + first:HALF * bank + first + TALL, :]] * (BLOCK // LANES), axis=1)
            value = weight[place] - scale * direct[place]
            if result is not None:
                result[place] = value
            target = pl.ds(pl.multiple_of(owner * SHAPES[bank][1] + place[1].start, BLOCK), BLOCK)
            replicas[bank][pl.ds(first, TALL), target] = value.astype(jnp.bfloat16)
            return carry

        by_blocks(shape, step, 0)

    def new_weight(bank, half, ways):
        rows = SHAPES[bank][0]
        mine = new_weights[bank].at[pl.ds(half * rows, rows)]
        form_weights(bank, half, me, SHAPES[bank], mine, directions[bank].at[half], mine)
        for way in ways:
            send_own(half, bank, way)

    spread_ratio(0, FIRST, weight_norms[0:1, :] / jnp.sqrt(collect(1)))
    new_weight(ATTN, 0, (1, 2, 0))
    ratio = weight_norms[0:3, :] / jnp.sqrt(collect(2))
    spread_ratio(FIRST, LANES, ratio)
    wait_bytes(early.at[0], early_sent.at[0])
    new_weight(ATTN, 1, (2, 0))
    for half in HALVES:
        new_weight(MLP, half, (1 + half, 0))
    value = wide_weight - row_acc[96:112, 0:HALF] * wide_dir
    new_weights[2][...] = value
    wide_value = value
    vec_row[0:1, 0:LANES] = ratio[1:2, :]
    vec_row[0:1, LANES:VEC_PAD] = ratio[2:3, :]
    value = vec_weight - vec_row[0:1, 0:VEC] * vec_dir
    new_weights[3][...] = value
    all_small[me] = small_message(wide_value, value)
    for way in (1, 2, 0):
        send_own(0, SMALL, way)
    send_own(1, ATTN, 1)
    for half in HALVES:
        send_own(half, MLP, 2 - half)

    wait_bytes(early, early_recv)
    for way, owner in enumerate((along_x, along_y)):
        form_weights(ATTN, 1, owner, (FIRST, EARLY), early.at[0, way], early.at[1, way], None)

    def send_pair(place, chunk):
        send(place, place, sent.at[1, chunk], pair_recv.at[chunk], peer)

    wait_bytes(all_small.at[pl.ds(0, 2)], own_small)
    place = all_small.at[small_near[0]]
    send(place, place, sent.at[1, SMALL], pass_recv.at[SMALL], small_near[1])
    for owner in small_near:
        send_pair(all_small.at[owner], SMALL)
    for chunk in (MLP, ATTN):
        wait_own(0, chunk)
        for half in HALVES:
            owner, target = flip(me, NEAR[half][0]), flip(me, NEAR[half][1])
            place = replica_chunk(half, owner, chunk)
            send_pair(place, chunk)
            if chunk == MLP:
                send(place, place, sent.at[1, MLP], pass_recv.at[MLP], target)
    for index, (first, last) in enumerate(PASSED):
        for half in HALVES:
            place = replica_part(half, flip(me, NEAR[half][0]), first, last)
            send(place, place, sent.at[1, ATTN], attn_pass_recv.at[index], flip(me, NEAR[half][1]))
    for target_core in (0, 1):
        for half in HALVES:
            place = replica_part(half, flip(me, NEAR[half][0]), ATTN_SHARD - TAIL, ATTN_SHARD)
            send(place, place, sent.at[1, ATTN], tail_recv, flip(me, NEAR[half][1] + (PEER if target_core else 0)))
    for chunk in BIG:
        wait_own(1, chunk)
        for half in HALVES:
            send_pair(replica_chunk(half, flip(me, NEAR[half][1]), chunk), chunk)
    far = flip(me, ALONG_X + ALONG_Y)
    wait_bytes(all_small.at[pl.ds(0, 1)], pass_recv.at[SMALL])
    send_pair(all_small.at[far], SMALL)
    wait_bytes(all_small.at[pl.ds(0, 4)], pair_recv.at[SMALL])
    wides, vecs = zip(*(small_parts(all_small[owner].astype(jnp.float32)) for owner in range(8)))
    replicas[2][...] = jnp.concatenate(wides, axis=1).astype(jnp.bfloat16)
    for owner in range(8):
        vec_columns[TALL * owner:TALL * owner + TALL, 0:VEC] = vecs[owner]
    vec_rows[...] = vec_columns[...].T
    replicas[3][...] = vec_rows[0:VEC, :].astype(jnp.bfloat16)
    wait_bytes(all_small, sent.at[0, SMALL])
    wait_bytes(all_small.at[pl.ds(0, len(FAR_FIRST))], sent.at[1, SMALL])
    wait_bytes(early.at[1], early_sent.at[1])
    wait_bytes(all_tiles.at[0, pl.ds(0, len(FAR_FIRST))], tile_sent)
    for bank in BIG:
        wait_bytes(replicas[bank], sent.at[0, bank])
    wait_bytes(replicas[MLP].at[:, pl.ds(0, MLP_SHARD)], pass_recv.at[MLP])
    for half in HALVES:
        send_pair(replica_chunk(half, far, MLP), MLP)
    for index, (first, last) in enumerate(PASSED):
        wait_bytes(replicas[ATTN].at[:, pl.ds(0, last - first)], attn_pass_recv.at[index])
        for half in HALVES:
            send_pair(replica_part(half, far, first, last), ATTN)
    for bank, received, gone in ((MLP, 0, 0), (ATTN, TAIL, EARLY)):
        columns = SHAPES[bank][1]
        wait_bytes(replicas[bank].at[:, pl.ds(0, 4 * columns - received)], pair_recv.at[bank])
        wait_bytes(replicas[bank].at[:, pl.ds(0, len(FAR_FIRST) * columns - gone)], sent.at[1, bank])
    wait_bytes(replicas[ATTN].at[:, pl.ds(0, 2 * TAIL)], tail_recv)


def write_out(*refs):
    count = (len(refs) - 1) // 2
    largest_first = sorted(range(count), key=lambda k: -refs[k].size)
    copies = [pltpu.make_async_copy(refs[k], refs[count + k], refs[-1]) for k in largest_first]
    for copy in copies:
        copy.start()
    for copy in copies:
        copy.wait()


def solution(mesh):
    shards = [jax.ShapeDtypeStruct(shape, jnp.float32) for shape in SHARDS]
    shapes = [jax.ShapeDtypeStruct(shape, jnp.bfloat16) for shape in zip(ROWS, LENGTHS)] + shards * 3
    f32, bf16 = jnp.float32, jnp.bfloat16
    dma = pltpu.SemaphoreType.DMA
    attn, mlp = SHAPES

    def sums(*lead):
        return [pltpu.VMEM((*lead, *attn), f32), pltpu.VMEM((*lead, *mlp), f32)]

    small = (TALL, VEC_PAD)
    scratch = [
        pltpu.VMEM((2, 2, 4, *attn), bf16), pltpu.VMEM((2, 2, 4, *mlp), bf16), pltpu.VMEM((2, 4, *small), bf16),
        *sums(2), pltpu.VMEM(small, f32), *sums(2), pltpu.VMEM(small, f32), *sums(2), pltpu.VMEM(small, f32), *sums(2),
        pltpu.VMEM((2, 2, FIRST, EARLY), f32), pltpu.VMEM((3, *SHARDS[2]), f32), pltpu.VMEM((3, *SHARDS[3]), f32),
        pltpu.VMEM((VEC, LANES), bf16), pltpu.VMEM((TALL, WIDE), bf16), pltpu.VMEM((8, *small), bf16),
        pltpu.VMEM((8, *small), bf16),
        pltpu.VMEM((VEC_PAD, LANES), f32), pltpu.VMEM((LANES, VEC_PAD), f32), pltpu.VMEM((8, VEC_PAD), f32),
        pltpu.VMEM((3, 8, 8, LANES), f32), pltpu.VMEM((LANES, LANES), f32),
        dma((6,)), dma((2, 3)), dma, dma((2, 2)), dma((2,)), dma((3,)), dma((3,)), dma((2, 2)), dma, dma((3,)), dma((3,)),
        dma((2,)), dma, dma, dma((len(PASSED),)), pltpu.SemaphoreType.REGULAR,
    ]
    count = len(shapes)
    anywhere = [pl.BlockSpec(memory_space=pl.ANY)] * count
    step = pl.pallas_call(
        kernel,
        out_shape=[pltpu.VMEM(shape.shape, shape.dtype) for shape in shapes],
        in_specs=anywhere,
        out_specs=[pl.BlockSpec(memory_space=pltpu.VMEM)] * count,
        scratch_shapes=scratch,
        compiler_params=pltpu.CompilerParams(collective_id=0, has_side_effects=True, vmem_limit_bytes=36 * MIB),
        name="lamb_step",
    )
    finish = pl.pallas_call(
        write_out,
        out_shape=shapes,
        in_specs=anywhere,
        out_specs=anywhere,
        scratch_shapes=[dma],
        compiler_params=pltpu.CompilerParams(vmem_limit_bytes=MIB),
        name="write_out",
    )

    def local_step(*banks):
        banks = [bank[0] for bank in banks[:4]] + [bank.T if bank.shape == (VEC, TALL) else bank for bank in banks[4:]]
        banks = [pltpu.with_memory_space_constraint(bank, pltpu.HBM) for bank in banks]
        results = finish(*step(*banks))
        return tuple(value.T if value.shape == (TALL, VEC) else value for value in results)

    grad_spec, shard_spec, full_spec = P("data", None, None), P(None, "data"), P(None, None)
    return jax.shard_map(local_step, mesh=mesh, in_specs=(grad_spec,) * 4 + (shard_spec,) * 12,
                         out_specs=(full_spec,) * 4 + (shard_spec,) * 12, check_vma=False)
```

```python
import functools

import jax
import jax.numpy as jnp
from jax import lax
from jax.experimental import pallas as pl
from jax.experimental.pallas import tpu as pltpu
from jax.sharding import PartitionSpec as P

STEP_NUMBER = 10
LEARN_RATE = 0.04
BETA_FIRST = 0.9
BETA_SECOND = 0.999
EPSILON = 1e-6
WEIGHT_DECAY = 0.01
MAX_NORM = 1.0
FIRST_SCALE = 1.0 / (1.0 - BETA_FIRST ** STEP_NUMBER)
SECOND_SCALE = 1.0 / (1.0 - BETA_SECOND ** STEP_NUMBER)
FIRST_FACTOR = FIRST_SCALE / SECOND_SCALE ** 0.5
EPSILON_TERM = EPSILON / SECOND_SCALE ** 0.5

MESH = pl.DeviceIdType.MESH
LANES = 128
TALL = 16
HALF = 64
FIRST = 32
EARLY = 1024
VEC = 146
VEC_PAD = 256
ATTN_SHARD = 2048
MLP_SHARD = 8192
STEP = 2048
BLOCK = 1024
WIDE = 512
TAIL = 640
PASSED = ((0, 1152), (1152, ATTN_SHARD - TAIL))
MIB = 2 ** 20
ROWS = (HALF, 32, TALL, VEC)
LENGTHS = (16384, 65536, WIDE, LANES)
SHARDS = ((HALF, ATTN_SHARD), (32, MLP_SHARD), (TALL, HALF), (TALL, VEC))
ATTN, MLP, SMALL = range(3)
BIG = (ATTN, MLP)
HALVES = range(2)
SHAPES = ((32, ATTN_SHARD), (TALL, MLP_SHARD))
PEER, ALONG_X, ALONG_Y = 1, 2, 4
NEAR = ((ALONG_X, ALONG_Y), (ALONG_Y, ALONG_X))
WIDE_LANES = (LANES, LANES + HALF)
FAR_FIRST = (6, 4, 2, 7, 5, 3, 1)
TILE_ROWS = (4, 1, 3)


def flip(index, mask):
    core, x, y = index % 2, (index // 2) % 2, index // 4
    if mask & PEER:
        core = 1 - core
    if mask & ALONG_X:
        x = 1 - x
    if mask & ALONG_Y:
        y = 1 - y
    return y * 4 + x * 2 + core


def aligned(index, size):
    return pl.ds(pl.multiple_of(index * size, size), size)


def moments(first, second, total, factors):
    new_first = BETA_FIRST * first + factors[0] * total
    new_second = BETA_SECOND * second + factors[1] * (total * total)
    return new_first, new_second


def direction(new_first, new_second, weight):
    return (new_first * FIRST_FACTOR) / (jnp.sqrt(new_second) + EPSILON_TERM) + WEIGHT_DECAY * weight


def fold(square):
    rows, columns = square.shape
    parts = [square[r:r + 8, k:k + LANES] for r in range(0, rows, 8) for k in range(0, columns, LANES)]
    while len(parts) > 1:
        parts = [a + b for a, b in zip(parts[::2], parts[1::2])] + ([parts[-1]] if len(parts) % 2 else [])
    return parts[0]


def add_all(values):
    return functools.reduce(lambda a, b: a + b, values)


def kernel(*refs):
    grads, weights, firsts, seconds = refs[0:4], refs[4:8], refs[8:12], refs[12:16]
    replicas, new_weights, new_firsts, new_seconds = refs[16:20], refs[20:24], refs[24:28], refs[28:32]
    (recv_attn, recv_mlp, recv_small, part_attn, part_mlp, part_small, last_attn, last_mlp, last_small,
     sum_attn, sum_mlp, sum_small, dir_attn, dir_mlp, early, state_wide, state_vec, vec_in, wide_in, small_out, all_small,
     vec_rows, vec_columns, vec_row, all_tiles, row_acc,
     load_sems, sent, tile_sent, scatter_recv, small_recv, last_recv, tile_recv, own_recv, own_small, pass_recv, pair_recv,
     early_sent, early_recv, tail_recv, attn_pass_recv, ready) = refs[32:]
    recvs, parts, lasts = (recv_attn, recv_mlp), (part_attn, part_mlp), (last_attn, last_mlp)
    me = lax.axis_index("data")
    core = me % 2

    def grad_chunk(half, owner, chunk):
        rows, columns = SHAPES[chunk]
        return grads[chunk].at[pl.ds(rows * half, rows), aligned(owner, columns)]

    def replica_chunk(half, owner, chunk):
        rows, columns = SHAPES[chunk]
        return replicas[chunk].at[pl.ds(rows * half, rows), aligned(owner, columns)]

    def replica_part(half, owner, first, last):
        rows, columns = SHAPES[ATTN]
        start = pl.multiple_of(owner * columns + first, LANES)
        return replicas[ATTN].at[pl.ds(rows * half, rows), pl.ds(start, last - first)]

    along_x, along_y = flip(me, ALONG_X), flip(me, ALONG_Y)
    small_near = (along_x * (1 - core) + along_y * core, along_y * (1 - core) + along_x * core)
    peer = flip(me, PEER)
    peer_next = flip(peer, ALONG_X) * (1 - core) + flip(peer, ALONG_Y) * core

    def send(source, target, send_sem, recv_sem, device):
        copy = pltpu.make_async_remote_copy(src_ref=source, dst_ref=target, send_sem=send_sem, recv_sem=recv_sem,
                                            device_id=(device,), device_id_type=MESH)
        copy.start()
        return copy

    def wait_bytes(ref, sem):
        pltpu.make_async_copy(ref, ref, sem).wait()

    barrier = pltpu.get_barrier_semaphore()

    def signal(semaphore, device):
        pl.semaphore_signal(semaphore, inc=1, device_id=(device,), device_id_type=MESH)

    signal(barrier, peer)

    @pl.when(core == 1)
    def _():
        for mask in (ALONG_X, ALONG_Y):
            for device in (flip(me, mask), flip(peer, mask)):
                signal(barrier, device)


    small_loads = [pltpu.make_async_copy(grads[2], wide_in, load_sems.at[4]),
                   pltpu.make_async_copy(grads[3], vec_in, load_sems.at[5])]
    for copy in small_loads:
        copy.start()
    for keep in range(2):
        for half in HALVES:
            for chunk in (MLP, ATTN):
                owner = me if keep else flip(me, NEAR[half][1])
                pltpu.make_async_copy(grad_chunk(half, owner, chunk), recvs[chunk].at[half, keep, 0],
                                      scatter_recv.at[keep, chunk]).start()
    for index, (source, target) in enumerate(((weights, new_weights), (firsts, new_firsts), (seconds, new_seconds))):
        for bank, place in enumerate((target[0], target[1], state_wide.at[index], state_vec.at[index])):
            pltpu.make_async_copy(source[bank], place, load_sems.at[bank]).start()
    pl.semaphore_wait(barrier, 3)

    def scatter(keep, chunk, slots):
        for slot in slots:
            for half in HALVES:
                target = peer if slot == 0 else flip(me, NEAR[half][0]) // 2 * 2 + slot - 1
                owner = target if keep else flip(target, NEAR[half][1])
                send(grad_chunk(half, owner, chunk), recvs[chunk].at[half, keep, 1 if slot == 0 else 2 + core],
                     sent.at[0, chunk], scatter_recv.at[keep, chunk], target)

    for chunk in (MLP, ATTN):
        scatter(0, chunk, (2, 0))

    @pl.when(core == 1)
    def _():
        signal(ready, along_x)
        signal(ready, along_y)
        pl.semaphore_wait(ready, 2)
        signal(ready, peer)

    @pl.when(core == 0)
    def _():
        pl.semaphore_wait(ready, 1)

    for chunk in (MLP, ATTN):
        scatter(0, chunk, (1,))
    for copy in small_loads:
        copy.wait()
    vec_rows[...] = jnp.zeros_like(vec_rows)
    vec_rows[0:VEC, :] = vec_in[...].astype(jnp.float32)
    vec_columns[...] = vec_rows[...].T

    def small_message(wide, vec):
        pad = jnp.zeros((TALL, VEC_PAD - VEC - HALF), jnp.float32)
        return jnp.concatenate([vec[:, 0:LANES], wide, vec[:, LANES:VEC], pad], axis=1).astype(jnp.bfloat16)

    def small_parts(message):
        vec = jnp.concatenate([message[:, 0:LANES], message[:, WIDE_LANES[1]:HALF + VEC]], axis=1)
        return message[:, slice(*WIDE_LANES)], vec

    wide_grad = wide_in[...].astype(jnp.float32)
    for owner in range(8):
        small_out[owner] = small_message(
            wide_grad[:, HALF * owner:HALF * owner + HALF], vec_columns[TALL * owner:TALL * owner + TALL, 0:VEC])
    for keep in range(2):
        recv_small[keep, 0] = small_out[me if keep else small_near[1]]
        places = [(along_x // 2 * 2, ALONG_Y), (along_y // 2 * 2 + 1, ALONG_X)]
        targets = [(target, target if keep else flip(target, way), 2 + core) for target, way in places]
        for target, owner, slot in [*targets, (peer, peer if keep else peer_next, 1)]:
            send(small_out.at[owner], recv_small.at[keep, slot], sent.at[0, SMALL], small_recv.at[keep], target)
    for chunk in (MLP, ATTN):
        scatter(1, chunk, (1, 2, 0))

    row = lax.broadcasted_iota(jnp.int32, (LANES, LANES), 0)
    lane = lax.broadcasted_iota(jnp.int32, (LANES, LANES), 1)
    eye = row == lane
    sub = lax.broadcasted_iota(jnp.int32, (8, LANES), 0)

    def lanes_of(first, last):
        column = jnp.sum(row_acc[first:last, :], axis=1, keepdims=True)
        return jnp.sum(jnp.where(eye[first:last, :], column, 0.0), axis=0, keepdims=True)

    def vec_lanes(square):
        vec_row[...] = jnp.zeros_like(vec_row)
        vec_row[0:1, 0:VEC] = jnp.sum(square, axis=0, keepdims=True)
        return vec_row[0:1, 0:LANES], vec_row[0:1, LANES:VEC_PAD]

    def tile_of(rows):
        tile = jnp.zeros((8, LANES), jnp.float32)
        for index, value in enumerate(rows):
            tile = jnp.where(sub == index, value, tile)
        return tile

    def exchange(which, value):
        all_tiles[which, me] = value
        place = all_tiles.at[which, me, pl.ds(0, TILE_ROWS[which])]
        for mask in FAR_FIRST:
            send(place, place, tile_sent, tile_recv.at[which], flip(me, mask))

    def collect(which):
        rows = TILE_ROWS[which]
        wait_bytes(all_tiles.at[which, pl.ds(0, len(FAR_FIRST)), pl.ds(0, rows)], tile_recv.at[which])
        return add_all([all_tiles[which, index, 0:rows] for index in range(8)])

    def by_rows(first, groups, columns, step):
        def group(g, carry):
            def inner(j, acc):
                return acc + step((aligned(g, 8), aligned(j, STEP)))

            row_acc[pl.ds(pl.multiple_of(first + g * 8, 8), 8), :] = lax.fori_loop(
                0, columns // STEP, inner, jnp.zeros((8, LANES), jnp.float32))
            return carry

        lax.fori_loop(0, groups, group, 0, unroll=4)

    def square_of(ref):
        return lambda place: fold(ref[place] * ref[place])

    for buffer, sem in ((recv_attn, load_sems.at[ATTN]), (recv_mlp, load_sems.at[MLP])):
        wait_bytes(buffer.at[:, :, pl.ds(0, 3)], sem)
    for bank, buffer in ((2, state_wide), (3, state_vec)):
        wait_bytes(buffer, load_sems.at[bank])
    row_acc[...] = jnp.zeros_like(row_acc)
    by_rows(0, 8, ATTN_SHARD, square_of(new_weights[0]))
    by_rows(HALF, 4, MLP_SHARD, square_of(new_weights[1]))
    wide_weight, vec_weight = state_wide[0], state_vec[0]
    row_acc[96:112, 0:HALF] = wide_weight * wide_weight
    weight_lanes = lanes_of(0, LANES)
    weight_low, weight_high = vec_lanes(vec_weight * vec_weight)

    def by_blocks(shape, step, init):
        rows, columns = shape
        for r in range(0, rows, TALL):
            init = lax.fori_loop(0, columns // BLOCK, functools.partial(
                lambda first, j, carry: step((pl.ds(first, TALL), aligned(j, BLOCK)), carry), r), init, unroll=2)
        return init

    def gather_sum(keep, chunk):
        wait_bytes(recvs[chunk].at[:, keep], scatter_recv.at[keep, chunk])
        for half in HALVES:
            source, target = recvs[chunk].at[half, keep], ((sum_attn, sum_mlp) if keep else parts)[chunk].at[half]

            def step(place, carry):
                value = [source[(slot, *place)].astype(jnp.float32) for slot in range(4)]
                target[place] = (value[0] + value[1]) + (value[2] + value[3])
                return carry

            by_blocks(SHAPES[chunk], step, 0)

    def gather_small(keep, target):
        wait_bytes(recv_small.at[keep, pl.ds(1, 3)], small_recv.at[keep])
        target[...] = add_all([recv_small[keep, slot].astype(jnp.float32) for slot in range(4)])

    for chunk in (MLP, ATTN):
        gather_sum(0, chunk)
    gather_small(0, part_small)
    send(part_small, last_small, sent.at[0, SMALL], last_recv.at[SMALL], small_near[1])
    pieces = ((MLP, pl.ds(0, TALL), MLP), (ATTN, pl.ds(0, TALL), ATTN), (ATTN, pl.ds(TALL, TALL), 3))
    for chunk, rows, index in pieces:
        for half in HALVES:
            send(parts[chunk].at[half, rows], lasts[chunk].at[half, rows], sent.at[0, chunk], last_recv.at[index],
                 flip(me, NEAR[half][1]))
    for chunk in (MLP, ATTN):
        gather_sum(1, chunk)
    gather_small(1, sum_small)

    wait_bytes(last_small, last_recv.at[SMALL])
    wide_total, vec_total = small_parts(sum_small[...] + last_small[...])
    square = fold(jnp.concatenate([wide_total * wide_total, jnp.zeros((TALL, HALF), jnp.float32)], axis=1))
    low, high = vec_lanes(vec_total * vec_total)
    square = square + tile_of([low, high])
    for chunk, rows, index in pieces:
        wait_bytes(lasts[chunk].at[:, rows], last_recv.at[index])
        for half in HALVES:
            total, rest = (sum_attn, sum_mlp)[chunk].at[half, rows], lasts[chunk].at[half, rows]

            def step(place, acc):
                value = total[place] + rest[place]
                total[place] = value
                return acc + fold(value * value)

            square = by_blocks((TALL, SHAPES[chunk][1]), step, square)

    exchange(0, tile_of([weight_lanes, weight_low, weight_high, jnp.sum(square, axis=0, keepdims=True)]))
    late_rows = pl.ds(FIRST, FIRST)
    early_columns = pl.ds(0, EARLY)

    def send_early(kind, source):
        for way, mask in enumerate((ALONG_X, ALONG_Y)):
            send(source, early.at[kind, way], early_sent.at[kind], early_recv, flip(me, mask))

    send_early(0, new_weights[ATTN].at[late_rows, early_columns])
    start = collect(0)
    square = jnp.sum(jnp.sum(start[3:4, :], axis=1, keepdims=True), axis=0, keepdims=True)
    clip = jnp.minimum(1.0, (8.0 * MAX_NORM) / jnp.sqrt(jnp.broadcast_to(square, (8, LANES)))) * 0.125
    factors = ((1.0 - BETA_FIRST) * clip, (1.0 - BETA_SECOND) * (clip * clip))
    factor_blocks = [jnp.concatenate([factor] * (STEP // LANES), axis=1) for factor in factors]
    weight_norms = LEARN_RATE * jnp.sqrt(start)

    sums, directions = (sum_attn, sum_mlp), (dir_attn, dir_mlp)

    def update(bank, half):
        rows = SHAPES[bank][0]

        def step(place):
            state = (pl.ds(pl.multiple_of(half * rows + place[0].start, 8), 8), place[1])
            new_first, new_second = moments(
                new_firsts[bank][state], new_seconds[bank][state], sums[bank].at[half][place], factor_blocks)
            value = direction(new_first, new_second, new_weights[bank][state])
            directions[bank].at[half][place] = value
            return fold(value * value)

        by_rows(HALF * bank + half * rows, rows // 8, SHAPES[bank][1], step)

    def store_moments(bank, half):
        rows = SHAPES[bank][0]

        def step(place, carry):
            state = (pl.ds(half * rows + place[0].start, TALL), place[1])
            wide_factors = [jnp.concatenate([block[:, 0:BLOCK]] * 2, axis=0) for block in factor_blocks]
            new_first, new_second = moments(
                new_firsts[bank][state], new_seconds[bank][state], sums[bank].at[half][place], wide_factors)
            new_firsts[bank][state] = new_first
            new_seconds[bank][state] = new_second
            return carry

        by_blocks(SHAPES[bank], step, 0)

    def update_small(bank, total, state):
        new_first, new_second = moments(state[1], state[2], total, [factor[0:1, 0:1] for factor in factors])
        new_firsts[bank][...] = new_first
        new_seconds[bank][...] = new_second
        return direction(new_first, new_second, state[0])

    update(ATTN, 0)
    exchange(1, tile_of([lanes_of(0, FIRST)]))
    update(ATTN, 1)
    send_early(1, dir_attn.at[1, :, early_columns])
    for half in HALVES:
        update(MLP, half)
    wide_dir = update_small(2, wide_total, state_wide)
    vec_dir = update_small(3, vec_total, state_vec)
    row_acc[96:112, 0:HALF] = wide_dir * wide_dir
    exchange(2, tile_of([lanes_of(FIRST, LANES), *vec_lanes(vec_dir * vec_dir)]))
    for bank in (ATTN, MLP):
        for half in HALVES:
            store_moments(bank, half)

    def send_own(half, chunk, way):
        place = all_small.at[me] if chunk == SMALL else replica_chunk(half, me, chunk)
        if (half, chunk) == (1, ATTN) and way:
            place = replica_part(1, me, EARLY, ATTN_SHARD)
        recv_sem = pair_recv.at[chunk] if not way else own_small if chunk == SMALL else own_recv.at[(way - 1 + half) % 2, chunk]
        send(place, place, sent.at[1, chunk], recv_sem, flip(me, (PEER, ALONG_X, ALONG_Y)[way]))

    def wait_own(kind, chunk):
        columns = SHAPES[chunk][1] - (EARLY // 2 if chunk == ATTN else 0)
        wait_bytes(replicas[chunk].at[:, pl.ds(0, columns)], own_recv.at[kind, chunk])

    def spread_ratio(first, last, ratio):
        row_acc[first:last, :] = jnp.broadcast_to(
            jnp.sum(jnp.where(eye[first:last, :], ratio[0:1, :], 0.0), axis=1, keepdims=True), (last - first, LANES))

    def form_weights(bank, half, owner, shape, weight, direct, result):
        rows = SHAPES[bank][0]

        def step(place, carry):
            first = half * rows + place[0].start
            scale = jnp.concatenate([row_acc[HALF * bank + first:HALF * bank + first + TALL, :]] * (BLOCK // LANES), axis=1)
            value = weight[place] - scale * direct[place]
            if result is not None:
                result[place] = value
            target = pl.ds(pl.multiple_of(owner * SHAPES[bank][1] + place[1].start, BLOCK), BLOCK)
            replicas[bank][pl.ds(first, TALL), target] = value.astype(jnp.bfloat16)
            return carry

        by_blocks(shape, step, 0)

    def new_weight(bank, half, ways):
        rows = SHAPES[bank][0]
        mine = new_weights[bank].at[pl.ds(half * rows, rows)]
        form_weights(bank, half, me, SHAPES[bank], mine, directions[bank].at[half], mine)
        for way in ways:
            send_own(half, bank, way)

    spread_ratio(0, FIRST, weight_norms[0:1, :] / jnp.sqrt(collect(1)))
    new_weight(ATTN, 0, (1, 2, 0))
    ratio = weight_norms[0:3, :] / jnp.sqrt(collect(2))
    spread_ratio(FIRST, LANES, ratio)
    wait_bytes(early.at[0], early_sent.at[0])
    new_weight(ATTN, 1, (2, 0))
    for half in HALVES:
        new_weight(MLP, half, (1 + half, 0))
    value = wide_weight - row_acc[96:112, 0:HALF] * wide_dir
    new_weights[2][...] = value
    wide_value = value
    vec_row[0:1, 0:LANES] = ratio[1:2, :]
    vec_row[0:1, LANES:VEC_PAD] = ratio[2:3, :]
    value = vec_weight - vec_row[0:1, 0:VEC] * vec_dir
    new_weights[3][...] = value
    all_small[me] = small_message(wide_value, value)
    for way in (1, 2, 0):
        send_own(0, SMALL, way)
    send_own(1, ATTN, 1)
    for half in HALVES:
        send_own(half, MLP, 2 - half)

    wait_bytes(early, early_recv)
    for way, owner in enumerate((along_x, along_y)):
        form_weights(ATTN, 1, owner, (FIRST, EARLY), early.at[0, way], early.at[1, way], None)

    def send_pair(place, chunk):
        send(place, place, sent.at[1, chunk], pair_recv.at[chunk], peer)

    wait_bytes(all_small.at[pl.ds(0, 2)], own_small)
    place = all_small.at[small_near[0]]
    send(place, place, sent.at[1, SMALL], pass_recv.at[SMALL], small_near[1])
    for owner in small_near:
        send_pair(all_small.at[owner], SMALL)
    for chunk in (MLP, ATTN):
        wait_own(0, chunk)
        for half in HALVES:
            owner, target = flip(me, NEAR[half][0]), flip(me, NEAR[half][1])
            place = replica_chunk(half, owner, chunk)
            send_pair(place, chunk)
            if chunk == MLP:
                send(place, place, sent.at[1, MLP], pass_recv.at[MLP], target)
    for index, (first, last) in enumerate(PASSED):
        for half in HALVES:
            place = replica_part(half, flip(me, NEAR[half][0]), first, last)
            send(place, place, sent.at[1, ATTN], attn_pass_recv.at[index], flip(me, NEAR[half][1]))
    for target_core in (0, 1):
        for half in HALVES:
            place = replica_part(half, flip(me, NEAR[half][0]), ATTN_SHARD - TAIL, ATTN_SHARD)
            send(place, place, sent.at[1, ATTN], tail_recv, flip(me, NEAR[half][1] + (PEER if target_core else 0)))
    for chunk in BIG:
        wait_own(1, chunk)
        for half in HALVES:
            send_pair(replica_chunk(half, flip(me, NEAR[half][1]), chunk), chunk)
    far = flip(me, ALONG_X + ALONG_Y)
    wait_bytes(all_small.at[pl.ds(0, 1)], pass_recv.at[SMALL])
    send_pair(all_small.at[far], SMALL)
    wait_bytes(all_small.at[pl.ds(0, 4)], pair_recv.at[SMALL])
    wides, vecs = zip(*(small_parts(all_small[owner].astype(jnp.float32)) for owner in range(8)))
    replicas[2][...] = jnp.concatenate(wides, axis=1).astype(jnp.bfloat16)
    for owner in range(8):
        vec_columns[TALL * owner:TALL * owner + TALL, 0:VEC] = vecs[owner]
    vec_rows[...] = vec_columns[...].T
    replicas[3][...] = vec_rows[0:VEC, :].astype(jnp.bfloat16)
    wait_bytes(all_small, sent.at[0, SMALL])
    wait_bytes(all_small.at[pl.ds(0, len(FAR_FIRST))], sent.at[1, SMALL])
    wait_bytes(early.at[1], early_sent.at[1])
    wait_bytes(all_tiles.at[0, pl.ds(0, len(FAR_FIRST))], tile_sent)
    for bank in BIG:
        wait_bytes(replicas[bank], sent.at[0, bank])
    wait_bytes(replicas[MLP].at[:, pl.ds(0, MLP_SHARD)], pass_recv.at[MLP])
    for half in HALVES:
        send_pair(replica_chunk(half, far, MLP), MLP)
    for index, (first, last) in enumerate(PASSED):
        wait_bytes(replicas[ATTN].at[:, pl.ds(0, last - first)], attn_pass_recv.at[index])
        for half in HALVES:
            send_pair(replica_part(half, far, first, last), ATTN)
    for bank, received, gone in ((MLP, 0, 0), (ATTN, TAIL, EARLY)):
        columns = SHAPES[bank][1]
        wait_bytes(replicas[bank].at[:, pl.ds(0, 4 * columns - received)], pair_recv.at[bank])
        wait_bytes(replicas[bank].at[:, pl.ds(0, len(FAR_FIRST) * columns - gone)], sent.at[1, bank])
    wait_bytes(replicas[ATTN].at[:, pl.ds(0, 2 * TAIL)], tail_recv)


def write_out(*refs):
    count = (len(refs) - 1) // 2
    largest_first = sorted(range(count), key=lambda k: -refs[k].size)
    copies = [pltpu.make_async_copy(refs[k], refs[count + k], refs[-1]) for k in largest_first]
    for copy in copies:
        copy.start()
    for copy in copies:
        copy.wait()


def solution(mesh):
    shards = [jax.ShapeDtypeStruct(shape, jnp.float32) for shape in SHARDS]
    shapes = [jax.ShapeDtypeStruct(shape, jnp.bfloat16) for shape in zip(ROWS, LENGTHS)] + shards * 3
    f32, bf16 = jnp.float32, jnp.bfloat16
    dma = pltpu.SemaphoreType.DMA
    attn, mlp = SHAPES

    def sums(*lead):
        return [pltpu.VMEM((*lead, *attn), f32), pltpu.VMEM((*lead, *mlp), f32)]

    small = (TALL, VEC_PAD)
    scratch = [
        pltpu.VMEM((2, 2, 4, *attn), bf16), pltpu.VMEM((2, 2, 4, *mlp), bf16), pltpu.VMEM((2, 4, *small), bf16),
        *sums(2), pltpu.VMEM(small, f32), *sums(2), pltpu.VMEM(small, f32), *sums(2), pltpu.VMEM(small, f32), *sums(2),
        pltpu.VMEM((2, 2, FIRST, EARLY), f32), pltpu.VMEM((3, *SHARDS[2]), f32), pltpu.VMEM((3, *SHARDS[3]), f32),
        pltpu.VMEM((VEC, LANES), bf16), pltpu.VMEM((TALL, WIDE), bf16), pltpu.VMEM((8, *small), bf16),
        pltpu.VMEM((8, *small), bf16),
        pltpu.VMEM((VEC_PAD, LANES), f32), pltpu.VMEM((LANES, VEC_PAD), f32), pltpu.VMEM((8, VEC_PAD), f32),
        pltpu.VMEM((3, 8, 8, LANES), f32), pltpu.VMEM((LANES, LANES), f32),
        dma((6,)), dma((2, 3)), dma, dma((2, 2)), dma((2,)), dma((4,)), dma((3,)), dma((2, 2)), dma, dma((3,)), dma((3,)),
        dma((2,)), dma, dma, dma((len(PASSED),)), pltpu.SemaphoreType.REGULAR,
    ]
    count = len(shapes)
    anywhere = [pl.BlockSpec(memory_space=pl.ANY)] * count
    step = pl.pallas_call(
        kernel,
        out_shape=[pltpu.VMEM(shape.shape, shape.dtype) for shape in shapes],
        in_specs=anywhere,
        out_specs=[pl.BlockSpec(memory_space=pltpu.VMEM)] * count,
        scratch_shapes=scratch,
        compiler_params=pltpu.CompilerParams(collective_id=0, has_side_effects=True, vmem_limit_bytes=36 * MIB),
        name="lamb_step",
    )
    finish = pl.pallas_call(
        write_out,
        out_shape=shapes,
        in_specs=anywhere,
        out_specs=anywhere,
        scratch_shapes=[dma],
        compiler_params=pltpu.CompilerParams(vmem_limit_bytes=MIB),
        name="write_out",
    )

    def local_step(*banks):
        banks = [bank[0] for bank in banks[:4]] + [bank.T if bank.shape == (VEC, TALL) else bank for bank in banks[4:]]
        banks = [pltpu.with_memory_space_constraint(bank, pltpu.HBM) for bank in banks]
        results = finish(*step(*banks))
        return tuple(value.T if value.shape == (TALL, VEC) else value for value in results)

    grad_spec, shard_spec, full_spec = P("data", None, None), P(None, "data"), P(None, None)
    return jax.shard_map(local_step, mesh=mesh, in_specs=(grad_spec,) * 4 + (shard_spec,) * 12,
                         out_specs=(full_spec,) * 4 + (shard_spec,) * 12, check_vma=False)
```
